8 devices in a mesh: row: 2 (over z, y), col: 4 (over x, core).
Axes of the slice: x: 2, y: 2, z: 1, core: 2. Of those that a mesh axis runs over, the one named last changes fastest.
Arguments:
- v_mat: float32 [4096, 4096], P('row', 'col')
- t_fac: float32 [128, 32, 32], P('col')
- z_vec: float32 [4096, 1024], P(None, ('col', 'row'))
Outputs:
- output: float32 [4096, 1024], P('row', 'col')
All inputs are finite; a program needn't handle non-finite values.
Results may differ from the reference program's by a relative error of at most 0.001.
Values sent between devices are 32-bit elements.
A program may use at most 1 GiB of HBM per device.

```python
import jax
import jax.numpy as jnp
from jax import lax

MAT_ORDER = 4096
PANEL_WIDTH = 32
NUM_VECTORS = 1024
ROW_SHARDS = 2
COL_SHARDS = 4


def stored_to_global(mat_order, panel_width, shards):
    stored_idx = jnp.arange(mat_order, dtype=jnp.int32)
    per_shard = mat_order // shards
    shard_idx = stored_idx // per_shard
    within = stored_idx % per_shard
    block_idx = within // panel_width
    offset = within % panel_width
    return (block_idx * shards + shard_idx) * panel_width + offset


def build_factors(v_mat):
    panels = v_mat.reshape(MAT_ORDER, MAT_ORDER // PANEL_WIDTH, PANEL_WIDTH)
    gram_mat = jnp.einsum('nsb,nse->sbe', panels, panels)
    half_diag = 0.5 * jnp.diagonal(gram_mat, axis1=1, axis2=2)
    inv_factor = jnp.triu(gram_mat, 1) + half_diag[:, :, None] * jnp.eye(PANEL_WIDTH, dtype=jnp.float32)
    return jnp.triu(jnp.linalg.inv(inv_factor))


def setup_inputs(seed: int = 0) -> dict:
    rng_key = jax.random.key(seed)
    key_v, key_z = jax.random.split(rng_key)
    raw_vals = jax.random.normal(key_v, (MAT_ORDER, MAT_ORDER), jnp.float32)
    row_ids = stored_to_global(MAT_ORDER, PANEL_WIDTH, ROW_SHARDS)[:, None]
    col_ids = stored_to_global(MAT_ORDER, PANEL_WIDTH, COL_SHARDS)[None, :]
    unit_diag = (row_ids == col_ids).astype(jnp.float32)
    v_mat = jnp.where(row_ids > col_ids, raw_vals, unit_diag)
    t_fac = build_factors(v_mat)
    z_vec = jax.random.normal(key_z, (MAT_ORDER, NUM_VECTORS), jnp.float32)
    return {'v_mat': v_mat, 't_fac': t_fac, 'z_vec': z_vec}


def reference(v_mat, t_fac, z_vec):
    num_panels = MAT_ORDER // PANEL_WIDTH
    local_panels = num_panels // COL_SHARDS

    def apply_panel(x_cur, panel_idx):
        panel_slot = (panel_idx % COL_SHARDS) * local_panels + panel_idx // COL_SHARDS
        v_pan = lax.dynamic_slice_in_dim(v_mat, panel_slot * PANEL_WIDTH, PANEL_WIDTH, axis=1)
        t_pan = lax.dynamic_index_in_dim(t_fac, panel_slot, axis=0, keepdims=False)
        w_blk = jnp.dot(v_pan.T, x_cur, preferred_element_type=jnp.float32)
        y_blk = jnp.dot(t_pan, w_blk, preferred_element_type=jnp.float32)
        x_new = x_cur - jnp.dot(v_pan, y_blk, preferred_element_type=jnp.float32)
        return x_new, None

    x_out, _ = lax.scan(apply_panel, z_vec, jnp.arange(num_panels - 1, -1, -1))
    return x_out
```

```python
import functools

import jax
import jax.numpy as jnp
from jax import lax
from jax.experimental import pallas as pl
from jax.experimental.pallas import tpu as pltpu
from jax.sharding import PartitionSpec as P

MESH = pl.DeviceIdType.MESH
F32, BF16 = jnp.float32, jnp.bfloat16
STEPS = 16
OFF = [k * (k - 1) // 2 for k in range(STEPS + 2)]
NT = (((1,), (1,)), ((), ()))
NN = (((1,), (0,)), ((), ()))
FX, FY, DX, DY, SO, SX, SY, SD, SE, LO = range(10)
TX, TY, TS, GX, GY, HX, HY, HD, HE = range(9)


def split3(a):
    p1 = a.astype(BF16)
    rest = a - p1.astype(F32)
    p2 = rest.astype(BF16)
    p3 = (rest - p2.astype(F32)).astype(BF16)
    return p1, p2, p3


def mul6(a, b, dims):
    dot = functools.partial(lax.dot_general, dimension_numbers=dims, preferred_element_type=F32)
    return (
        dot(a[0], b[0]) + dot(a[1], b[0]) + dot(a[2], b[0]) + dot(a[0], b[1]) + dot(a[1], b[1]) + dot(a[0], b[2])
    )


def mulf(a, b, dims=NN):
    return mul6(split3(a), split3(b), dims)


def kernel(vt_ref, tp_ref, z_ref, out_ref, land, tl, xt, vp, acc, yp, rs, ss, ts, zs, os):
    r, c = lax.axis_index("row"), lax.axis_index("col")
    cs = c + 1 - 2 * lax.rem(c, 2)
    cx = lax.rem(c + 2, 4)
    csx = lax.rem(cs + 2, 4)
    ry = 1 - r
    to_x, to_y, to_s = (r, cx), (ry, c), (r, cs)

    barrier = pltpu.get_barrier_semaphore()
    for dev in (to_x, to_y, to_s):
        pl.semaphore_signal(barrier, inc=1, device_id=dev, device_id_type=MESH)
    pl.semaphore_wait(barrier, 3)

    def seg(k, rr, cc, lo=0, n=None):
        return land.at[pl.ds(OFF[k] + lo, k if n is None else n), rr, :, cc]

    def remote(src, dst, send, recv, dev):
        return pltpu.make_async_remote_copy(
            src_ref=src, dst_ref=dst, send_sem=send, recv_sem=recv, device_id=dev, device_id_type=MESH
        )

    def own(k):
        return vt_ref.at[pl.ds(STEPS - k, k), pl.ds(2 * (STEPS - k), 2)]

    def halves(k):
        h = (k + 1) // 2 if k % 2 else k // 2
        if k % 4 == 1:
            h = k // 2
        return (0, h), (h, k - h)

    def c_own(k):
        return [
            remote(own(k), seg(k, r, c), ss.at[TX, k], rs.at[FX, k], to_x),
            remote(own(k), seg(k, r, c), ss.at[TY, k], rs.at[FY, k], to_y),
            remote(own(k), seg(k, r, c), ss.at[TS, k], rs.at[SO, k], to_s),
        ]

    def c_loc(k):
        return pltpu.make_async_copy(own(k), seg(k, r, c), rs.at[LO, k])

    def c_fwd(k):
        (a0, an), (b0, bn) = halves(k)
        out = []
        if an:
            out.append(remote(seg(k, r, cx, a0, an), seg(k, r, cx, a0, an), ss.at[GY, k], rs.at[DY, k], to_y))
        if bn:
            out.append(remote(seg(k, ry, c, b0, bn), seg(k, ry, c, b0, bn), ss.at[GX, k], rs.at[DX, k], to_x))
        return out

    def c_sib(k):
        return [
            remote(seg(k, r, cx), seg(k, r, cx), ss.at[HX, k], rs.at[SX, k], to_s),
            remote(seg(k, ry, c), seg(k, ry, c), ss.at[HY, k], rs.at[SY, k], to_s),
        ]

    def c_dia(k):
        (a0, an), (b0, bn) = halves(k)
        out = []
        if an:
            out.append(remote(seg(k, ry, cx, a0, an), seg(k, ry, cx, a0, an), ss.at[HD, k], rs.at[SD, k], to_s))
        if bn:
            out.append(remote(seg(k, ry, cx, b0, bn), seg(k, ry, cx, b0, bn), ss.at[HE, k], rs.at[SE, k], to_s))
        return out

    def arrive(dst, sem):
        pltpu.make_async_copy(dst, dst, sem).wait()

    def wait_first(k):
        arrive(seg(k, r, cx), rs.at[FX, k])
        arrive(seg(k, ry, c), rs.at[FY, k])

    def wait_dia(k):
        (a0, an), (b0, bn) = halves(k)
        if an:
            arrive(seg(k, ry, cx, a0, an), rs.at[DY, k])
        if bn:
            arrive(seg(k, ry, cx, b0, bn), rs.at[DX, k])

    def wait_sib(k):
        arrive(seg(k, r, c), rs.at[LO, k])
        arrive(seg(k, r, cs), rs.at[SO, k])
        arrive(seg(k, r, csx), rs.at[SX, k])
        arrive(seg(k, ry, cs), rs.at[SY, k])
        (a0, an), (b0, bn) = halves(k)
        if an:
            arrive(seg(k, ry, csx, a0, an), rs.at[SD, k])
        if bn:
            arrive(seg(k, ry, csx, b0, bn), rs.at[SE, k])

    def start_own(k):
        for cp in c_own(k):
            cp.start()
        c_loc(k).start()

    def at_step(k, fn, lo, hi):
        for kk in range(lo, hi + 1):
            @pl.when(k == kk)
            def _(kk=kk):
                fn(kk)

    t_copies = [
        remote(tp_ref, tl.at[:, c], ts.at[0], ts.at[1], to_x),
        remote(tp_ref, tl.at[:, c], ts.at[2], ts.at[3], to_s),
    ]
    t_on = remote(tl.at[:, cx], tl.at[:, cx], ts.at[4], ts.at[5], to_s)
    t_loc = pltpu.make_async_copy(tp_ref, tl.at[:, c], ts.at[6])
    z_loc = pltpu.make_async_copy(z_ref, xt, zs.at[0])

    start_own(1)
    for cp in t_copies:
        cp.start()
    t_loc.start()
    z_loc.start()
    start_own(2)
    wait_first(1)
    for cp in c_fwd(1) + c_sib(1):
        cp.start()
    arrive(tl.at[:, cx], ts.at[1])
    t_on.start()
    arrive(tl.at[:, cs], ts.at[3])
    arrive(tl.at[:, csx], ts.at[5])
    t_loc.wait()
    z_loc.wait()

    lane = lax.broadcasted_iota(jnp.int32, (128, 128), 1)
    sub = lax.broadcasted_iota(jnp.int32, (128, 128), 0)
    pr, pc = sub // 32, lane // 32
    level1 = (pr // 2 == pc // 2) & (pr < pc)
    level2 = pr // 2 < pc // 2

    def step(k, carry):
        def ahead(kk):
            if kk + 2 <= STEPS:
                start_own(kk + 2)
            if kk + 1 <= STEPS:
                wait_first(kk + 1)
                for cp in c_fwd(kk + 1) + c_sib(kk + 1):
                    cp.start()
            wait_dia(kk)
            for cp in c_dia(kk):
                cp.start()
            wait_sib(kk)

        at_step(k, ahead, 1, STEPS)

        J = STEPS - k
        off = k * (k - 1) // 2
        acc[...] = jnp.zeros_like(acc)

        def tile(m, carry):
            v = jnp.concatenate([land[off + m, 0].reshape(256, 128), land[off + m, 1].reshape(256, 128)], axis=1)
            x = jnp.concatenate([xt[0, J + m], xt[1, J + m]], axis=1)
            vs = split3(v)
            for i in range(3):
                vp[i, m] = vs[i]
            lhs = [jnp.concatenate([a, b], axis=0) for a, b in zip(split3(x), vs)]
            acc[...] += mul6(lhs, vs, NT)
            return carry

        lax.fori_loop(0, k, tile, 0)

        q, h = J // 2, lax.rem(J, 2)

        def diag(tt):
            rows = []
            for cc in range(4):
                t32 = tl[q, cc]
                t32 = jnp.where(h == 0, t32, pltpu.roll(t32, 64, 1))
                shift = (32 * cc - 32 * tt) % 128
                rows.append(pltpu.roll(t32, shift, 1) if shift else t32)
            full = jnp.concatenate(rows, axis=0)
            return jnp.where(pr == pc, full, 0.0)

        halves_t = []
        for tt in range(2):
            g = acc[128 + 128 * tt : 256 + 128 * tt, 128 * tt : 128 * tt + 128]
            t = diag(tt)
            t = t - mulf(t, mulf(jnp.where(level1, g, 0.0), t))
            t = t - mulf(t, mulf(jnp.where(level2, g, 0.0), t))
            halves_t.append(t)
        t1, t2 = halves_t
        t12 = -mulf(t1, mulf(acc[128:256, 128:256], t2))
        w1, w2 = acc[0:128, 0:128], acc[0:128, 128:256]
        w2s = split3(w2)
        y1 = mul6(split3(w1), split3(t1), NT) + mul6(w2s, split3(t12), NT)
        y2 = mul6(w2s, split3(t2), NT)
        ys = split3(jnp.concatenate([y1, y2], axis=1))
        for i in range(3):
            yp[i] = ys[i]

        def send(m):
            return remote(xt.at[ry, m], out_ref.at[r, m], os.at[0], os.at[1], to_y)

        def update(m, carry):
            d = mul6([yp[i] for i in range(3)], [vp[i, m] for i in range(3)], NN)
            xt[0, J + m] = xt[0, J + m] - d[:, :128]
            xt[1, J + m] = xt[1, J + m] - d[:, 128:]

            @pl.when((k == STEPS) & (m > 0))
            def _():
                send(m - 1).start()

            return carry

        lax.fori_loop(0, k, update, 0)
        return carry

    lax.fori_loop(1, STEPS + 1, step, 0)

    o_loc = pltpu.make_async_copy(xt.at[r], out_ref.at[r], os.at[2])
    last = remote(xt.at[ry, STEPS - 1], out_ref.at[r, STEPS - 1], os.at[0], os.at[1], to_y)

    for cp in t_copies:
        cp.wait_send()
    t_on.wait_send()
    for k in range(1, STEPS + 1):
        for cp in c_own(k) + c_fwd(k) + c_sib(k) + c_dia(k):
            cp.wait_send()
    last.start()
    o_loc.start()
    o_loc.wait()
    whole = remote(xt.at[ry], out_ref.at[r], os.at[0], os.at[1], to_y)
    whole.wait_send()
    arrive(out_ref.at[ry], os.at[1])


def solution(mesh):
    def body(v_loc, t_loc, z_loc):
        vt = jnp.transpose(v_loc.reshape(16, 128, 1024), (0, 2, 1)).reshape(16, 32, 32, 128)
        tp = jnp.transpose(t_loc.reshape(8, 4, 32, 32), (0, 2, 1, 3)).reshape(8, 32, 128)
        zt = jnp.transpose(z_loc.reshape(2, 16, 128, 128), (0, 1, 3, 2))
        out = pl.pallas_call(
            kernel,
            out_shape=jax.ShapeDtypeStruct((2, 16, 128, 128), F32),
            in_specs=[pl.BlockSpec(memory_space=pl.ANY)] * 3,
            out_specs=pl.BlockSpec(memory_space=pl.ANY),
            scratch_shapes=[
                pltpu.VMEM((OFF[STEPS + 1], 2, 2, 4, 32, 128), F32),
                pltpu.VMEM((8, 4, 32, 128), F32),
                pltpu.VMEM((2, 16, 128, 128), F32),
                pltpu.VMEM((3, 16, 256, 256), BF16),
                pltpu.VMEM((384, 256), F32),
                pltpu.VMEM((3, 128, 256), BF16),
                pltpu.SemaphoreType.DMA((10, STEPS + 1)),
                pltpu.SemaphoreType.DMA((9, STEPS + 1)),
                pltpu.SemaphoreType.DMA((7,)),
                pltpu.SemaphoreType.DMA((1,)),
                pltpu.SemaphoreType.DMA((3,)),
            ],
            compiler_params=pltpu.CompilerParams(
                collective_id=0, has_side_effects=True, vmem_limit_bytes=64 * 1024 * 1024 - 65536
            ),
        )(vt, tp, zt)
        return jnp.transpose(out, (1, 3, 0, 2)).reshape(2048, 256)

    return jax.shard_map(
        body,
        mesh=mesh,
        in_specs=(P("row", "col"), P("col", None, None), P(None, ("col", "row"))),
        out_specs=P("row", "col"),
        check_vma=False,
    )
```

```python
import functools

import jax
import jax.numpy as jnp
from jax import lax
from jax.experimental import pallas as pl
from jax.experimental.pallas import tpu as pltpu
from jax.sharding import PartitionSpec as P

MESH = pl.DeviceIdType.MESH
F32, BF16 = jnp.float32, jnp.bfloat16
STEPS = 16
OFF = [k * (k - 1) // 2 for k in range(STEPS + 2)]
NT = (((1,), (1,)), ((), ()))
NN = (((1,), (0,)), ((), ()))
SWAP = 13
REST = STEPS - SWAP
O, F, D, S, T, X = range(6)
BEFORE = {
    1: ((O, 1), (T, 0), (O, 2), (F, 1), (O, 3), (F, 2), (O, 4), (D, 1), (S, 1)),
    2: ((S, 2),),
    3: ((F, 5), (D, 3), (D, 4), (S, 3)),
    4: ((S, 4),),
    5: ((D, 5), (S, 5), (O, 8)),
    6: ((D, 6), (S, 6), (O, 9)),
    7: ((D, 7), (S, 7)),
}
BEFORE |= {k: ((F, k + 1), (D, k), (S, k)) for k in range(8, 16)}
BEFORE[16] = ((D, 16), (S, 16))
MIDDLE = {1: ((O, 5),), 2: ((F, 4), (O, 6)), 3: ((O, 7),)}
MIDDLE |= {k: ((O, k + 3),) for k in range(7, 14)}
MIDDLE[14] = ((X, 0),)
AFTER = {1: ((F, 3), (D, 2)), 4: ((F, 6),), 5: ((F, 7),), 6: ((F, 8),)}
ALONG_Y = [0, 0, 1, 1, 2, 2, 3, 3, 4, 4, 5, 5, 6, 6, 7, 0, 0]
FX, FY, DX, DY, SO, SX, SY, SD, SE, LO = range(10)
TX, TY, TS, GX, GY, HX, HY, HD, HE = range(9)


def split3(a):
    p1 = a.astype(BF16)
    rest = a - p1.astype(F32)
    p2 = rest.astype(BF16)
    p3 = (rest - p2.astype(F32)).astype(BF16)
    return p1, p2, p3


def mul6(a, b, dims):
    dot = functools.partial(lax.dot_general, dimension_numbers=dims, preferred_element_type=F32)
    return (
        dot(a[0], b[0]) + dot(a[1], b[0]) + dot(a[2], b[0]) + dot(a[0], b[1]) + dot(a[1], b[1]) + dot(a[0], b[2])
    )


def mulf(a, b, dims=NN):
    return mul6(split3(a), split3(b), dims)


def kernel(vt_ref, tp_ref, z_ref, out_ref, land, tl, xt, xs, xn, yo, yn, vp, acc, yp, rs, ss, ts, zs, os, ys):
    r, c = lax.axis_index("row"), lax.axis_index("col")
    cs = c + 1 - 2 * lax.rem(c, 2)
    cx = lax.rem(c + 2, 4)
    csx = lax.rem(cs + 2, 4)
    ry = 1 - r
    to_x, to_y, to_s = (r, cx), (ry, c), (r, cs)

    barrier = pltpu.get_barrier_semaphore()
    for dev in (to_x, to_y, to_s):
        pl.semaphore_signal(barrier, inc=1, device_id=dev, device_id_type=MESH)
    pl.semaphore_wait(barrier, 3)

    def seg(k, rr, cc, lo=0, n=None):
        return land.at[pl.ds(OFF[k] + lo, k if n is None else n), rr, :, cc]

    def remote(src, dst, send, recv, dev):
        return pltpu.make_async_remote_copy(
            src_ref=src, dst_ref=dst, send_sem=send, recv_sem=recv, device_id=dev, device_id_type=MESH
        )

    def own(k):
        return vt_ref.at[pl.ds(STEPS - k, k), pl.ds(2 * (STEPS - k), 2)]

    def halves(k):
        h = ALONG_Y[k]
        return (0, h), (h, k - h)

    def c_own(k):
        return [
            remote(own(k), seg(k, r, c), ss.at[TX, k], rs.at[FX, k], to_x),
            remote(own(k), seg(k, r, c), ss.at[TY, k], rs.at[FY, k], to_y),
            remote(own(k), seg(k, r, c), ss.at[TS, k], rs.at[SO, k], to_s),
        ]

    def c_loc(k):
        return pltpu.make_async_copy(own(k), seg(k, r, c), rs.at[LO, k])

    def c_fwd(k):
        (a0, an), (b0, bn) = halves(k)
        out = []
        if an:
            out.append(remote(seg(k, r, cx, a0, an), seg(k, r, cx, a0, an), ss.at[GY, k], rs.at[DY, k], to_y))
        if bn:
            out.append(remote(seg(k, ry, c, b0, bn), seg(k, ry, c, b0, bn), ss.at[GX, k], rs.at[DX, k], to_x))
        return out

    def c_sib(k):
        return [
            remote(seg(k, r, cx), seg(k, r, cx), ss.at[HX, k], rs.at[SX, k], to_s),
            remote(seg(k, ry, c), seg(k, ry, c), ss.at[HY, k], rs.at[SY, k], to_s),
        ]

    def c_dia(k):
        (a0, an), (b0, bn) = halves(k)
        out = []
        if an:
            out.append(remote(seg(k, ry, cx, a0, an), seg(k, ry, cx, a0, an), ss.at[HD, k], rs.at[SD, k], to_s))
        if bn:
            out.append(remote(seg(k, ry, cx, b0, bn), seg(k, ry, cx, b0, bn), ss.at[HE, k], rs.at[SE, k], to_s))
        return out

    def arrive(dst, sem):
        pltpu.make_async_copy(dst, dst, sem).wait()

    def wait_first(k):
        arrive(seg(k, r, cx), rs.at[FX, k])
        arrive(seg(k, ry, c), rs.at[FY, k])

    def wait_dia(k):
        (a0, an), (b0, bn) = halves(k)
        if an:
            arrive(seg(k, ry, cx, a0, an), rs.at[DY, k])
        if bn:
            arrive(seg(k, ry, cx, b0, bn), rs.at[DX, k])

    def wait_sib(k):
        arrive(seg(k, r, c), rs.at[LO, k])
        arrive(seg(k, r, cs), rs.at[SO, k])
        arrive(seg(k, r, csx), rs.at[SX, k])
        arrive(seg(k, ry, cs), rs.at[SY, k])
        (a0, an), (b0, bn) = halves(k)
        if an:
            arrive(seg(k, ry, csx, a0, an), rs.at[SD, k])
        if bn:
            arrive(seg(k, ry, csx, b0, bn), rs.at[SE, k])

    def start_own(k):
        for cp in c_own(k):
            cp.start()
        c_loc(k).start()

    t_copies = [
        remote(tp_ref, tl.at[:, c], ts.at[0], ts.at[1], to_x),
        remote(tp_ref, tl.at[:, c], ts.at[2], ts.at[3], to_s),
    ]
    t_on = remote(tl.at[:, cx], tl.at[:, cx], ts.at[4], ts.at[5], to_s)
    t_loc = pltpu.make_async_copy(tp_ref, tl.at[:, c], ts.at[6])
    z_loc = pltpu.make_async_copy(z_ref, xt, zs.at[0])

    x_copy = remote(xs, xn, os.at[0], os.at[1], to_y)

    def y_copy(i):
        return remote(yo.at[i], yn.at[i], ys.at[0, i], ys.at[1, i], to_y)

    def do(ops):
        for op, k in ops:
            if op == O:
                start_own(k)
            elif op == F:
                wait_first(k)
                for cp in c_fwd(k) + c_sib(k):
                    cp.start()
                if k == 1:
                    arrive(tl.at[:, cx], ts.at[1])
                    t_on.start()
            elif op == D:
                wait_dia(k)
                for cp in c_dia(k):
                    cp.start()
            elif op == S:
                wait_sib(k)
                if k == 1:
                    arrive(tl.at[:, cs], ts.at[3])
                    arrive(tl.at[:, csx], ts.at[5])
                    t_loc.wait()
                    z_loc.wait()
                if k > SWAP + 1:
                    y_copy(k - SWAP - 2).start()
            elif op == T:
                for cp in t_copies:
                    cp.start()
                t_loc.start()
                z_loc.start()
            else:
                x_copy.start()

    def point(k, table):
        for kk, ops in table.items():
            @pl.when(k == kk)
            def _(ops=ops):
                do(ops)

    lane = lax.broadcasted_iota(jnp.int32, (128, 128), 1)
    sub = lax.broadcasted_iota(jnp.int32, (128, 128), 0)
    pr, pc = sub // 32, lane // 32
    level1 = (pr // 2 == pc // 2) & (pr < pc)
    level2 = pr // 2 < pc // 2

    def step(k, carry):
        point(k, BEFORE)
        J = STEPS - k
        off = k * (k - 1) // 2
        acc[...] = jnp.zeros_like(acc)

        def tile(m, carry):
            v = jnp.concatenate([land[off + m, 0].reshape(256, 128), land[off + m, 1].reshape(256, 128)], axis=1)
            x = jnp.concatenate([xt[0, J + m], xt[1, J + m]], axis=1)
            vs = split3(v)
            for i in range(3):
                vp[i, m] = vs[i]
            lhs = [jnp.concatenate([a, b], axis=0) for a, b in zip(split3(x), vs)]
            acc[...] += mul6(lhs, vs, NT)
            return carry

        mid = lax.div(k + 1, 2)
        lax.fori_loop(0, mid, tile, 0)
        point(k, MIDDLE)
        lax.fori_loop(mid, k, tile, 0)

        q, h = J // 2, lax.rem(J, 2)

        def diag(tt):
            rows = []
            for cc in range(4):
                t32 = tl[q, cc]
                t32 = jnp.where(h == 0, t32, pltpu.roll(t32, 64, 1))
                shift = (32 * cc - 32 * tt) % 128
                rows.append(pltpu.roll(t32, shift, 1) if shift else t32)
            full = jnp.concatenate(rows, axis=0)
            return jnp.where(pr == pc, full, 0.0)

        halves_t = []
        for tt in range(2):
            g = acc[128 + 128 * tt : 256 + 128 * tt, 128 * tt : 128 * tt + 128]
            t = diag(tt)
            t = t - mulf(t, mulf(jnp.where(level1, g, 0.0), t))
            t = t - mulf(t, mulf(jnp.where(level2, g, 0.0), t))
            halves_t.append(t)
        t1, t2 = halves_t
        t12 = -mulf(t1, mulf(acc[128:256, 128:256], t2))
        w1, w2 = acc[0:128, 0:128], acc[0:128, 128:256]
        w2s = split3(w2)
        y1 = mul6(split3(w1), split3(t1), NT) + mul6(w2s, split3(t12), NT)
        y2 = mul6(w2s, split3(t2), NT)
        y = jnp.concatenate([y1, y2], axis=1)
        for i, part in enumerate(split3(y)):
            yp[i] = part

        @pl.when(k > SWAP)
        def _():
            yo[k - SWAP - 1] = y

        point(k, AFTER)

        def update(m, carry):
            d = mul6([yp[i] for i in range(3)], [vp[i, m] for i in range(3)], NN)
            xt[0, J + m] = xt[0, J + m] - d[:, :128]
            xt[1, J + m] = xt[1, J + m] - d[:, 128:]
            return carry

        @pl.when(k < STEPS)
        def _():
            lax.fori_loop(0, k, update, 0)

        @pl.when(k == SWAP)
        def _():
            def stage(m, carry):
                xs[m] = xt[ry, m]
                return carry

            lax.fori_loop(0, STEPS, stage, 0)

        return carry

    lax.fori_loop(1, STEPS + 1, step, 0)

    def half(dst, k, parts, lo, hi):
        def tile(m, carry):
            v = split3(land[OFF[k] + m, r].reshape(256, 128))
            dst[STEPS - k + m] = dst[STEPS - k + m] - mul6(parts, v, NN)
            return carry

        lax.fori_loop(lo, hi, tile, 0)

    last = [yp[i] for i in range(3)]
    half(xt.at[r], STEPS, last, 0, 4)
    y_copy(REST - 1).start()
    half(xt.at[r], STEPS, last, 4, STEPS)
    o_loc = pltpu.make_async_copy(xt.at[r], out_ref.at[r], os.at[2])
    o_loc.start()
    arrive(xn, os.at[1])
    for i in range(REST):
        arrive(yn.at[i], ys.at[1, i])
        half(xn, SWAP + 1 + i, split3(yn[i]), 0, SWAP + 1 + i)
    o_nbr = pltpu.make_async_copy(xn, out_ref.at[ry], os.at[3])
    o_nbr.start()

    for cp in t_copies:
        cp.wait_send()
    t_on.wait_send()
    for k in range(1, STEPS + 1):
        for cp in c_own(k) + c_fwd(k) + c_sib(k) + c_dia(k):
            cp.wait_send()
    x_copy.wait_send()
    for i in range(REST):
        y_copy(i).wait_send()
    o_loc.wait()
    o_nbr.wait()


def solution(mesh):
    def body(v_loc, t_loc, z_loc):
        vt = jnp.transpose(v_loc.reshape(16, 128, 1024), (0, 2, 1)).reshape(16, 32, 32, 128)
        tp = jnp.transpose(t_loc.reshape(8, 4, 32, 32), (0, 2, 1, 3)).reshape(8, 32, 128)
        zt = jnp.transpose(z_loc.reshape(2, 16, 128, 128), (0, 1, 3, 2))
        out = pl.pallas_call(
            kernel,
            out_shape=jax.ShapeDtypeStruct((2, 16, 128, 128), F32),
            in_specs=[pl.BlockSpec(memory_space=pl.ANY)] * 3,
            out_specs=pl.BlockSpec(memory_space=pl.ANY),
            scratch_shapes=[
                pltpu.VMEM((OFF[STEPS + 1], 2, 2, 4, 32, 128), F32),
                pltpu.VMEM((8, 4, 32, 128), F32),
                pltpu.VMEM((2, 16, 128, 128), F32),
                pltpu.VMEM((16, 128, 128), F32),
                pltpu.VMEM((16, 128, 128), F32),
                pltpu.VMEM((REST, 128, 256), F32),
                pltpu.VMEM((REST, 128, 256), F32),
                pltpu.VMEM((3, 16, 256, 256), BF16),
                pltpu.VMEM((384, 256), F32),
                pltpu.VMEM((3, 128, 256), BF16),
                pltpu.SemaphoreType.DMA((10, STEPS + 1)),
                pltpu.SemaphoreType.DMA((9, STEPS + 1)),
                pltpu.SemaphoreType.DMA((7,)),
                pltpu.SemaphoreType.DMA((1,)),
                pltpu.SemaphoreType.DMA((4,)),
                pltpu.SemaphoreType.DMA((2, REST)),
            ],
            compiler_params=pltpu.CompilerParams(
                collective_id=0, has_side_effects=True, vmem_limit_bytes=64 * 1024 * 1024 - 65536
            ),
        )(vt, tp, zt)
        return jnp.transpose(out, (1, 3, 0, 2)).reshape(2048, 256)

    return jax.shard_map(
        body,
        mesh=mesh,
        in_specs=(P("row", "col"), P("col", None, None), P(None, ("col", "row"))),
        out_specs=P("row", "col"),
        check_vma=False,
    )
```

```python
import functools

import jax
import jax.numpy as jnp
from jax import lax
from jax.experimental import pallas as pl
from jax.experimental.pallas import tpu as pltpu
from jax.sharding import PartitionSpec as P

MESH = pl.DeviceIdType.MESH
F32, BF16 = jnp.float32, jnp.bfloat16
STEPS = 16
OFF = [k * (k - 1) // 2 for k in range(STEPS + 2)]
NT = (((1,), (1,)), ((), ()))
NN = (((1,), (0,)), ((), ()))
SWAP = 13
REST = STEPS - SWAP
O, F, D, S, T, X = range(6)
BEFORE = {
    1: ((O, 1), (T, 0), (O, 2), (F, 1), (O, 3), (F, 2), (O, 4), (D, 1), (S, 1)),
    2: ((S, 2),),
    3: ((F, 5), (D, 3), (D, 4), (S, 3)),
    4: ((S, 4),),
    5: ((D, 5), (S, 5), (O, 8)),
    6: ((D, 6), (S, 6), (O, 9)),
    7: ((D, 7), (S, 7)),
}
BEFORE |= {k: ((F, k + 1), (D, k), (S, k)) for k in range(8, 16)}
BEFORE[16] = ((D, 16), (S, 16))
MIDDLE = {1: ((O, 5),), 2: ((F, 4), (O, 6)), 3: ((O, 7),)}
MIDDLE |= {k: ((O, k + 3),) for k in range(7, 14)}
MIDDLE[14] = ((X, 0),)
AFTER = {1: ((F, 3), (D, 2)), 4: ((F, 6),), 5: ((F, 7),), 6: ((F, 8),)}
ALONG_Y = [0, 0, 1, 1, 2, 2, 3, 3, 4, 4, 5, 5, 6, 6, 7, 0, 0]
FX, FY, DX, DY, SO, SX, SY, SD, SE, LO = range(10)
TX, TY, TS, GX, GY, HX, HY, HD, HE = range(9)


def split3(a):
    p1 = a.astype(BF16)
    rest = a - p1.astype(F32)
    p2 = rest.astype(BF16)
    p3 = (rest - p2.astype(F32)).astype(BF16)
    return p1, p2, p3


def mul6(a, b, dims):
    dot = functools.partial(lax.dot_general, dimension_numbers=dims, preferred_element_type=F32)
    return (
        dot(a[0], b[0]) + dot(a[1], b[0]) + dot(a[2], b[0]) + dot(a[0], b[1]) + dot(a[1], b[1]) + dot(a[0], b[2])
    )


def mulf(a, b, dims=NN):
    return mul6(split3(a), split3(b), dims)


def kernel(vt_ref, tp_ref, z_ref, out_ref, land, tl, xt, xs, xn, yo, yn, vp, acc, yp, rs, ss, ts, zs, os, ys):
    r, c = lax.axis_index("row"), lax.axis_index("col")
    cs = c + 1 - 2 * lax.rem(c, 2)
    cx = lax.rem(c + 2, 4)
    csx = lax.rem(cs + 2, 4)
    ry = 1 - r
    to_x, to_y, to_s = (r, cx), (ry, c), (r, cs)

    def seg(k, rr, cc, lo=0, n=None):
        return land.at[pl.ds(8 * OFF[k] + (rr * 4 + cc) * k + lo, k if n is None else n)]

    def rows(k, base, rr, m):
        got = [land[base + (rr * 4 + cc) * k + m] for cc in range(4)]
        return jnp.concatenate([g[:32] for g in got] + [g[32:] for g in got], axis=0)

    def remote(src, dst, send, recv, dev):
        return pltpu.make_async_remote_copy(
            src_ref=src, dst_ref=dst, send_sem=send, recv_sem=recv, device_id=dev, device_id_type=MESH
        )

    def own(k):
        return vt_ref.at[pl.ds(STEPS - k, k), STEPS - k]

    def halves(k):
        h = ALONG_Y[k]
        return (0, h), (h, k - h)

    def c_own(k):
        mine = seg(k, r, c)
        return [
            remote(mine, mine, ss.at[TX, k], rs.at[FX, k], to_x),
            remote(mine, mine, ss.at[TY, k], rs.at[FY, k], to_y),
            remote(mine, mine, ss.at[TS, k], rs.at[SO, k], to_s),
        ]

    def c_loc(k):
        return pltpu.make_async_copy(own(k), seg(k, r, c), rs.at[LO, k])

    def c_fwd(k):
        (a0, an), (b0, bn) = halves(k)
        out = []
        if an:
            out.append(remote(seg(k, r, cx, a0, an), seg(k, r, cx, a0, an), ss.at[GY, k], rs.at[DY, k], to_y))
        if bn:
            out.append(remote(seg(k, ry, c, b0, bn), seg(k, ry, c, b0, bn), ss.at[GX, k], rs.at[DX, k], to_x))
        return out

    def c_sib(k):
        return [
            remote(seg(k, r, cx), seg(k, r, cx), ss.at[HX, k], rs.at[SX, k], to_s),
            remote(seg(k, ry, c), seg(k, ry, c), ss.at[HY, k], rs.at[SY, k], to_s),
        ]

    def c_dia(k):
        (a0, an), (b0, bn) = halves(k)
        out = []
        if an:
            out.append(remote(seg(k, ry, cx, a0, an), seg(k, ry, cx, a0, an), ss.at[HD, k], rs.at[SD, k], to_s))
        if bn:
            out.append(remote(seg(k, ry, cx, b0, bn), seg(k, ry, cx, b0, bn), ss.at[HE, k], rs.at[SE, k], to_s))
        return out

    def arrive(dst, sem):
        pltpu.make_async_copy(dst, dst, sem).wait()

    def wait_first(k):
        arrive(seg(k, r, cx), rs.at[FX, k])
        arrive(seg(k, ry, c), rs.at[FY, k])

    def wait_dia(k):
        (a0, an), (b0, bn) = halves(k)
        if an:
            arrive(seg(k, ry, cx, a0, an), rs.at[DY, k])
        if bn:
            arrive(seg(k, ry, cx, b0, bn), rs.at[DX, k])

    def wait_sib(k):
        arrive(seg(k, r, cs), rs.at[SO, k])
        arrive(seg(k, r, csx), rs.at[SX, k])
        arrive(seg(k, ry, cs), rs.at[SY, k])
        (a0, an), (b0, bn) = halves(k)
        if an:
            arrive(seg(k, ry, csx, a0, an), rs.at[SD, k])
        if bn:
            arrive(seg(k, ry, csx, b0, bn), rs.at[SE, k])

    def start_own(k):
        c_loc(k).wait()
        for cp in c_own(k):
            cp.start()

    for k in range(1, STEPS + 1):
        c_loc(k).start()
    barrier = pltpu.get_barrier_semaphore()
    for dev in (to_x, to_y, to_s):
        pl.semaphore_signal(barrier, inc=1, device_id=dev, device_id_type=MESH)
    pl.semaphore_wait(barrier, 3)

    t_copies = [
        remote(tp_ref, tl.at[:, c], ts.at[0], ts.at[1], to_x),
        remote(tp_ref, tl.at[:, c], ts.at[2], ts.at[3], to_s),
    ]
    t_on = remote(tl.at[:, cx], tl.at[:, cx], ts.at[4], ts.at[5], to_s)
    t_loc = pltpu.make_async_copy(tp_ref, tl.at[:, c], ts.at[6])
    z_loc = pltpu.make_async_copy(z_ref, xt, zs.at[0])

    x_copy = remote(xs, xn, os.at[0], os.at[1], to_y)

    def y_copy(i):
        return remote(yo.at[i], yn.at[i], ys.at[0, i], ys.at[1, i], to_y)

    def do(ops):
        for op, k in ops:
            if op == O:
                start_own(k)
            elif op == F:
                wait_first(k)
                for cp in c_fwd(k) + c_sib(k):
                    cp.start()
                if k == 1:
                    arrive(tl.at[:, cx], ts.at[1])
                    t_on.start()
            elif op == D:
                wait_dia(k)
                for cp in c_dia(k):
                    cp.start()
            elif op == S:
                wait_sib(k)
                if k == 1:
                    arrive(tl.at[:, cs], ts.at[3])
                    arrive(tl.at[:, csx], ts.at[5])
                    t_loc.wait()
                    z_loc.wait()
                if k > SWAP + 1:
                    y_copy(k - SWAP - 2).start()
            elif op == T:
                for cp in t_copies:
                    cp.start()
                t_loc.start()
                z_loc.start()
            else:
                x_copy.start()

    def point(k, table):
        for kk, ops in table.items():
            @pl.when(k == kk)
            def _(ops=ops):
                do(ops)

    lane = lax.broadcasted_iota(jnp.int32, (128, 128), 1)
    sub = lax.broadcasted_iota(jnp.int32, (128, 128), 0)
    pr, pc = sub // 32, lane // 32
    level1 = (pr // 2 == pc // 2) & (pr < pc)
    level2 = pr // 2 < pc // 2

    def step(k, carry):
        point(k, BEFORE)
        J = STEPS - k
        base = 4 * k * (k - 1)
        acc[...] = jnp.zeros_like(acc)

        def tile(m, carry):
            v = jnp.concatenate([rows(k, base, 0, m), rows(k, base, 1, m)], axis=1)
            x = jnp.concatenate([xt[0, J + m], xt[1, J + m]], axis=1)
            vs = split3(v)
            for i in range(3):
                vp[i, m] = vs[i]
            lhs = [jnp.concatenate([a, b], axis=0) for a, b in zip(split3(x), vs)]
            acc[...] += mul6(lhs, vs, NT)
            return carry

        mid = lax.div(k + 1, 2)
        lax.fori_loop(0, mid, tile, 0)
        point(k, MIDDLE)
        lax.fori_loop(mid, k, tile, 0)

        q, h = J // 2, lax.rem(J, 2)

        def diag(tt):
            rows = []
            for cc in range(4):
                t32 = tl[q, cc]
                t32 = jnp.where(h == 0, t32, pltpu.roll(t32, 64, 1))
                shift = (32 * cc - 32 * tt) % 128
                rows.append(pltpu.roll(t32, shift, 1) if shift else t32)
            full = jnp.concatenate(rows, axis=0)
            return jnp.where(pr == pc, full, 0.0)

        halves_t = []
        for tt in range(2):
            g = acc[128 + 128 * tt : 256 + 128 * tt, 128 * tt : 128 * tt + 128]
            t = diag(tt)
            t = t - mulf(t, mulf(jnp.where(level1, g, 0.0), t))
            t = t - mulf(t, mulf(jnp.where(level2, g, 0.0), t))
            halves_t.append(t)
        t1, t2 = halves_t
        t12 = -mulf(t1, mulf(acc[128:256, 128:256], t2))
        w1, w2 = acc[0:128, 0:128], acc[0:128, 128:256]
        w2s = split3(w2)
        y1 = mul6(split3(w1), split3(t1), NT) + mul6(w2s, split3(t12), NT)
        y2 = mul6(w2s, split3(t2), NT)
        y = jnp.concatenate([y1, y2], axis=1)
        for i, part in enumerate(split3(y)):
            yp[i] = part

        @pl.when(k > SWAP)
        def _():
            yo[k - SWAP - 1] = y

        point(k, AFTER)

        def update(m, carry):
            d = mul6([yp[i] for i in range(3)], [vp[i, m] for i in range(3)], NN)
            xt[0, J + m] = xt[0, J + m] - d[:, :128]
            xt[1, J + m] = xt[1, J + m] - d[:, 128:]
            return carry

        @pl.when(k < STEPS)
        def _():
            lax.fori_loop(0, k, update, 0)

        @pl.when(k == SWAP)
        def _():
            def stage(m, carry):
                xs[m] = xt[ry, m]
                return carry

            lax.fori_loop(0, STEPS, stage, 0)

        return carry

    lax.fori_loop(1, STEPS + 1, step, 0)

    def half(dst, k, parts, lo, hi):
        def tile(m, carry):
            v = split3(rows(k, 8 * OFF[k], r, m))
            dst[STEPS - k + m] = dst[STEPS - k + m] - mul6(parts, v, NN)
            return carry

        lax.fori_loop(lo, hi, tile, 0)

    last = [yp[i] for i in range(3)]
    half(xt.at[r], STEPS, last, 0, 4)
    y_copy(REST - 1).start()
    half(xt.at[r], STEPS, last, 4, STEPS)
    o_loc = pltpu.make_async_copy(xt.at[r], out_ref.at[r], os.at[2])
    o_loc.start()
    arrive(xn, os.at[1])
    for i in range(REST):
        arrive(yn.at[i], ys.at[1, i])
        half(xn, SWAP + 1 + i, split3(yn[i]), 0, SWAP + 1 + i)
    o_nbr = pltpu.make_async_copy(xn, out_ref.at[ry], os.at[3])
    o_nbr.start()

    for cp in t_copies:
        cp.wait_send()
    t_on.wait_send()
    for k in range(1, STEPS + 1):
        for cp in c_own(k) + c_fwd(k) + c_sib(k) + c_dia(k):
            cp.wait_send()
    x_copy.wait_send()
    for i in range(REST):
        y_copy(i).wait_send()
    o_loc.wait()
    o_nbr.wait()


def solution(mesh):
    def body(v_loc, t_loc, z_loc):
        vt = jnp.transpose(v_loc.reshape(16, 128, 1024), (0, 2, 1)).reshape(16, 16, 64, 128)
        tp = jnp.transpose(t_loc.reshape(8, 4, 32, 32), (0, 2, 1, 3)).reshape(8, 32, 128)
        zt = jnp.transpose(z_loc.reshape(2, 16, 128, 128), (0, 1, 3, 2))
        out = pl.pallas_call(
            kernel,
            out_shape=jax.ShapeDtypeStruct((2, 16, 128, 128), F32),
            in_specs=[pl.BlockSpec(memory_space=pl.ANY)] * 3,
            out_specs=pl.BlockSpec(memory_space=pl.ANY),
            scratch_shapes=[
                pltpu.VMEM((8 * OFF[STEPS + 1], 64, 128), F32),
                pltpu.VMEM((8, 4, 32, 128), F32),
                pltpu.VMEM((2, 16, 128, 128), F32),
                pltpu.VMEM((16, 128, 128), F32),
                pltpu.VMEM((16, 128, 128), F32),
                pltpu.VMEM((REST, 128, 256), F32),
                pltpu.VMEM((REST, 128, 256), F32),
                pltpu.VMEM((3, 16, 256, 256), BF16),
                pltpu.VMEM((384, 256), F32),
                pltpu.VMEM((3, 128, 256), BF16),
                pltpu.SemaphoreType.DMA((10, STEPS + 1)),
                pltpu.SemaphoreType.DMA((9, STEPS + 1)),
                pltpu.SemaphoreType.DMA((7,)),
                pltpu.SemaphoreType.DMA((1,)),
                pltpu.SemaphoreType.DMA((4,)),
                pltpu.SemaphoreType.DMA((2, REST)),
            ],
            compiler_params=pltpu.CompilerParams(
                collective_id=0, has_side_effects=True, vmem_limit_bytes=64 * 1024 * 1024 - 65536
            ),
        )(vt, tp, zt)
        return jnp.transpose(out, (1, 3, 0, 2)).reshape(2048, 256)

    return jax.shard_map(
        body,
        mesh=mesh,
        in_specs=(P("row", "col"), P("col", None, None), P(None, ("col", "row"))),
        out_specs=P("row", "col"),
        check_vma=False,
    )
```

```python
import functools

import jax
import jax.numpy as jnp
from jax import lax
from jax.experimental import pallas as pl
from jax.experimental.pallas import tpu as pltpu
from jax.sharding import PartitionSpec as P

MESH = pl.DeviceIdType.MESH
F32, BF16 = jnp.float32, jnp.bfloat16
STEPS = 16
OFF = [k * (k - 1) // 2 for k in range(STEPS + 2)]
NT = (((1,), (1,)), ((), ()))
NN = (((1,), (0,)), ((), ()))
SWAP = 13
REST = STEPS - SWAP
O, F, D, S, T, X = range(6)
BEFORE = {
    1: ((O, 1), (T, 0), (O, 2), (F, 1), (O, 3), (F, 2), (O, 4), (D, 1), (S, 1)),
    2: ((S, 2),),
    3: ((F, 5), (D, 3), (D, 4), (S, 3)),
    4: ((S, 4),),
    5: ((D, 5), (S, 5), (O, 8)),
    6: ((D, 6), (S, 6), (O, 9)),
    7: ((D, 7), (S, 7)),
}
BEFORE |= {k: ((F, k + 1), (D, k), (S, k)) for k in range(8, 16)}
BEFORE[16] = ((D, 16), (S, 16))
MIDDLE = {1: ((O, 5),), 2: ((F, 4), (O, 6)), 3: ((O, 7),)}
MIDDLE |= {k: ((O, k + 3),) for k in range(7, 14)}
MIDDLE[14] = ((X, 0),)
AFTER = {1: ((F, 3), (D, 2)), 4: ((F, 6),), 5: ((F, 7),), 6: ((F, 8),)}
ALONG_Y = [0, 0, 1, 1, 2, 2, 3, 3, 4, 4, 5, 5, 6, 6, 7, 0, 0]
FX, FY, DX, DY, SO, SX, SY, SD, SE, LO = range(10)
TX, TY, TS, GX, GY, HX, HY, HD, HE = range(9)


def split3(a):
    p1 = a.astype(BF16)
    rest = a - p1.astype(F32)
    p2 = rest.astype(BF16)
    p3 = (rest - p2.astype(F32)).astype(BF16)
    return p1, p2, p3


def mul6(a, b, dims):
    dot = functools.partial(lax.dot_general, dimension_numbers=dims, preferred_element_type=F32)
    return (
        dot(a[0], b[0]) + dot(a[1], b[0]) + dot(a[2], b[0]) + dot(a[0], b[1]) + dot(a[1], b[1]) + dot(a[0], b[2])
    )


def mulf(a, b, dims=NN):
    return mul6(split3(a), split3(b), dims)


def kernel(vt_ref, tp_ref, z_ref, out_ref, land, tl, xt, xs, xn, yo, yn, vp, acc, yp, rs, ss, ts, zs, os, ys):
    r, c = lax.axis_index("row"), lax.axis_index("col")
    cs = c + 1 - 2 * lax.rem(c, 2)
    cx = lax.rem(c + 2, 4)
    csx = lax.rem(cs + 2, 4)
    ry = 1 - r
    to_x, to_y, to_s = (r, cx), (ry, c), (r, cs)

    def seg(k, rr, cc, lo=0, n=None):
        return land.at[pl.ds(8 * OFF[k] + (rr * 4 + cc) * k + lo, k if n is None else n)]

    def rows(k, base, rr, m):
        got = [land[base + (rr * 4 + cc) * k + m] for cc in range(4)]
        return jnp.concatenate([g[:32] for g in got] + [g[32:] for g in got], axis=0)

    def remote(src, dst, send, recv, dev):
        return pltpu.make_async_remote_copy(
            src_ref=src, dst_ref=dst, send_sem=send, recv_sem=recv, device_id=dev, device_id_type=MESH
        )

    def own(k):
        return vt_ref.at[pl.ds(STEPS - k, k), STEPS - k]

    def halves(k):
        h = ALONG_Y[k]
        return (0, h), (h, k - h)

    def c_own(k):
        mine = seg(k, r, c)
        return [
            remote(mine, mine, ss.at[TX, k], rs.at[FX, k], to_x),
            remote(mine, mine, ss.at[TY, k], rs.at[FY, k], to_y),
            remote(mine, mine, ss.at[TS, k], rs.at[SO, k], to_s),
        ]

    def c_own_start(k):
        if k < 2:
            return c_own(k)
        h = k // 2
        a, b = seg(k, r, c, 0, h), seg(k, r, c, h, k - h)
        return [
            remote(a, a, ss.at[TX, k], rs.at[FX, k], to_x),
            remote(a, a, ss.at[TY, k], rs.at[FY, k], to_y),
            remote(b, b, ss.at[TX, k], rs.at[FX, k], to_x),
            remote(b, b, ss.at[TY, k], rs.at[FY, k], to_y),
            c_own(k)[2],
        ]

    def c_loc(k):
        return pltpu.make_async_copy(own(k), seg(k, r, c), rs.at[LO, k])

    def c_fwd(k):
        (a0, an), (b0, bn) = halves(k)
        out = []
        if an:
            out.append(remote(seg(k, r, cx, a0, an), seg(k, r, cx, a0, an), ss.at[GY, k], rs.at[DY, k], to_y))
        if bn:
            out.append(remote(seg(k, ry, c, b0, bn), seg(k, ry, c, b0, bn), ss.at[GX, k], rs.at[DX, k], to_x))
        return out

    def c_sib(k):
        return [
            remote(seg(k, r, cx), seg(k, r, cx), ss.at[HX, k], rs.at[SX, k], to_s),
            remote(seg(k, ry, c), seg(k, ry, c), ss.at[HY, k], rs.at[SY, k], to_s),
        ]

    def c_dia(k):
        (a0, an), (b0, bn) = halves(k)
        out = []
        if an:
            out.append(remote(seg(k, ry, cx, a0, an), seg(k, ry, cx, a0, an), ss.at[HD, k], rs.at[SD, k], to_s))
        if bn:
            out.append(remote(seg(k, ry, cx, b0, bn), seg(k, ry, cx, b0, bn), ss.at[HE, k], rs.at[SE, k], to_s))
        return out

    def arrive(dst, sem):
        pltpu.make_async_copy(dst, dst, sem).wait()

    def wait_first(k):
        arrive(seg(k, r, cx), rs.at[FX, k])
        arrive(seg(k, ry, c), rs.at[FY, k])

    def wait_dia(k):
        (a0, an), (b0, bn) = halves(k)
        if an:
            arrive(seg(k, ry, cx, a0, an), rs.at[DY, k])
        if bn:
            arrive(seg(k, ry, cx, b0, bn), rs.at[DX, k])

    def wait_sib(k):
        arrive(seg(k, r, cs), rs.at[SO, k])
        arrive(seg(k, r, csx), rs.at[SX, k])
        arrive(seg(k, ry, cs), rs.at[SY, k])
        (a0, an), (b0, bn) = halves(k)
        if an:
            arrive(seg(k, ry, csx, a0, an), rs.at[SD, k])
        if bn:
            arrive(seg(k, ry, csx, b0, bn), rs.at[SE, k])

    def start_own(k):
        c_loc(k).wait()
        for cp in c_own_start(k):
            cp.start()

    for k in range(1, STEPS + 1):
        c_loc(k).start()
    barrier = pltpu.get_barrier_semaphore()
    for dev in (to_x, to_y, to_s):
        pl.semaphore_signal(barrier, inc=1, device_id=dev, device_id_type=MESH)
    pl.semaphore_wait(barrier, 3)

    t_copies = [
        remote(tp_ref, tl.at[:, c], ts.at[0], ts.at[1], to_x),
        remote(tp_ref, tl.at[:, c], ts.at[2], ts.at[3], to_s),
    ]
    t_on = remote(tl.at[:, cx], tl.at[:, cx], ts.at[4], ts.at[5], to_s)
    t_loc = pltpu.make_async_copy(tp_ref, tl.at[:, c], ts.at[6])
    z_loc = pltpu.make_async_copy(z_ref, xt, zs.at[0])

    x_copy = remote(xs, xn, os.at[0], os.at[1], to_y)

    def y_copy(i):
        return remote(yo.at[i], yn.at[i], ys.at[0, i], ys.at[1, i], to_y)

    def do(ops):
        for op, k in ops:
            if op == O:
                start_own(k)
            elif op == F:
                wait_first(k)
                for cp in c_fwd(k) + c_sib(k):
                    cp.start()
                if k == 1:
                    arrive(tl.at[:, cx], ts.at[1])
                    t_on.start()
            elif op == D:
                wait_dia(k)
                for cp in c_dia(k):
                    cp.start()
            elif op == S:
                wait_sib(k)
                if k == 1:
                    arrive(tl.at[:, cs], ts.at[3])
                    arrive(tl.at[:, csx], ts.at[5])
                    t_loc.wait()
                    z_loc.wait()
                if k > SWAP + 1:
                    y_copy(k - SWAP - 2).start()
            elif op == T:
                for cp in t_copies:
                    cp.start()
                t_loc.start()
                z_loc.start()
            else:
                x_copy.start()

    def point(k, table):
        for kk, ops in table.items():
            @pl.when(k == kk)
            def _(ops=ops):
                do(ops)

    lane = lax.broadcasted_iota(jnp.int32, (128, 128), 1)
    sub = lax.broadcasted_iota(jnp.int32, (128, 128), 0)
    pr, pc = sub // 32, lane // 32
    level1 = (pr // 2 == pc // 2) & (pr < pc)
    level2 = pr // 2 < pc // 2

    def step(k, carry):
        point(k, BEFORE)
        J = STEPS - k
        base = 4 * k * (k - 1)
        acc[...] = jnp.zeros_like(acc)

        def tile(m, carry):
            v = jnp.concatenate([rows(k, base, 0, m), rows(k, base, 1, m)], axis=1)
            x = jnp.concatenate([xt[0, J + m], xt[1, J + m]], axis=1)
            vs = split3(v)
            for i in range(3):
                vp[i, m] = vs[i]
            lhs = [jnp.concatenate([a, b], axis=0) for a, b in zip(split3(x), vs)]
            acc[...] += mul6(lhs, vs, NT)
            return carry

        mid = lax.div(k + 1, 2)
        lax.fori_loop(0, mid, tile, 0)
        point(k, MIDDLE)
        lax.fori_loop(mid, k, tile, 0)

        q, h = J // 2, lax.rem(J, 2)

        def diag(tt):
            rows = []
            for cc in range(4):
                t32 = tl[q, cc]
                t32 = jnp.where(h == 0, t32, pltpu.roll(t32, 64, 1))
                shift = (32 * cc - 32 * tt) % 128
                rows.append(pltpu.roll(t32, shift, 1) if shift else t32)
            full = jnp.concatenate(rows, axis=0)
            return jnp.where(pr == pc, full, 0.0)

        halves_t = []
        for tt in range(2):
            g = acc[128 + 128 * tt : 256 + 128 * tt, 128 * tt : 128 * tt + 128]
            t = diag(tt)
            t = t - mulf(t, mulf(jnp.where(level1, g, 0.0), t))
            t = t - mulf(t, mulf(jnp.where(level2, g, 0.0), t))
            halves_t.append(t)
        t1, t2 = halves_t
        t12 = -mulf(t1, mulf(acc[128:256, 128:256], t2))
        w1, w2 = acc[0:128, 0:128], acc[0:128, 128:256]
        w2s = split3(w2)
        y1 = mul6(split3(w1), split3(t1), NT) + mul6(w2s, split3(t12), NT)
        y2 = mul6(w2s, split3(t2), NT)
        y = jnp.concatenate([y1, y2], axis=1)
        for i, part in enumerate(split3(y)):
            yp[i] = part

        @pl.when(k > SWAP)
        def _():
            yo[k - SWAP - 1] = y

        point(k, AFTER)

        def update(m, carry):
            d = mul6([yp[i] for i in range(3)], [vp[i, m] for i in range(3)], NN)
            xt[0, J + m] = xt[0, J + m] - d[:, :128]
            xt[1, J + m] = xt[1, J + m] - d[:, 128:]
            return carry

        @pl.when(k < STEPS)
        def _():
            lax.fori_loop(0, k, update, 0)

        @pl.when(k == SWAP)
        def _():
            def stage(m, carry):
                xs[m] = xt[ry, m]
                return carry

            lax.fori_loop(0, STEPS, stage, 0)

        return carry

    lax.fori_loop(1, STEPS + 1, step, 0)

    def half(dst, k, parts, lo, hi):
        def tile(m, carry):
            v = split3(rows(k, 8 * OFF[k], r, m))
            dst[STEPS - k + m] = dst[STEPS - k + m] - mul6(parts, v, NN)
            return carry

        lax.fori_loop(lo, hi, tile, 0)

    last = [yp[i] for i in range(3)]
    half(xt.at[r], STEPS, last, 0, 4)
    y_copy(REST - 1).start()
    half(xt.at[r], STEPS, last, 4, STEPS)
    o_loc = pltpu.make_async_copy(xt.at[r], out_ref.at[r], os.at[2])
    o_loc.start()
    arrive(xn, os.at[1])
    for i in range(REST):
        arrive(yn.at[i], ys.at[1, i])
        half(xn, SWAP + 1 + i, split3(yn[i]), 0, SWAP + 1 + i)
    o_nbr = pltpu.make_async_copy(xn, out_ref.at[ry], os.at[3])
    o_nbr.start()

    for cp in t_copies:
        cp.wait_send()
    t_on.wait_send()
    for k in range(1, STEPS + 1):
        for cp in c_own(k) + c_fwd(k) + c_sib(k) + c_dia(k):
            cp.wait_send()
    x_copy.wait_send()
    for i in range(REST):
        y_copy(i).wait_send()
    o_loc.wait()
    o_nbr.wait()


def solution(mesh):
    def body(v_loc, t_loc, z_loc):
        vt = jnp.transpose(v_loc.reshape(16, 128, 1024), (0, 2, 1)).reshape(16, 16, 64, 128)
        tp = jnp.transpose(t_loc.reshape(8, 4, 32, 32), (0, 2, 1, 3)).reshape(8, 32, 128)
        zt = jnp.transpose(z_loc.reshape(2, 16, 128, 128), (0, 1, 3, 2))
        out = pl.pallas_call(
            kernel,
            out_shape=jax.ShapeDtypeStruct((2, 16, 128, 128), F32),
            in_specs=[pl.BlockSpec(memory_space=pl.ANY)] * 3,
            out_specs=pl.BlockSpec(memory_space=pl.ANY),
            scratch_shapes=[
                pltpu.VMEM((8 * OFF[STEPS + 1], 64, 128), F32),
                pltpu.VMEM((8, 4, 32, 128), F32),
                pltpu.VMEM((2, 16, 128, 128), F32),
                pltpu.VMEM((16, 128, 128), F32),
                pltpu.VMEM((16, 128, 128), F32),
                pltpu.VMEM((REST, 128, 256), F32),
                pltpu.VMEM((REST, 128, 256), F32),
                pltpu.VMEM((3, 16, 256, 256), BF16),
                pltpu.VMEM((384, 256), F32),
                pltpu.VMEM((3, 128, 256), BF16),
                pltpu.SemaphoreType.DMA((10, STEPS + 1)),
                pltpu.SemaphoreType.DMA((9, STEPS + 1)),
                pltpu.SemaphoreType.DMA((7,)),
                pltpu.SemaphoreType.DMA((1,)),
                pltpu.SemaphoreType.DMA((4,)),
                pltpu.SemaphoreType.DMA((2, REST)),
            ],
            compiler_params=pltpu.CompilerParams(
                collective_id=0, has_side_effects=True, vmem_limit_bytes=64 * 1024 * 1024 - 65536
            ),
        )(vt, tp, zt)
        return jnp.transpose(out, (1, 3, 0, 2)).reshape(2048, 256)

    return jax.shard_map(
        body,
        mesh=mesh,
        in_specs=(P("row", "col"), P("col", None, None), P(None, ("col", "row"))),
        out_specs=P("row", "col"),
        check_vma=False,
    )
```

```python
import functools

import jax
import jax.numpy as jnp
from jax import lax
from jax.experimental import pallas as pl
from jax.experimental.pallas import tpu as pltpu
from jax.sharding import PartitionSpec as P

MESH = pl.DeviceIdType.MESH
F32, BF16 = jnp.float32, jnp.bfloat16
STEPS = 16
OFF = [k * (k - 1) // 2 for k in range(STEPS + 2)]
NT = (((1,), (1,)), ((), ()))
NN = (((1,), (0,)), ((), ()))
SWAP = 13
REST = STEPS - SWAP
O, F, D, S, T, X = range(6)
BEFORE = {k: ((S, k),) for k in range(2, STEPS + 1)}
BEFORE[1] = ((O, 1), (O, 2), (T, 0), (O, 3), (F, 1), (O, 4), (F, 2), (D, 1), (S, 1))
MIDDLE = {k: ((F, k + 2), (O, k + 4)) for k in range(1, 13)}
MIDDLE[13] = ((F, 15),)
MIDDLE[14] = ((X, 0), (F, 16))
AFTER = {k: ((D, k + 1),) for k in range(1, 16)}
ALONG_Y = [0, 0, 1, 1, 2, 2, 3, 3, 4, 4, 5, 5, 6, 6, 7, 0, 0]
FX, FY, DX, DY, SO, SX, SY, SD, SE, LO = range(10)
TX, TY, TS, GX, GY, HX, HY, HD, HE = range(9)


def split3(a):
    p1 = a.astype(BF16)
    rest = a - p1.astype(F32)
    p2 = rest.astype(BF16)
    p3 = (rest - p2.astype(F32)).astype(BF16)
    return p1, p2, p3


def mul6(a, b, dims):
    dot = functools.partial(lax.dot_general, dimension_numbers=dims, preferred_element_type=F32)
    return (
        dot(a[0], b[0]) + dot(a[1], b[0]) + dot(a[2], b[0]) + dot(a[0], b[1]) + dot(a[1], b[1]) + dot(a[0], b[2])
    )


def mulf(a, b, dims=NN):
    return mul6(split3(a), split3(b), dims)


def by_four(lo, hi, fn):
    fours = lax.div(hi - lo, 4)

    def four(i, carry):
        fn(lo + 4 * i, 4)
        return carry

    def one(m, carry):
        fn(m, 1)
        return carry

    lax.fori_loop(0, fours, four, 0)
    lax.fori_loop(lo + 4 * fours, hi, one, 0)


def kernel(vt_ref, tp_ref, z_ref, out_ref, land, tl, xt, xs, xn, yo, yn, vp, lp, acc, yp, rs, ss, ts, zs, os, ys):
    r, c = lax.axis_index("row"), lax.axis_index("col")
    cs = c + 1 - 2 * lax.rem(c, 2)
    cx = lax.rem(c + 2, 4)
    csx = lax.rem(cs + 2, 4)
    ry = 1 - r
    to_x, to_y, to_s = (r, cx), (ry, c), (r, cs)

    def seg(k, rr, cc, lo=0, n=None):
        return land.at[pl.ds(8 * OFF[k] + (rr * 4 + cc) * k + lo, k if n is None else n)]

    def rows(k, base, rr, m):
        got = [land[base + (rr * 4 + cc) * k + m] for cc in range(4)]
        return jnp.concatenate([g[:32] for g in got] + [g[32:] for g in got], axis=0)

    def remote(src, dst, send, recv, dev):
        return pltpu.make_async_remote_copy(
            src_ref=src, dst_ref=dst, send_sem=send, recv_sem=recv, device_id=dev, device_id_type=MESH
        )

    def own(k):
        return vt_ref.at[pl.ds(STEPS - k, k), STEPS - k]

    def halves(k):
        h = ALONG_Y[k]
        return (0, h), (h, k - h)

    def c_own(k):
        mine = seg(k, r, c)
        return [
            remote(mine, mine, ss.at[TX, k], rs.at[FX, k], to_x),
            remote(mine, mine, ss.at[TY, k], rs.at[FY, k], to_y),
            remote(mine, mine, ss.at[TS, k], rs.at[SO, k], to_s),
        ]

    def c_loc(k):
        return pltpu.make_async_copy(own(k), seg(k, r, c), rs.at[LO, k])

    def c_fwd(k):
        (a0, an), (b0, bn) = halves(k)
        out = []
        if an:
            out.append(remote(seg(k, r, cx, a0, an), seg(k, r, cx, a0, an), ss.at[GY, k], rs.at[DY, k], to_y))
        if bn:
            out.append(remote(seg(k, ry, c, b0, bn), seg(k, ry, c, b0, bn), ss.at[GX, k], rs.at[DX, k], to_x))
        return out

    def c_sib(k):
        return [
            remote(seg(k, r, cx), seg(k, r, cx), ss.at[HX, k], rs.at[SX, k], to_s),
            remote(seg(k, ry, c), seg(k, ry, c), ss.at[HY, k], rs.at[SY, k], to_s),
        ]

    def c_dia(k):
        (a0, an), (b0, bn) = halves(k)
        out = []
        if an:
            out.append(remote(seg(k, ry, cx, a0, an), seg(k, ry, cx, a0, an), ss.at[HD, k], rs.at[SD, k], to_s))
        if bn:
            out.append(remote(seg(k, ry, cx, b0, bn), seg(k, ry, cx, b0, bn), ss.at[HE, k], rs.at[SE, k], to_s))
        return out

    def arrive(dst, sem):
        pltpu.make_async_copy(dst, dst, sem).wait()

    def wait_first(k):
        arrive(seg(k, r, cx), rs.at[FX, k])
        arrive(seg(k, ry, c), rs.at[FY, k])

    def wait_dia(k):
        (a0, an), (b0, bn) = halves(k)
        if an:
            arrive(seg(k, ry, cx, a0, an), rs.at[DY, k])
        if bn:
            arrive(seg(k, ry, cx, b0, bn), rs.at[DX, k])

    def wait_sib(k):
        arrive(seg(k, r, cs), rs.at[SO, k])
        arrive(seg(k, r, csx), rs.at[SX, k])
        arrive(seg(k, ry, cs), rs.at[SY, k])
        (a0, an), (b0, bn) = halves(k)
        if an:
            arrive(seg(k, ry, csx, a0, an), rs.at[SD, k])
        if bn:
            arrive(seg(k, ry, csx, b0, bn), rs.at[SE, k])

    def start_own(k):
        c_loc(k).wait()
        for cp in c_own(k):
            cp.start()

    for k in range(1, STEPS + 1):
        c_loc(k).start()
    barrier = pltpu.get_barrier_semaphore()
    for dev in (to_x, to_y, to_s):
        pl.semaphore_signal(barrier, inc=1, device_id=dev, device_id_type=MESH)
    pl.semaphore_wait(barrier, 3)

    t_copies = [
        remote(tp_ref, tl.at[:, c], ts.at[0], ts.at[1], to_x),
        remote(tp_ref, tl.at[:, c], ts.at[2], ts.at[3], to_s),
    ]
    t_on = remote(tl.at[:, cx], tl.at[:, cx], ts.at[4], ts.at[5], to_s)
    t_loc = pltpu.make_async_copy(tp_ref, tl.at[:, c], ts.at[6])
    z_loc = pltpu.make_async_copy(z_ref, xt, zs.at[0])

    x_copy = remote(xs, xn, os.at[0], os.at[1], to_y)

    def y_copy(i):
        return remote(yo.at[i], yn.at[i], ys.at[0, i], ys.at[1, i], to_y)

    def do(ops):
        for op, k in ops:
            if op == O:
                start_own(k)
            elif op == F:
                wait_first(k)
                for cp in c_fwd(k) + c_sib(k):
                    cp.start()
                if k == 1:
                    arrive(tl.at[:, cx], ts.at[1])
                    t_on.start()
            elif op == D:
                wait_dia(k)
                for cp in c_dia(k):
                    cp.start()
            elif op == S:
                wait_sib(k)
                if k == 1:
                    arrive(tl.at[:, cs], ts.at[3])
                    arrive(tl.at[:, csx], ts.at[5])
                    t_loc.wait()
                    z_loc.wait()
                if k > SWAP + 1:
                    y_copy(k - SWAP - 2).start()
            elif op == T:
                for cp in t_copies:
                    cp.start()
                t_loc.start()
                z_loc.start()
            else:
                x_copy.start()

    def point(k, table):
        for kk, ops in table.items():
            @pl.when(k == kk)
            def _(ops=ops):
                do(ops)

    lane = lax.broadcasted_iota(jnp.int32, (128, 128), 1)
    sub = lax.broadcasted_iota(jnp.int32, (128, 128), 0)
    pr, pc = sub // 32, lane // 32
    level1 = (pr // 2 == pc // 2) & (pr < pc)
    level2 = pr // 2 < pc // 2

    def step(k, carry):
        point(k, BEFORE)
        J = STEPS - k
        base = 4 * k * (k - 1)
        acc[...] = jnp.zeros_like(acc)

        def prepare(m, p):
            m = jnp.minimum(m, k - 1)
            for g in range(12):
                if g < 4:
                    here = [xt[rr, J + m, 32 * g : 32 * g + 32] for rr in range(2)]
                else:
                    tt, cc = divmod(g - 4, 4)
                    here = [land[base + (rr * 4 + cc) * k + m, 32 * tt : 32 * tt + 32] for rr in range(2)]
                for i, part in enumerate(split3(jnp.concatenate(here, axis=1))):
                    lp[p, i, 32 * g : 32 * g + 32] = part
                    if g >= 4:
                        vp[i, m, 32 * g - 128 : 32 * g - 96] = part

        def product(p):
            return mul6([lp[p, i] for i in range(3)], [lp[p, i, 128:384] for i in range(3)], NT)

        def pair(i, carry):
            acc[...] += product(0) + product(1)
            prepare(2 * i + 2, 0)
            prepare(2 * i + 3, 1)
            return carry

        pairs = lax.div(k, 2)
        mid = lax.div(pairs + 1, 2)
        prepare(0, 0)
        prepare(1, 1)
        lax.fori_loop(0, mid, pair, 0)
        point(k, MIDDLE)
        lax.fori_loop(mid, pairs, pair, 0)

        @pl.when(lax.rem(k, 2) == 1)
        def _():
            acc[...] += product(0)

        q, h = J // 2, lax.rem(J, 2)

        def diag(tt):
            rows = []
            for cc in range(4):
                t32 = tl[q, cc]
                t32 = jnp.where(h == 0, t32, pltpu.roll(t32, 64, 1))
                shift = (32 * cc - 32 * tt) % 128
                rows.append(pltpu.roll(t32, shift, 1) if shift else t32)
            full = jnp.concatenate(rows, axis=0)
            return jnp.where(pr == pc, full, 0.0)

        halves_t = []
        for tt in range(2):
            g = acc[128 + 128 * tt : 256 + 128 * tt, 128 * tt : 128 * tt + 128]
            t = diag(tt)
            t = t - mulf(t, mulf(jnp.where(level1, g, 0.0), t))
            t = t - mulf(t, mulf(jnp.where(level2, g, 0.0), t))
            halves_t.append(t)
        t1, t2 = halves_t
        t12 = -mulf(t1, mulf(acc[128:256, 128:256], t2))
        w1, w2 = acc[0:128, 0:128], acc[0:128, 128:256]
        w2s = split3(w2)
        y1 = mul6(split3(w1), split3(t1), NT) + mul6(w2s, split3(t12), NT)
        y2 = mul6(w2s, split3(t2), NT)
        y = jnp.concatenate([y1, y2], axis=1)
        for i, part in enumerate(split3(y)):
            yp[i] = part

        @pl.when(k > SWAP)
        def _():
            yo[k - SWAP - 1] = y

        point(k, AFTER)

        def update(m, n):
            ps = [yp[i] for i in range(3)]
            ds = [mul6(ps, [vp[i, m + u] for i in range(3)], NN) for u in range(n)]
            for u, d in enumerate(ds):
                xt[0, J + m + u] = xt[0, J + m + u] - d[:, :128]
                xt[1, J + m + u] = xt[1, J + m + u] - d[:, 128:]

        @pl.when(k < STEPS)
        def _():
            by_four(0, k, update)

        @pl.when(k == SWAP)
        def _():
            def stage(m, carry):
                xs[m] = xt[ry, m]
                return carry

            lax.fori_loop(0, STEPS, stage, 0)

        return carry

    lax.fori_loop(1, STEPS + 1, step, 0)

    def half(dst, k, parts, lo, hi):
        def tiles(m, n):
            ds = [mul6(parts, split3(rows(k, 8 * OFF[k], r, m + u)), NN) for u in range(n)]
            for u, d in enumerate(ds):
                dst[STEPS - k + m + u] = dst[STEPS - k + m + u] - d

        by_four(lo, hi, tiles)

    last = [yp[i] for i in range(3)]
    half(xt.at[r], STEPS, last, 0, 4)
    y_copy(REST - 1).start()
    half(xt.at[r], STEPS, last, 4, STEPS)
    o_loc = pltpu.make_async_copy(xt.at[r], out_ref.at[r], os.at[2])
    o_loc.start()
    arrive(xn, os.at[1])
    for i in range(REST):
        arrive(yn.at[i], ys.at[1, i])
        half(xn, SWAP + 1 + i, split3(yn[i]), 0, SWAP + 1 + i)
    o_nbr = pltpu.make_async_copy(xn, out_ref.at[ry], os.at[3])
    o_nbr.start()

    for cp in t_copies:
        cp.wait_send()
    t_on.wait_send()
    for k in range(1, STEPS + 1):
        for cp in c_own(k) + c_fwd(k) + c_sib(k) + c_dia(k):
            cp.wait_send()
    x_copy.wait_send()
    for i in range(REST):
        y_copy(i).wait_send()
    o_loc.wait()
    o_nbr.wait()


def solution(mesh):
    def body(v_loc, t_loc, z_loc):
        vt = jnp.transpose(v_loc.reshape(16, 128, 1024), (0, 2, 1)).reshape(16, 16, 64, 128)
        tp = jnp.transpose(t_loc.reshape(8, 4, 32, 32), (0, 2, 1, 3)).reshape(8, 32, 128)
        zt = jnp.transpose(z_loc.reshape(2, 16, 128, 128), (0, 1, 3, 2))
        out = pl.pallas_call(
            kernel,
            out_shape=jax.ShapeDtypeStruct((2, 16, 128, 128), F32),
            in_specs=[pl.BlockSpec(memory_space=pl.ANY)] * 3,
            out_specs=pl.BlockSpec(memory_space=pl.ANY),
            scratch_shapes=[
                pltpu.VMEM((8 * OFF[STEPS + 1], 64, 128), F32),
                pltpu.VMEM((8, 4, 32, 128), F32),
                pltpu.VMEM((2, 16, 128, 128), F32),
                pltpu.VMEM((16, 128, 128), F32),
                pltpu.VMEM((16, 128, 128), F32),
                pltpu.VMEM((REST, 128, 256), F32),
                pltpu.VMEM((REST, 128, 256), F32),
                pltpu.VMEM((3, 16, 256, 256), BF16),
                pltpu.VMEM((2, 3, 384, 256), BF16),
                pltpu.VMEM((384, 256), F32),
                pltpu.VMEM((3, 128, 256), BF16),
                pltpu.SemaphoreType.DMA((10, STEPS + 1)),
                pltpu.SemaphoreType.DMA((9, STEPS + 1)),
                pltpu.SemaphoreType.DMA((7,)),
                pltpu.SemaphoreType.DMA((1,)),
                pltpu.SemaphoreType.DMA((4,)),
                pltpu.SemaphoreType.DMA((2, REST)),
            ],
            compiler_params=pltpu.CompilerParams(
                collective_id=0, has_side_effects=True, vmem_limit_bytes=64 * 1024 * 1024 - 65536
            ),
        )(vt, tp, zt)
        return jnp.transpose(out, (1, 3, 0, 2)).reshape(2048, 256)

    return jax.shard_map(
        body,
        mesh=mesh,
        in_specs=(P("row", "col"), P("col", None, None), P(None, ("col", "row"))),
        out_specs=P("row", "col"),
        check_vma=False,
    )
```

```python
import functools

import jax
import jax.numpy as jnp
from jax import lax
from jax.experimental import pallas as pl
from jax.experimental.pallas import tpu as pltpu
from jax.sharding import PartitionSpec as P

MESH = pl.DeviceIdType.MESH
F32, BF16 = jnp.float32, jnp.bfloat16
STEPS = 16
OFF = [k * (k - 1) // 2 for k in range(STEPS + 2)]
NT = (((1,), (1,)), ((), ()))
NN = (((1,), (0,)), ((), ()))
SWAP = 13
REST = STEPS - SWAP
O, F, D, S, T, X, V = range(7)
BEFORE = {k: ((S, k),) for k in range(2, STEPS + 1)}
BEFORE[1] = ((V, 1), (V, 2), (O, 1), (O, 2), (V, 3), (T, 0), (O, 3), (F, 1), (O, 4), (F, 2), (D, 1), (S, 1))
BEFORE[14] = ((S, 14), (X, 0))
BEFORE[15] = ((D, 15), (S, 15))
MIDDLE = {k: ((F, k + 2), (O, k + 4)) for k in range(1, 13)}
MIDDLE |= {k: MIDDLE[k] + ((V, (k + 7) // 2),) for k in range(1, 10, 2)}
MIDDLE[13] = ((F, 15),)
MIDDLE[14] = ((F, 16),)
AFTER = {k: ((D, k + 1),) for k in (*range(1, 14), 15)}
ALONG_Y = [0, 0, 1, 1, 2, 2, 3, 3, 4, 4, 5, 5, 6, 6, 7, 7, 0]
FX, FY, DX, DY, SO, SX, SY, SD, SE, LO = range(10)
TX, TY, TS, GX, GY, HX, HY, HD, HE = range(9)


def split3(a):
    p1 = a.astype(BF16)
    rest = a - p1.astype(F32)
    p2 = rest.astype(BF16)
    p3 = (rest - p2.astype(F32)).astype(BF16)
    return p1, p2, p3


def mul6(a, b, dims):
    dot = functools.partial(lax.dot_general, dimension_numbers=dims, preferred_element_type=F32)
    return (
        dot(a[0], b[0]) + dot(a[1], b[0]) + dot(a[2], b[0]) + dot(a[0], b[1]) + dot(a[1], b[1]) + dot(a[0], b[2])
    )


def mulf(a, b, dims=NN):
    return mul6(split3(a), split3(b), dims)


def by_four(lo, hi, fn):
    fours = lax.div(hi - lo, 4)

    def four(i, carry):
        fn(lo + 4 * i, 4)
        return carry

    def one(m, carry):
        fn(m, 1)
        return carry

    lax.fori_loop(0, fours, four, 0)
    lax.fori_loop(lo + 4 * fours, hi, one, 0)


def kernel(v_ref, t_ref, z_ref, out_ref, vs_in, t_in, z_in, ob, land, tl, xt, xs, xn, yo, yn, vp, lp, acc, yp, rs, ss, ts, zs, os, ys):
    r, c = lax.axis_index("row"), lax.axis_index("col")
    cs = c + 1 - 2 * lax.rem(c, 2)
    cx = lax.rem(c + 2, 4)
    csx = lax.rem(cs + 2, 4)
    ry = 1 - r
    to_x, to_y, to_s = (r, cx), (ry, c), (r, cs)

    def seg(k, rr, cc, lo=0, n=None):
        return land.at[pl.ds(8 * OFF[k] + (rr * 4 + cc) * k + lo, k if n is None else n)]

    def rows(k, base, rr, m):
        got = [land[base + (rr * 4 + cc) * k + m] for cc in range(4)]
        return jnp.concatenate([g[:32] for g in got] + [g[32:] for g in got], axis=0)

    def remote(src, dst, send, recv, dev):
        return pltpu.make_async_remote_copy(
            src_ref=src, dst_ref=dst, send_sem=send, recv_sem=recv, device_id=dev, device_id_type=MESH
        )

    def halves(k):
        h = ALONG_Y[k]
        return (0, h), (h, k - h)

    def c_own(k):
        mine = seg(k, r, c)
        return [
            remote(mine, mine, ss.at[TX, k], rs.at[FX, k], to_x),
            remote(mine, mine, ss.at[TY, k], rs.at[FY, k], to_y),
            remote(mine, mine, ss.at[TS, k], rs.at[SO, k], to_s),
        ]

    def c_loc(n):
        q = STEPS // 2 - n
        return pltpu.make_async_copy(
            v_ref.at[pl.ds(256 * q, 256 * n), pl.ds(128 * q, 128)], vs_in.at[pl.ds(256 * OFF[n], 256 * n)], rs.at[LO, n]
        )

    def turn(n):
        c_loc(n).wait()
        even, odd = (8 * OFF[k] + (r * 4 + c) * k for k in (2 * n, 2 * n - 1))

        def tile(m, carry):
            t = vs_in[pl.ds(pl.multiple_of(256 * OFF[n] + 128 * m, 128), 128)].T
            land[even + m] = t[:64]

            @pl.when(m > 0)
            def _():
                land[odd + m - 1] = t[64:]

            return carry

        lax.fori_loop(0, 2 * n, tile, 0)

    def c_fwd(k):
        (a0, an), (b0, bn) = halves(k)
        out = []
        if an:
            out.append(remote(seg(k, r, cx, a0, an), seg(k, r, cx, a0, an), ss.at[GY, k], rs.at[DY, k], to_y))
        if bn:
            out.append(remote(seg(k, ry, c, b0, bn), seg(k, ry, c, b0, bn), ss.at[GX, k], rs.at[DX, k], to_x))
        return out

    def c_sib(k):
        return [
            remote(seg(k, r, cx), seg(k, r, cx), ss.at[HX, k], rs.at[SX, k], to_s),
            remote(seg(k, ry, c), seg(k, ry, c), ss.at[HY, k], rs.at[SY, k], to_s),
        ]

    def c_dia(k):
        (a0, an), (b0, bn) = halves(k)
        out = []
        if an:
            out.append(remote(seg(k, ry, cx, a0, an), seg(k, ry, cx, a0, an), ss.at[HD, k], rs.at[SD, k], to_s))
        if bn:
            out.append(remote(seg(k, ry, cx, b0, bn), seg(k, ry, cx, b0, bn), ss.at[HE, k], rs.at[SE, k], to_s))
        return out

    def arrive(dst, sem):
        pltpu.make_async_copy(dst, dst, sem).wait()

    def wait_first(k):
        arrive(seg(k, r, cx), rs.at[FX, k])
        arrive(seg(k, ry, c), rs.at[FY, k])

    def wait_dia(k):
        (a0, an), (b0, bn) = halves(k)
        if an:
            arrive(seg(k, ry, cx, a0, an), rs.at[DY, k])
        if bn:
            arrive(seg(k, ry, cx, b0, bn), rs.at[DX, k])

    def wait_sib(k):
        arrive(seg(k, r, cs), rs.at[SO, k])
        arrive(seg(k, r, csx), rs.at[SX, k])
        arrive(seg(k, ry, cs), rs.at[SY, k])
        (a0, an), (b0, bn) = halves(k)
        if an:
            arrive(seg(k, ry, csx, a0, an), rs.at[SD, k])
        if bn:
            arrive(seg(k, ry, csx, b0, bn), rs.at[SE, k])

    def start_own(k):
        for cp in c_own(k):
            cp.start()

    t_loc = pltpu.make_async_copy(t_ref, t_in, ts.at[6])
    z_loc = pltpu.make_async_copy(z_ref, z_in, zs.at[0])
    for n in range(1, STEPS // 2 + 1):
        c_loc(n).start()
        if n == 2:
            t_loc.start()
            z_loc.start()
    barrier = pltpu.get_barrier_semaphore()
    for dev in (to_x, to_y, to_s):
        pl.semaphore_signal(barrier, inc=1, device_id=dev, device_id_type=MESH)
    pl.semaphore_wait(barrier, 3)

    t_copies = [
        remote(tl.at[:, c], tl.at[:, c], ts.at[0], ts.at[1], to_x),
        remote(tl.at[:, c], tl.at[:, c], ts.at[2], ts.at[3], to_s),
    ]
    t_on = remote(tl.at[:, cx], tl.at[:, cx], ts.at[4], ts.at[5], to_s)

    x_copy = remote(xs, xn, os.at[0], os.at[1], to_y)

    def y_copy(i):
        return remote(yo.at[i], yn.at[i], ys.at[0, i], ys.at[1, i], to_y)

    def do(ops):
        for op, k in ops:
            if op == O:
                start_own(k)
            elif op == F:
                wait_first(k)
                for cp in c_fwd(k) + c_sib(k):
                    cp.start()
                if k == 1:
                    arrive(tl.at[:, cx], ts.at[1])
                    t_on.start()
            elif op == D:
                wait_dia(k)
                for cp in c_dia(k):
                    cp.start()
            elif op == S:
                wait_sib(k)
                if k == 1:
                    arrive(tl.at[:, cs], ts.at[3])
                    arrive(tl.at[:, csx], ts.at[5])
                    z_loc.wait()
                if k > SWAP + 1:
                    y_copy(k - SWAP - 2).start()
            elif op == T:
                for cp in t_copies:
                    cp.start()
            elif op == V:
                turn(k)
                if k == 2:
                    t_loc.wait()
                    for q in range(8):
                        tl[q, c] = jnp.concatenate([t_in[4 * q + t] for t in range(4)], axis=1)
            else:
                x_copy.start()

    def point(k, table):
        for kk, ops in table.items():
            @pl.when(k == kk)
            def _(ops=ops):
                do(ops)

    lane = lax.broadcasted_iota(jnp.int32, (128, 128), 1)
    sub = lax.broadcasted_iota(jnp.int32, (128, 128), 0)
    pr, pc = sub // 32, lane // 32
    level1 = (pr // 2 == pc // 2) & (pr < pc)
    level2 = pr // 2 < pc // 2

    def step(k, carry):
        point(k, BEFORE)
        J = STEPS - k
        base = 4 * k * (k - 1)
        acc[...] = jnp.zeros_like(acc)
        for rr in range(2):
            xt[rr, J] = z_in[pl.ds(pl.multiple_of(2048 * rr + 128 * J, 128), 128)].T

        def prepare(m, p):
            m = jnp.minimum(m, k - 1)
            for g in range(12):
                if g < 4:
                    here = [xt[rr, J + m, 32 * g : 32 * g + 32] for rr in range(2)]
                else:
                    tt, cc = divmod(g - 4, 4)
                    here = [land[base + (rr * 4 + cc) * k + m, 32 * tt : 32 * tt + 32] for rr in range(2)]
                for i, part in enumerate(split3(jnp.concatenate(here, axis=1))):
                    lp[p, i, 32 * g : 32 * g + 32] = part
                    if g >= 4:
                        vp[i, m, 32 * g - 128 : 32 * g - 96] = part

        def product(p):
            return mul6([lp[p, i] for i in range(3)], [lp[p, i, 128:384] for i in range(3)], NT)

        def pair(i, carry):
            acc[...] += product(0) + product(1)
            prepare(2 * i + 2, 0)
            prepare(2 * i + 3, 1)
            return carry

        pairs = lax.div(k, 2)
        mid = lax.div(pairs + 1, 2)
        prepare(0, 0)
        prepare(1, 1)
        lax.fori_loop(0, mid, pair, 0)
        point(k, MIDDLE)
        lax.fori_loop(mid, pairs, pair, 0)

        @pl.when(lax.rem(k, 2) == 1)
        def _():
            acc[...] += product(0)

        q, h = J // 2, lax.rem(J, 2)

        def diag(tt):
            rows = []
            for cc in range(4):
                t32 = tl[q, cc]
                t32 = jnp.where(h == 0, t32, pltpu.roll(t32, 64, 1))
                shift = (32 * cc - 32 * tt) % 128
                rows.append(pltpu.roll(t32, shift, 1) if shift else t32)
            full = jnp.concatenate(rows, axis=0)
            return jnp.where(pr == pc, full, 0.0)

        halves_t = []
        for tt in range(2):
            g = acc[128 + 128 * tt : 256 + 128 * tt, 128 * tt : 128 * tt + 128]
            t = diag(tt)
            t = t - mulf(t, mulf(jnp.where(level1, g, 0.0), t))
            t = t - mulf(t, mulf(jnp.where(level2, g, 0.0), t))
            halves_t.append(t)
        t1, t2 = halves_t
        t12 = -mulf(t1, mulf(acc[128:256, 128:256], t2))
        w1, w2 = acc[0:128, 0:128], acc[0:128, 128:256]
        w2s = split3(w2)
        y1 = mul6(split3(w1), split3(t1), NT) + mul6(w2s, split3(t12), NT)
        y2 = mul6(w2s, split3(t2), NT)
        y = jnp.concatenate([y1, y2], axis=1)
        for i, part in enumerate(split3(y)):
            yp[i] = part

        @pl.when(k > SWAP)
        def _():
            yo[k - SWAP - 1] = y

        point(k, AFTER)

        def update(m, n):
            ps = [yp[i] for i in range(3)]
            ds = [mul6(ps, [vp[i, m + u] for i in range(3)], NN) for u in range(n)]
            for u, d in enumerate(ds):
                xt[0, J + m + u] = xt[0, J + m + u] - d[:, :128]
                xt[1, J + m + u] = xt[1, J + m + u] - d[:, 128:]

        @pl.when(k < STEPS)
        def _():
            by_four(0, k, update)

        @pl.when(k == SWAP)
        def _():
            for m in range(STEPS - SWAP):
                xt[ry, m] = z_in[pl.ds(pl.multiple_of(2048 * ry + 128 * m, 128), 128)].T

            def stage(m, carry):
                xs[m] = xt[ry, m]
                return carry

            lax.fori_loop(0, STEPS, stage, 0)

        return carry

    lax.fori_loop(1, STEPS + 1, step, 0)

    def half(dst, k, parts, lo, hi, put=None):
        def tiles(m, n):
            ds = [mul6(parts, split3(rows(k, 8 * OFF[k], r, m + u)), NN) for u in range(n)]
            for u, d in enumerate(ds):
                x = dst[STEPS - k + m + u] - d
                if put is None:
                    dst[STEPS - k + m + u] = x
                else:
                    here = pl.ds(pl.multiple_of(128 * (m + u), 128), 128)
                    ob[here, pl.ds(pl.multiple_of(128 * put, 128), 128)] = x.T

        by_four(lo, hi, tiles)

    last = [yp[i] for i in range(3)]
    half(xt.at[r], STEPS, last, 0, 4, r)
    y_copy(REST - 1).start()
    half(xt.at[r], STEPS, last, 4, STEPS, r)
    arrive(xn, os.at[1])
    for i in range(REST):
        arrive(yn.at[i], ys.at[1, i])
        if i < REST - 1:
            half(xn, SWAP + 1 + i, split3(yn[i]), 0, SWAP + 1 + i)
    theirs = split3(yn[REST - 1])
    outs = []
    for i in range(4):
        half(xn, STEPS, theirs, 4 * i, 4 * i + 4, ry)
        here = pl.ds(512 * i, 512)
        outs.append(pltpu.make_async_copy(ob.at[here], out_ref.at[here], rs.at[LO, 9 + i]))
        if i:
            outs[i - 1].start()

    for cp in t_copies:
        cp.wait_send()
    t_on.wait_send()
    for k in range(1, STEPS + 1):
        for cp in c_own(k) + c_fwd(k) + c_sib(k) + c_dia(k):
            cp.wait_send()
    x_copy.wait_send()
    for i in range(REST):
        y_copy(i).wait_send()
    outs[3].start()
    for cp in outs:
        cp.wait()


def solution(mesh):
    def body(v_loc, t_loc, z_loc):
        return pl.pallas_call(
            kernel,
            out_shape=jax.ShapeDtypeStruct((2048, 256), F32),
            in_specs=[pl.BlockSpec(memory_space=pl.ANY)] * 3,
            out_specs=pl.BlockSpec(memory_space=pl.ANY),
            scratch_shapes=[
                pltpu.VMEM((256 * OFF[9], 128), F32),
                pltpu.VMEM((32, 32, 32), F32),
                pltpu.VMEM((4096, 128), F32),
                pltpu.VMEM((2048, 256), F32),
                pltpu.VMEM((8 * OFF[STEPS + 1], 64, 128), F32),
                pltpu.VMEM((8, 4, 32, 128), F32),
                pltpu.VMEM((2, 16, 128, 128), F32),
                pltpu.VMEM((16, 128, 128), F32),
                pltpu.VMEM((16, 128, 128), F32),
                pltpu.VMEM((REST, 128, 256), F32),
                pltpu.VMEM((REST, 128, 256), F32),
                pltpu.VMEM((3, 16, 256, 256), BF16),
                pltpu.VMEM((2, 3, 384, 256), BF16),
                pltpu.VMEM((384, 256), F32),
                pltpu.VMEM((3, 128, 256), BF16),
                pltpu.SemaphoreType.DMA((10, STEPS + 1)),
                pltpu.SemaphoreType.DMA((9, STEPS + 1)),
                pltpu.SemaphoreType.DMA((7,)),
                pltpu.SemaphoreType.DMA((1,)),
                pltpu.SemaphoreType.DMA((4,)),
                pltpu.SemaphoreType.DMA((2, REST)),
            ],
            compiler_params=pltpu.CompilerParams(
                collective_id=0, has_side_effects=True, vmem_limit_bytes=64 * 1024 * 1024 - 65536
            ),
        )(v_loc, t_loc, z_loc)

    return jax.shard_map(
        body,
        mesh=mesh,
        in_specs=(P("row", "col"), P("col", None, None), P(None, ("col", "row"))),
        out_specs=P("row", "col"),
        check_vma=False,
    )
```

```python
import functools

import jax
import jax.numpy as jnp
from jax import lax
from jax.experimental import pallas as pl
from jax.experimental.pallas import tpu as pltpu
from jax.sharding import PartitionSpec as P

MESH = pl.DeviceIdType.MESH
F32, BF16 = jnp.float32, jnp.bfloat16
STEPS = 16
OFF = [k * (k - 1) // 2 for k in range(STEPS + 2)]
NT = (((1,), (1,)), ((), ()))
NN = (((1,), (0,)), ((), ()))
SWAP = 13
REST = STEPS - SWAP
O, F, D, S, T, X, V = range(7)
BEFORE = {k: ((S, k),) for k in range(2, STEPS + 1)}
BEFORE[1] = ((V, 1), (V, 2), (O, 1), (O, 2), (V, 3), (T, 0), (O, 3), (F, 1), (O, 4), (F, 2), (D, 1), (S, 1))
BEFORE[14] = ((S, 14), (X, 0))
BEFORE[15] = ((D, 15), (S, 15))
MIDDLE = {k: ((F, k + 2), (O, k + 4)) for k in range(1, 13)}
MIDDLE |= {k: MIDDLE[k] + ((V, (k + 7) // 2),) for k in range(1, 10, 2)}
MIDDLE[13] = ((F, 15),)
MIDDLE[14] = ((F, 16),)
AFTER = {k: ((D, k + 1),) for k in (*range(1, 14), 15)}
ALONG_Y = [0, 0, 1, 1, 2, 2, 3, 3, 4, 4, 5, 5, 6, 6, 7, 7, 0]
FX, FY, DX, DY, SO, SX, SY, SD, SE, LO = range(10)
TX, TY, TS, GX, GY, HX, HY, HD, HE = range(9)


def split3(a):
    p1 = a.astype(BF16)
    rest = a - p1.astype(F32)
    p2 = rest.astype(BF16)
    p3 = (rest - p2.astype(F32)).astype(BF16)
    return p1, p2, p3


def mul6(a, b, dims):
    dot = functools.partial(lax.dot_general, dimension_numbers=dims, preferred_element_type=F32)
    return (
        dot(a[0], b[0]) + dot(a[1], b[0]) + dot(a[2], b[0]) + dot(a[0], b[1]) + dot(a[1], b[1]) + dot(a[0], b[2])
    )


def mulf(a, b, dims=NN):
    return mul6(split3(a), split3(b), dims)


def by_four(lo, hi, fn):
    fours = lax.div(hi - lo, 4)

    def four(i, carry):
        fn(lo + 4 * i, 4)
        return carry

    def one(m, carry):
        fn(m, 1)
        return carry

    lax.fori_loop(0, fours, four, 0)
    lax.fori_loop(lo + 4 * fours, hi, one, 0)


def kernel(v_ref, t_ref, z_ref, out_ref, vs_in, t_in, z_in, ob, land, tl, xt, xs, xn, yo, yn, vp, lp, acc, yp, rs, ss, ts, zs, os, ys):
    r, c = lax.axis_index("row"), lax.axis_index("col")
    cs = c + 1 - 2 * lax.rem(c, 2)
    cx = lax.rem(c + 2, 4)
    csx = lax.rem(cs + 2, 4)
    ry = 1 - r
    to_x, to_y, to_s = (r, cx), (ry, c), (r, cs)

    def seg(k, rr, cc, lo=0, n=None):
        return land.at[pl.ds(8 * OFF[k] + (rr * 4 + cc) * k + lo, k if n is None else n)]

    def rows(k, base, rr, m):
        got = [land[base + (rr * 4 + cc) * k + m] for cc in range(4)]
        return jnp.concatenate([g[:32] for g in got] + [g[32:] for g in got], axis=0)

    def remote(src, dst, send, recv, dev):
        return pltpu.make_async_remote_copy(
            src_ref=src, dst_ref=dst, send_sem=send, recv_sem=recv, device_id=dev, device_id_type=MESH
        )

    def halves(k):
        h = ALONG_Y[k]
        return (0, h), (h, k - h)

    def c_own(k):
        mine = seg(k, r, c)
        return [
            remote(mine, mine, ss.at[TX, k], rs.at[FX, k], to_x),
            remote(mine, mine, ss.at[TY, k], rs.at[FY, k], to_y),
            remote(mine, mine, ss.at[TS, k], rs.at[SO, k], to_s),
        ]

    def c_loc(n):
        q = STEPS // 2 - n
        return pltpu.make_async_copy(
            v_ref.at[pl.ds(256 * q, 256 * n), pl.ds(128 * q, 128)], vs_in.at[pl.ds(256 * OFF[n], 256 * n)], rs.at[LO, n]
        )

    def turn(n):
        c_loc(n).wait()
        even, odd = (8 * OFF[k] + (r * 4 + c) * k for k in (2 * n, 2 * n - 1))

        def tile(m, carry):
            t = vs_in[pl.ds(pl.multiple_of(256 * OFF[n] + 128 * m, 128), 128)].T
            land[even + m] = t[:64]

            @pl.when(m > 0)
            def _():
                land[odd + m - 1] = t[64:]

            return carry

        lax.fori_loop(0, 2 * n, tile, 0)

    def c_fwd(k):
        (a0, an), (b0, bn) = halves(k)
        out = []
        if an:
            out.append(remote(seg(k, r, cx, a0, an), seg(k, r, cx, a0, an), ss.at[GY, k], rs.at[DY, k], to_y))
        if bn:
            out.append(remote(seg(k, ry, c, b0, bn), seg(k, ry, c, b0, bn), ss.at[GX, k], rs.at[DX, k], to_x))
        return out

    def c_sib(k):
        return [
            remote(seg(k, r, cx), seg(k, r, cx), ss.at[HX, k], rs.at[SX, k], to_s),
            remote(seg(k, ry, c), seg(k, ry, c), ss.at[HY, k], rs.at[SY, k], to_s),
        ]

    def c_dia(k):
        (a0, an), (b0, bn) = halves(k)
        out = []
        if an:
            out.append(remote(seg(k, ry, cx, a0, an), seg(k, ry, cx, a0, an), ss.at[HD, k], rs.at[SD, k], to_s))
        if bn:
            out.append(remote(seg(k, ry, cx, b0, bn), seg(k, ry, cx, b0, bn), ss.at[HE, k], rs.at[SE, k], to_s))
        return out

    def arrive(dst, sem):
        pltpu.make_async_copy(dst, dst, sem).wait()

    def wait_first(k):
        arrive(seg(k, r, cx), rs.at[FX, k])
        arrive(seg(k, ry, c), rs.at[FY, k])

    def wait_dia(k):
        (a0, an), (b0, bn) = halves(k)
        if an:
            arrive(seg(k, ry, cx, a0, an), rs.at[DY, k])
        if bn:
            arrive(seg(k, ry, cx, b0, bn), rs.at[DX, k])

    def wait_sib(k):
        arrive(seg(k, r, cs), rs.at[SO, k])
        arrive(seg(k, r, csx), rs.at[SX, k])
        arrive(seg(k, ry, cs), rs.at[SY, k])
        (a0, an), (b0, bn) = halves(k)
        if an:
            arrive(seg(k, ry, csx, a0, an), rs.at[SD, k])
        if bn:
            arrive(seg(k, ry, csx, b0, bn), rs.at[SE, k])

    def start_own(k):
        for cp in c_own(k):
            cp.start()

    t_loc = pltpu.make_async_copy(t_ref, t_in, ts.at[6])
    z_loc = pltpu.make_async_copy(z_ref, z_in, zs.at[0])
    for n in range(1, STEPS // 2 + 1):
        c_loc(n).start()
        if n == 2:
            t_loc.start()
            z_loc.start()
    barrier = pltpu.get_barrier_semaphore()
    for dev in (to_x, to_y, to_s):
        pl.semaphore_signal(barrier, inc=1, device_id=dev, device_id_type=MESH)
    pl.semaphore_wait(barrier, 3)

    t_copies = [
        remote(tl.at[:, c], tl.at[:, c], ts.at[0], ts.at[1], to_x),
        remote(tl.at[:, c], tl.at[:, c], ts.at[2], ts.at[3], to_s),
    ]
    t_on = remote(tl.at[:, cx], tl.at[:, cx], ts.at[4], ts.at[5], to_s)

    x_copy = remote(xs, xn, os.at[0], os.at[1], to_y)

    def y_copy(i):
        return remote(yo.at[i], yn.at[i], ys.at[0, i], ys.at[1, i], to_y)

    def do(ops):
        for op, k in ops:
            if op == O:
                start_own(k)
            elif op == F:
                wait_first(k)
                for cp in c_fwd(k) + c_sib(k):
                    cp.start()
                if k == 1:
                    arrive(tl.at[:, cx], ts.at[1])
                    t_on.start()
            elif op == D:
                wait_dia(k)
                for cp in c_dia(k):
                    cp.start()
            elif op == S:
                wait_sib(k)
                if k == 1:
                    arrive(tl.at[:, cs], ts.at[3])
                    arrive(tl.at[:, csx], ts.at[5])
                    z_loc.wait()
                if k > SWAP + 1:
                    y_copy(k - SWAP - 2).start()
            elif op == T:
                for cp in t_copies:
                    cp.start()
            elif op == V:
                turn(k)
                if k == 2:
                    t_loc.wait()
                    for q in range(8):
                        tl[q, c] = jnp.concatenate([t_in[4 * q + t] for t in range(4)], axis=1)
            else:
                x_copy.start()

    def point(k, table):
        for kk, ops in table.items():
            @pl.when(k == kk)
            def _(ops=ops):
                do(ops)

    lane = lax.broadcasted_iota(jnp.int32, (128, 128), 1)
    sub = lax.broadcasted_iota(jnp.int32, (128, 128), 0)
    pr, pc = sub // 32, lane // 32
    level1 = (pr // 2 == pc // 2) & (pr < pc)
    level2 = pr // 2 < pc // 2

    def step(k, carry):
        point(k, BEFORE)
        J = STEPS - k
        base = 4 * k * (k - 1)
        acc[...] = jnp.zeros_like(acc)
        for rr in range(2):
            xt[rr, J] = z_in[pl.ds(pl.multiple_of(2048 * rr + 128 * J, 128), 128)].T

        def prepare(m, p):
            m = jnp.minimum(m, k - 1)
            for g in range(12):
                if g < 4:
                    here = [xt[rr, J + m, 32 * g : 32 * g + 32] for rr in range(2)]
                else:
                    tt, cc = divmod(g - 4, 4)
                    here = [land[base + (rr * 4 + cc) * k + m, 32 * tt : 32 * tt + 32] for rr in range(2)]
                for i, part in enumerate(split3(jnp.concatenate(here, axis=1))):
                    lp[p, i, 32 * g : 32 * g + 32] = part
                    if g >= 4:
                        vp[i, m, 32 * g - 128 : 32 * g - 96] = part

        def product(p):
            return mul6([lp[p, i] for i in range(3)], [lp[p, i, 128:384] for i in range(3)], NT)

        def four(i, carry):
            acc[...] += product(0) + product(1)
            prepare(4 * i + 2, 2)
            prepare(4 * i + 3, 3)
            acc[...] += product(2) + product(3)
            prepare(4 * i + 4, 0)
            prepare(4 * i + 5, 1)
            return carry

        fours, left = lax.div(k, 4), lax.rem(k, 4)
        mid = lax.div(fours + 1, 2)
        prepare(0, 0)
        prepare(1, 1)
        lax.fori_loop(0, mid, four, 0)
        point(k, MIDDLE)
        lax.fori_loop(mid, fours, four, 0)

        @pl.when(left == 1)
        def _():
            acc[...] += product(0)

        @pl.when(left >= 2)
        def _():
            acc[...] += product(0) + product(1)

        @pl.when(left == 3)
        def _():
            prepare(k - 1, 2)
            acc[...] += product(2)

        q, h = J // 2, lax.rem(J, 2)

        def diag(tt):
            rows = []
            for cc in range(4):
                t32 = tl[q, cc]
                t32 = jnp.where(h == 0, t32, pltpu.roll(t32, 64, 1))
                shift = (32 * cc - 32 * tt) % 128
                rows.append(pltpu.roll(t32, shift, 1) if shift else t32)
            full = jnp.concatenate(rows, axis=0)
            return jnp.where(pr == pc, full, 0.0)

        halves_t = []
        for tt in range(2):
            g = acc[128 + 128 * tt : 256 + 128 * tt, 128 * tt : 128 * tt + 128]
            t = diag(tt)
            t = t - mulf(t, mulf(jnp.where(level1, g, 0.0), t))
            t = t - mulf(t, mulf(jnp.where(level2, g, 0.0), t))
            halves_t.append(t)
        t1, t2 = halves_t
        t12 = -mulf(t1, mulf(acc[128:256, 128:256], t2))
        w1, w2 = acc[0:128, 0:128], acc[0:128, 128:256]
        w2s = split3(w2)
        y1 = mul6(split3(w1), split3(t1), NT) + mul6(w2s, split3(t12), NT)
        y2 = mul6(w2s, split3(t2), NT)
        y = jnp.concatenate([y1, y2], axis=1)
        for i, part in enumerate(split3(y)):
            yp[i] = part

        @pl.when(k > SWAP)
        def _():
            yo[k - SWAP - 1] = y

        point(k, AFTER)

        def update(m, n):
            ps = [yp[i] for i in range(3)]
            ds = [mul6(ps, [vp[i, m + u] for i in range(3)], NN) for u in range(n)]
            for u, d in enumerate(ds):
                xt[0, J + m + u] = xt[0, J + m + u] - d[:, :128]
                xt[1, J + m + u] = xt[1, J + m + u] - d[:, 128:]

        @pl.when(k < STEPS)
        def _():
            by_four(0, k, update)

        @pl.when(k == SWAP)
        def _():
            for m in range(STEPS - SWAP):
                xt[ry, m] = z_in[pl.ds(pl.multiple_of(2048 * ry + 128 * m, 128), 128)].T

            def stage(m, carry):
                xs[m] = xt[ry, m]
                return carry

            lax.fori_loop(0, STEPS, stage, 0)

        return carry

    lax.fori_loop(1, STEPS + 1, step, 0)

    def half(dst, k, parts, lo, hi, put=None):
        def tiles(m, n):
            ds = [mul6(parts, split3(rows(k, 8 * OFF[k], r, m + u)), NN) for u in range(n)]
            for u, d in enumerate(ds):
                x = dst[STEPS - k + m + u] - d
                if put is None:
                    dst[STEPS - k + m + u] = x
                else:
                    here = pl.ds(pl.multiple_of(128 * (m + u), 128), 128)
                    ob[here, pl.ds(pl.multiple_of(128 * put, 128), 128)] = x.T

        by_four(lo, hi, tiles)

    last = [yp[i] for i in range(3)]
    half(xt.at[r], STEPS, last, 0, 4, r)
    y_copy(REST - 1).start()
    half(xt.at[r], STEPS, last, 4, STEPS, r)
    arrive(xn, os.at[1])
    for i in range(REST):
        arrive(yn.at[i], ys.at[1, i])
        if i < REST - 1:
            half(xn, SWAP + 1 + i, split3(yn[i]), 0, SWAP + 1 + i)
    theirs = split3(yn[REST - 1])
    outs = []
    for i in range(4):
        half(xn, STEPS, theirs, 4 * i, 4 * i + 4, ry)
        here = pl.ds(512 * i, 512)
        outs.append(pltpu.make_async_copy(ob.at[here], out_ref.at[here], rs.at[LO, 9 + i]))
        if i:
            outs[i - 1].start()

    for cp in t_copies:
        cp.wait_send()
    t_on.wait_send()
    for k in range(1, STEPS + 1):
        for cp in c_own(k) + c_fwd(k) + c_sib(k) + c_dia(k):
            cp.wait_send()
    x_copy.wait_send()
    for i in range(REST):
        y_copy(i).wait_send()
    outs[3].start()
    for cp in outs:
        cp.wait()


def solution(mesh):
    def body(v_loc, t_loc, z_loc):
        return pl.pallas_call(
            kernel,
            out_shape=jax.ShapeDtypeStruct((2048, 256), F32),
            in_specs=[pl.BlockSpec(memory_space=pl.ANY)] * 3,
            out_specs=pl.BlockSpec(memory_space=pl.ANY),
            scratch_shapes=[
                pltpu.VMEM((256 * OFF[9], 128), F32),
                pltpu.VMEM((32, 32, 32), F32),
                pltpu.VMEM((4096, 128), F32),
                pltpu.VMEM((2048, 256), F32),
                pltpu.VMEM((8 * OFF[STEPS + 1], 64, 128), F32),
                pltpu.VMEM((8, 4, 32, 128), F32),
                pltpu.VMEM((2, 16, 128, 128), F32),
                pltpu.VMEM((16, 128, 128), F32),
                pltpu.VMEM((16, 128, 128), F32),
                pltpu.VMEM((REST, 128, 256), F32),
                pltpu.VMEM((REST, 128, 256), F32),
                pltpu.VMEM((3, 16, 256, 256), BF16),
                pltpu.VMEM((4, 3, 384, 256), BF16),
                pltpu.VMEM((384, 256), F32),
                pltpu.VMEM((3, 128, 256), BF16),
                pltpu.SemaphoreType.DMA((10, STEPS + 1)),
                pltpu.SemaphoreType.DMA((9, STEPS + 1)),
                pltpu.SemaphoreType.DMA((7,)),
                pltpu.SemaphoreType.DMA((1,)),
                pltpu.SemaphoreType.DMA((4,)),
                pltpu.SemaphoreType.DMA((2, REST)),
            ],
            compiler_params=pltpu.CompilerParams(
                collective_id=0, has_side_effects=True, vmem_limit_bytes=64 * 1024 * 1024 - 65536
            ),
        )(v_loc, t_loc, z_loc)

    return jax.shard_map(
        body,
        mesh=mesh,
        in_specs=(P("row", "col"), P("col", None, None), P(None, ("col", "row"))),
        out_specs=P("row", "col"),
        check_vma=False,
    )
```

```python
import functools

import jax
import jax.numpy as jnp
from jax import lax
from jax.experimental import pallas as pl
from jax.experimental.pallas import tpu as pltpu
from jax.sharding import PartitionSpec as P

MESH = pl.DeviceIdType.MESH
F32, BF16 = jnp.float32, jnp.bfloat16
STEPS = 16
OFF = [k * (k - 1) // 2 for k in range(STEPS + 2)]
NT = (((1,), (1,)), ((), ()))
NN = (((1,), (0,)), ((), ()))
SWAP = 14
REST = STEPS - SWAP
O, F, D, S, T, X, V, E = range(8)
BEFORE = {k: ((S, k),) for k in range(2, STEPS + 1)}
BEFORE[1] = ((V, 1), (V, 2), (O, 1), (O, 2), (V, 3), (T, 0), (O, 3), (F, 1), (O, 4), (F, 2), (D, 1), (S, 1))
BEFORE[14] = ((F, 15), (S, 14))
BEFORE[15] = ((F, 16), (X, 0), (D, 15), (S, 15))
MIDDLE = {k: ((F, k + 2), (O, k + 4)) for k in range(1, 13)}
MIDDLE |= {k: MIDDLE[k] + ((V, (k + 7) // 2),) for k in range(1, 10, 2)}
MIDDLE[16] = ((E, 16),)
AFTER = {k: ((D, k + 1),) for k in (*range(1, 14), 15)}
ALONG_Y = [0, 0, 1, 1, 2, 2, 3, 3, 4, 4, 5, 5, 6, 6, 7, 7, 10]
FX, FY, DX, DY, SO, SX, SY, SD, SE, LO = range(10)
TX, TY, TS, GX, GY, HX, HY, HD, HE = range(9)


def split3(a):
    p1 = a.astype(BF16)
    rest = a - p1.astype(F32)
    p2 = rest.astype(BF16)
    p3 = (rest - p2.astype(F32)).astype(BF16)
    return p1, p2, p3


def mul6(a, b, dims):
    dot = functools.partial(lax.dot_general, dimension_numbers=dims, preferred_element_type=F32)
    return (
        dot(a[0], b[0]) + dot(a[1], b[0]) + dot(a[2], b[0]) + dot(a[0], b[1]) + dot(a[1], b[1]) + dot(a[0], b[2])
    )


def mulf(a, b, dims=NN):
    return mul6(split3(a), split3(b), dims)


def by_four(lo, hi, fn):
    fours = lax.div(hi - lo, 4)

    def four(i, carry):
        fn(lo + 4 * i, 4)
        return carry

    def one(m, carry):
        fn(m, 1)
        return carry

    lax.fori_loop(0, fours, four, 0)
    lax.fori_loop(lo + 4 * fours, hi, one, 0)


def kernel(v_ref, t_ref, z_ref, out_ref, vs_in, t_in, z_in, ob, land, tl, xt, xs, xn, yo, yn, vp, lp, acc, yp, rs, ss, ts, zs, os, ys):
    r, c = lax.axis_index("row"), lax.axis_index("col")
    cs = c + 1 - 2 * lax.rem(c, 2)
    cx = lax.rem(c + 2, 4)
    csx = lax.rem(cs + 2, 4)
    ry = 1 - r
    to_x, to_y, to_s = (r, cx), (ry, c), (r, cs)

    def seg(k, rr, cc, lo=0, n=None):
        return land.at[pl.ds(8 * OFF[k] + (rr * 4 + cc) * k + lo, k if n is None else n)]

    def rows(k, base, rr, m):
        got = [land[base + (rr * 4 + cc) * k + m] for cc in range(4)]
        return jnp.concatenate([g[:32] for g in got] + [g[32:] for g in got], axis=0)

    def remote(src, dst, send, recv, dev):
        return pltpu.make_async_remote_copy(
            src_ref=src, dst_ref=dst, send_sem=send, recv_sem=recv, device_id=dev, device_id_type=MESH
        )

    def halves(k):
        h = ALONG_Y[k]
        return (0, h), (h, k - h)

    def c_own(k):
        mine = seg(k, r, c)
        return [
            remote(mine, mine, ss.at[TX, k], rs.at[FX, k], to_x),
            remote(mine, mine, ss.at[TY, k], rs.at[FY, k], to_y),
            remote(mine, mine, ss.at[TS, k], rs.at[SO, k], to_s),
        ]

    def c_loc(n):
        q = STEPS // 2 - n
        return pltpu.make_async_copy(
            v_ref.at[pl.ds(256 * q, 256 * n), pl.ds(128 * q, 128)], vs_in.at[pl.ds(256 * OFF[n], 256 * n)], rs.at[LO, n]
        )

    def turn(n):
        c_loc(n).wait()
        even, odd = (8 * OFF[k] + (r * 4 + c) * k for k in (2 * n, 2 * n - 1))

        def tile(m, carry):
            t = vs_in[pl.ds(pl.multiple_of(256 * OFF[n] + 128 * m, 128), 128)].T
            land[even + m] = t[:64]

            @pl.when(m > 0)
            def _():
                land[odd + m - 1] = t[64:]

            return carry

        lax.fori_loop(0, 2 * n, tile, 0)

    def c_fwd(k):
        (a0, an), (b0, bn) = halves(k)
        out = []
        if k == STEPS:
            out.append(remote(seg(k, ry, c, a0, an), seg(k, ry, c, a0, an), ss.at[GY, k], rs.at[DY, k], to_x))
        elif an:
            out.append(remote(seg(k, r, cx, a0, an), seg(k, r, cx, a0, an), ss.at[GY, k], rs.at[DY, k], to_y))
        if bn:
            out.append(remote(seg(k, ry, c, b0, bn), seg(k, ry, c, b0, bn), ss.at[GX, k], rs.at[DX, k], to_x))
        return out

    def c_sib(k):
        return [
            remote(seg(k, r, cx), seg(k, r, cx), ss.at[HX, k], rs.at[SX, k], to_s),
            remote(seg(k, ry, c), seg(k, ry, c), ss.at[HY, k], rs.at[SY, k], to_s),
        ]

    def c_dia(k):
        (a0, an), (b0, bn) = halves(k)
        out = []
        if an:
            out.append(remote(seg(k, ry, cx, a0, an), seg(k, ry, cx, a0, an), ss.at[HD, k], rs.at[SD, k], to_s))
        if bn:
            out.append(remote(seg(k, ry, cx, b0, bn), seg(k, ry, cx, b0, bn), ss.at[HE, k], rs.at[SE, k], to_s))
        return out

    def arrive(dst, sem):
        pltpu.make_async_copy(dst, dst, sem).wait()

    def wait_first(k):
        arrive(seg(k, r, cx), rs.at[FX, k])
        arrive(seg(k, ry, c), rs.at[FY, k])

    def wait_dia(k):
        (a0, an), (b0, bn) = halves(k)
        if an:
            arrive(seg(k, ry, cx, a0, an), rs.at[DY, k])
        if bn and k < STEPS:
            arrive(seg(k, ry, cx, b0, bn), rs.at[DX, k])

    def wait_sib(k):
        arrive(seg(k, r, cs), rs.at[SO, k])
        arrive(seg(k, r, csx), rs.at[SX, k])
        arrive(seg(k, ry, cs), rs.at[SY, k])
        (a0, an), (b0, bn) = halves(k)
        if an:
            arrive(seg(k, ry, csx, a0, an), rs.at[SD, k])
        if bn and k < STEPS:
            arrive(seg(k, ry, csx, b0, bn), rs.at[SE, k])

    def start_own(k):
        for cp in c_own(k):
            cp.start()

    t_loc = pltpu.make_async_copy(t_ref, t_in, ts.at[6])
    z_loc = pltpu.make_async_copy(z_ref, z_in, zs.at[0])
    for n in range(1, STEPS // 2 + 1):
        c_loc(n).start()
        if n == 2:
            t_loc.start()
            z_loc.start()
    barrier = pltpu.get_barrier_semaphore()
    for dev in (to_x, to_y, to_s):
        pl.semaphore_signal(barrier, inc=1, device_id=dev, device_id_type=MESH)
    pl.semaphore_wait(barrier, 3)

    t_copies = [
        remote(tl.at[:, c], tl.at[:, c], ts.at[0], ts.at[1], to_x),
        remote(tl.at[:, c], tl.at[:, c], ts.at[2], ts.at[3], to_s),
    ]
    t_on = remote(tl.at[:, cx], tl.at[:, cx], ts.at[4], ts.at[5], to_s)

    x_copy = remote(xs, xn, os.at[0], os.at[1], to_y)

    def y_copy(i):
        return remote(yo.at[i], yn.at[i], ys.at[0, i], ys.at[1, i], to_y)

    def do(ops):
        for op, k in ops:
            if op == O:
                start_own(k)
            elif op == F:
                wait_first(k)
                for cp in c_fwd(k) + c_sib(k):
                    cp.start()
                if k == 1:
                    arrive(tl.at[:, cx], ts.at[1])
                    t_on.start()
            elif op == D:
                wait_dia(k)
                for cp in c_dia(k)[: 1 if k == STEPS else 2]:
                    cp.start()
            elif op == E:
                b0, bn = halves(k)[1]
                arrive(seg(k, ry, cx, b0, bn), rs.at[DX, k])
                c_dia(k)[1].start()
                arrive(seg(k, ry, csx, b0, bn), rs.at[SE, k])
            elif op == S:
                wait_sib(k)
                if k == 1:
                    arrive(tl.at[:, cs], ts.at[3])
                    arrive(tl.at[:, csx], ts.at[5])
                    z_loc.wait()
                if k > SWAP + 1:
                    y_copy(k - SWAP - 2).start()
            elif op == T:
                for cp in t_copies:
                    cp.start()
            elif op == V:
                turn(k)
                if k == 2:
                    t_loc.wait()
                    for q in range(8):
                        tl[q, c] = jnp.concatenate([t_in[4 * q + t] for t in range(4)], axis=1)
            else:
                x_copy.start()

    def point(k, table):
        for kk, ops in table.items():
            @pl.when(k == kk)
            def _(ops=ops):
                do(ops)

    lane = lax.broadcasted_iota(jnp.int32, (128, 128), 1)
    sub = lax.broadcasted_iota(jnp.int32, (128, 128), 0)
    pr, pc = sub // 32, lane // 32
    level1 = (pr // 2 == pc // 2) & (pr < pc)
    level2 = pr // 2 < pc // 2

    def step(k, carry):
        point(k, BEFORE)
        J = STEPS - k
        base = 4 * k * (k - 1)
        acc[...] = jnp.zeros_like(acc)
        for rr in range(2):
            xt[rr, J] = z_in[pl.ds(pl.multiple_of(2048 * rr + 128 * J, 128), 128)].T

        def prepare(m, p):
            m = jnp.minimum(m, k - 1)
            for g in range(12):
                if g < 4:
                    here = [xt[rr, J + m, 32 * g : 32 * g + 32] for rr in range(2)]
                else:
                    tt, cc = divmod(g - 4, 4)
                    here = [land[base + (rr * 4 + cc) * k + m, 32 * tt : 32 * tt + 32] for rr in range(2)]
                for i, part in enumerate(split3(jnp.concatenate(here, axis=1))):
                    lp[p, i, 32 * g : 32 * g + 32] = part
                    if g >= 4:
                        vp[i, m, 32 * g - 128 : 32 * g - 96] = part

        def product(p):
            return mul6([lp[p, i] for i in range(3)], [lp[p, i, 128:384] for i in range(3)], NT)

        def four(i, carry):
            acc[...] += product(0) + product(1)
            prepare(4 * i + 2, 2)
            prepare(4 * i + 3, 3)
            acc[...] += product(2) + product(3)
            prepare(4 * i + 4, 0)
            prepare(4 * i + 5, 1)
            return carry

        fours, left = lax.div(k, 4), lax.rem(k, 4)
        mid = lax.div(fours + 1, 2)
        prepare(0, 0)
        prepare(1, 1)
        lax.fori_loop(0, mid, four, 0)
        point(k, MIDDLE)
        lax.fori_loop(mid, fours, four, 0)

        @pl.when(left == 1)
        def _():
            acc[...] += product(0)

        @pl.when(left >= 2)
        def _():
            acc[...] += product(0) + product(1)

        @pl.when(left == 3)
        def _():
            prepare(k - 1, 2)
            acc[...] += product(2)

        q, h = J // 2, lax.rem(J, 2)

        def diag(tt):
            rows = []
            for cc in range(4):
                t32 = tl[q, cc]
                t32 = jnp.where(h == 0, t32, pltpu.roll(t32, 64, 1))
                shift = (32 * cc - 32 * tt) % 128
                rows.append(pltpu.roll(t32, shift, 1) if shift else t32)
            full = jnp.concatenate(rows, axis=0)
            return jnp.where(pr == pc, full, 0.0)

        halves_t = []
        for tt in range(2):
            g = acc[128 + 128 * tt : 256 + 128 * tt, 128 * tt : 128 * tt + 128]
            t = diag(tt)
            t = t - mulf(t, mulf(jnp.where(level1, g, 0.0), t))
            t = t - mulf(t, mulf(jnp.where(level2, g, 0.0), t))
            halves_t.append(t)
        t1, t2 = halves_t
        t12 = -mulf(t1, mulf(acc[128:256, 128:256], t2))
        w1, w2 = acc[0:128, 0:128], acc[0:128, 128:256]
        w2s = split3(w2)
        y1 = mul6(split3(w1), split3(t1), NT) + mul6(w2s, split3(t12), NT)
        y2 = mul6(w2s, split3(t2), NT)
        y = jnp.concatenate([y1, y2], axis=1)
        for i, part in enumerate(split3(y)):
            yp[i] = part

        @pl.when(k > SWAP)
        def _():
            yo[k - SWAP - 1] = y

        point(k, AFTER)

        def update(m, n):
            ps = [yp[i] for i in range(3)]
            ds = [mul6(ps, [vp[i, m + u] for i in range(3)], NN) for u in range(n)]
            for u, d in enumerate(ds):
                xt[0, J + m + u] = xt[0, J + m + u] - d[:, :128]
                xt[1, J + m + u] = xt[1, J + m + u] - d[:, 128:]

        @pl.when(k < STEPS)
        def _():
            by_four(0, k, update)

        @pl.when(k == SWAP)
        def _():
            for m in range(STEPS - SWAP):
                xt[ry, m] = z_in[pl.ds(pl.multiple_of(2048 * ry + 128 * m, 128), 128)].T

            def stage(m, carry):
                xs[m] = xt[ry, m]
                return carry

            lax.fori_loop(0, STEPS, stage, 0)

        return carry

    lax.fori_loop(1, STEPS + 1, step, 0)

    def half(dst, k, parts, lo, hi, put=None):
        def tiles(m, n):
            ds = [mul6(parts, split3(rows(k, 8 * OFF[k], r, m + u)), NN) for u in range(n)]
            for u, d in enumerate(ds):
                x = dst[STEPS - k + m + u] - d
                if put is None:
                    dst[STEPS - k + m + u] = x
                else:
                    here = pl.ds(pl.multiple_of(128 * (m + u), 128), 128)
                    ob[here, pl.ds(pl.multiple_of(128 * put, 128), 128)] = x.T

        by_four(lo, hi, tiles)

    last = [yp[i] for i in range(3)]
    half(xt.at[r], STEPS, last, 0, 4, r)
    y_copy(REST - 1).start()
    half(xt.at[r], STEPS, last, 4, STEPS, r)
    arrive(xn, os.at[1])
    for i in range(REST):
        arrive(yn.at[i], ys.at[1, i])
        if i < REST - 1:
            half(xn, SWAP + 1 + i, split3(yn[i]), 0, SWAP + 1 + i)
    theirs = split3(yn[REST - 1])
    outs = []
    for i in range(4):
        half(xn, STEPS, theirs, 4 * i, 4 * i + 4, ry)
        here = pl.ds(512 * i, 512)
        outs.append(pltpu.make_async_copy(ob.at[here], out_ref.at[here], rs.at[LO, 9 + i]))
        if i:
            outs[i - 1].start()

    for cp in t_copies:
        cp.wait_send()
    t_on.wait_send()
    for k in range(1, STEPS + 1):
        for cp in c_own(k) + c_fwd(k) + c_sib(k) + c_dia(k):
            cp.wait_send()
    x_copy.wait_send()
    for i in range(REST):
        y_copy(i).wait_send()
    outs[3].start()
    for cp in outs:
        cp.wait()


def solution(mesh):
    def body(v_loc, t_loc, z_loc):
        return pl.pallas_call(
            kernel,
            out_shape=jax.ShapeDtypeStruct((2048, 256), F32),
            in_specs=[pl.BlockSpec(memory_space=pl.ANY)] * 3,
            out_specs=pl.BlockSpec(memory_space=pl.ANY),
            scratch_shapes=[
                pltpu.VMEM((256 * OFF[9], 128), F32),
                pltpu.VMEM((32, 32, 32), F32),
                pltpu.VMEM((4096, 128), F32),
                pltpu.VMEM((2048, 256), F32),
                pltpu.VMEM((8 * OFF[STEPS + 1], 64, 128), F32),
                pltpu.VMEM((8, 4, 32, 128), F32),
                pltpu.VMEM((2, 16, 128, 128), F32),
                pltpu.VMEM((16, 128, 128), F32),
                pltpu.VMEM((16, 128, 128), F32),
                pltpu.VMEM((REST, 128, 256), F32),
                pltpu.VMEM((REST, 128, 256), F32),
                pltpu.VMEM((3, 16, 256, 256), BF16),
                pltpu.VMEM((4, 3, 384, 256), BF16),
                pltpu.VMEM((384, 256), F32),
                pltpu.VMEM((3, 128, 256), BF16),
                pltpu.SemaphoreType.DMA((10, STEPS + 1)),
                pltpu.SemaphoreType.DMA((9, STEPS + 1)),
                pltpu.SemaphoreType.DMA((7,)),
                pltpu.SemaphoreType.DMA((1,)),
                pltpu.SemaphoreType.DMA((4,)),
                pltpu.SemaphoreType.DMA((2, REST)),
            ],
            compiler_params=pltpu.CompilerParams(
                collective_id=0, has_side_effects=True, vmem_limit_bytes=64 * 1024 * 1024 - 65536
            ),
        )(v_loc, t_loc, z_loc)

    return jax.shard_map(
        body,
        mesh=mesh,
        in_specs=(P("row", "col"), P("col", None, None), P(None, ("col", "row"))),
        out_specs=P("row", "col"),
        check_vma=False,
    )
```

```python
import functools

import jax
import jax.numpy as jnp
from jax import lax
from jax.experimental import pallas as pl
from jax.experimental.pallas import tpu as pltpu
from jax.sharding import PartitionSpec as P

MESH = pl.DeviceIdType.MESH
F32, BF16 = jnp.float32, jnp.bfloat16
STEPS = 16
OFF = [k * (k - 1) // 2 for k in range(STEPS + 2)]
NT = (((1,), (1,)), ((), ()))
NN = (((1,), (0,)), ((), ()))
SWAP = 14
REST = STEPS - SWAP
O, F, D, S, T, X, V, E, R, W = range(10)
BEFORE = {k: ((S, k),) for k in range(2, STEPS + 1)}
BEFORE[1] = ((V, 1), (V, 2), (O, 1), (O, 2), (V, 3), (T, 0), (O, 3), (O, 4), (F, 1), (F, 2), (D, 1), (S, 1))
BEFORE[14] = ((F, 15), (S, 14))
BEFORE[15] = ((F, 16), (X, 0), (W, 13), (D, 15), (S, 15))
BEFORE[16] = ((S, 16), (E, 16))
MIDDLE = {k: ((F, k + 2), (O, k + 4)) for k in range(1, 13)}
MIDDLE |= {k: MIDDLE[k] + ((V, (k + 7) // 2),) for k in range(1, 10, 2)}
MIDDLE[16] = ((R, 16),)
AFTER = {k: ((D, k + 1),) for k in (*range(1, 14), 15)}
ALONG_Y = [0, 0, 1, 1, 2, 2, 3, 4, 4, 5, 5, 6, 6, 7, 7, 5, 10]
FX, FY, DX, DY, SO, SX, SY, SD, SE, LO = range(10)
TX, TY, TS, GX, GY, HX, HY, HD, HE = range(9)


def split3(a):
    p1 = a.astype(BF16)
    rest = a - p1.astype(F32)
    p2 = rest.astype(BF16)
    p3 = (rest - p2.astype(F32)).astype(BF16)
    return p1, p2, p3


def mul6(a, b, dims):
    dot = functools.partial(lax.dot_general, dimension_numbers=dims, preferred_element_type=F32)
    return (
        dot(a[0], b[0]) + dot(a[1], b[0]) + dot(a[2], b[0]) + dot(a[0], b[1]) + dot(a[1], b[1]) + dot(a[0], b[2])
    )


def mulf(a, b, dims=NN):
    return mul6(split3(a), split3(b), dims)


def by_four(lo, hi, fn):
    fours = lax.div(hi - lo, 4)

    def four(i, carry):
        fn(lo + 4 * i, 4)
        return carry

    def one(m, carry):
        fn(m, 1)
        return carry

    lax.fori_loop(0, fours, four, 0)
    lax.fori_loop(lo + 4 * fours, hi, one, 0)


def kernel(v_ref, t_ref, z_ref, out_ref, vs_in, t_in, z_in, ob, land, tl, xt, xs, xn, yo, yn, vp, lp, acc, yp, rs, ss, ts, zs, os, ys):
    r, c = lax.axis_index("row"), lax.axis_index("col")
    cs = c + 1 - 2 * lax.rem(c, 2)
    cx = lax.rem(c + 2, 4)
    csx = lax.rem(cs + 2, 4)
    ry = 1 - r
    to_x, to_y, to_s = (r, cx), (ry, c), (r, cs)

    def seg(k, rr, cc, lo=0, n=None):
        return land.at[pl.ds(8 * OFF[k] + (rr * 4 + cc) * k + lo, k if n is None else n)]

    def rows(k, base, rr, m):
        got = [land[base + (rr * 4 + cc) * k + m] for cc in range(4)]
        return jnp.concatenate([g[:32] for g in got] + [g[32:] for g in got], axis=0)

    def remote(src, dst, send, recv, dev):
        return pltpu.make_async_remote_copy(
            src_ref=src, dst_ref=dst, send_sem=send, recv_sem=recv, device_id=dev, device_id_type=MESH
        )

    def halves(k):
        h = ALONG_Y[k]
        return (0, h), (h, k - h)

    def c_own(k):
        mine = seg(k, r, c)
        return [
            remote(mine, mine, ss.at[TX, k], rs.at[FX, k], to_x),
            remote(mine, mine, ss.at[TY, k], rs.at[FY, k], to_y),
            remote(mine, mine, ss.at[TS, k], rs.at[SO, k], to_s),
        ]

    def c_loc(n):
        q = STEPS // 2 - n
        return pltpu.make_async_copy(
            v_ref.at[pl.ds(256 * q, 256 * n), pl.ds(128 * q, 128)], vs_in.at[pl.ds(256 * OFF[n], 256 * n)], rs.at[LO, n]
        )

    def turn(n):
        c_loc(n).wait()
        even, odd = (8 * OFF[k] + (r * 4 + c) * k for k in (2 * n, 2 * n - 1))

        def tile(m, carry):
            t = vs_in[pl.ds(pl.multiple_of(256 * OFF[n] + 128 * m, 128), 128)].T
            land[even + m] = t[:64]

            @pl.when(m > 0)
            def _():
                land[odd + m - 1] = t[64:]

            return carry

        lax.fori_loop(0, 2 * n, tile, 0)

    def c_fwd(k):
        (a0, an), (b0, bn) = halves(k)
        out = []
        if k == STEPS:
            out.append(remote(seg(k, ry, c, a0, an), seg(k, ry, c, a0, an), ss.at[GY, k], rs.at[DY, k], to_x))
        elif an:
            out.append(remote(seg(k, r, cx, a0, an), seg(k, r, cx, a0, an), ss.at[GY, k], rs.at[DY, k], to_y))
        if bn:
            out.append(remote(seg(k, ry, c, b0, bn), seg(k, ry, c, b0, bn), ss.at[GX, k], rs.at[DX, k], to_x))
        return out

    def c_sib(k):
        return [
            remote(seg(k, r, cx), seg(k, r, cx), ss.at[HX, k], rs.at[SX, k], to_s),
            remote(seg(k, ry, c), seg(k, ry, c), ss.at[HY, k], rs.at[SY, k], to_s),
        ]

    def c_dia(k):
        (a0, an), (b0, bn) = halves(k)
        out = []
        if an:
            out.append(remote(seg(k, ry, cx, a0, an), seg(k, ry, cx, a0, an), ss.at[HD, k], rs.at[SD, k], to_s))
        if bn:
            out.append(remote(seg(k, ry, cx, b0, bn), seg(k, ry, cx, b0, bn), ss.at[HE, k], rs.at[SE, k], to_s))
        return out

    def arrive(dst, sem):
        pltpu.make_async_copy(dst, dst, sem).wait()

    def wait_first(k):
        arrive(seg(k, r, cx), rs.at[FX, k])
        arrive(seg(k, ry, c), rs.at[FY, k])

    def wait_dia(k):
        (a0, an), (b0, bn) = halves(k)
        if an:
            arrive(seg(k, ry, cx, a0, an), rs.at[DY, k])
        if bn and k < STEPS:
            arrive(seg(k, ry, cx, b0, bn), rs.at[DX, k])

    def wait_sib(k):
        arrive(seg(k, r, cs), rs.at[SO, k])
        arrive(seg(k, r, csx), rs.at[SX, k])
        arrive(seg(k, ry, cs), rs.at[SY, k])
        (a0, an), (b0, bn) = halves(k)
        if an:
            arrive(seg(k, ry, csx, a0, an), rs.at[SD, k])
        if bn and k < STEPS:
            arrive(seg(k, ry, csx, b0, bn), rs.at[SE, k])

    def start_own(k):
        for cp in c_own(k):
            cp.start()

    t_loc = pltpu.make_async_copy(t_ref, t_in, ts.at[6])
    z_loc = pltpu.make_async_copy(z_ref, z_in, zs.at[0])
    for n in range(1, STEPS // 2 + 1):
        c_loc(n).start()
        if n == 2:
            t_loc.start()
            z_loc.start()
    barrier = pltpu.get_barrier_semaphore()
    for dev in (to_x, to_y, to_s):
        pl.semaphore_signal(barrier, inc=1, device_id=dev, device_id_type=MESH)
    pl.semaphore_wait(barrier, 3)

    t_copies = [
        remote(tl.at[:, c], tl.at[:, c], ts.at[0], ts.at[1], to_x),
        remote(tl.at[:, c], tl.at[:, c], ts.at[2], ts.at[3], to_s),
    ]
    t_on = remote(tl.at[:, cx], tl.at[:, cx], ts.at[4], ts.at[5], to_s)

    x_copy = remote(xs, xn, os.at[0], os.at[1], to_y)

    def y_copy(i):
        return remote(yo.at[i], yn.at[i], ys.at[0, i], ys.at[1, i], to_y)

    def sent(lo, hi):
        if lo == 1:
            for cp in t_copies + [t_on]:
                cp.wait_send()
        for k in range(lo, hi + 1):
            for cp in c_own(k) + c_fwd(k) + c_sib(k) + c_dia(k):
                cp.wait_send()

    def do(ops):
        for op, k in ops:
            if op == O:
                start_own(k)
            elif op == F:
                wait_first(k)
                for cp in c_fwd(k) + c_sib(k):
                    cp.start()
                if k == 1:
                    arrive(tl.at[:, cx], ts.at[1])
                    t_on.start()
            elif op == D:
                wait_dia(k)
                for cp in c_dia(k)[: 1 if k == STEPS else 2]:
                    cp.start()
            elif op == E:
                b0, bn = halves(k)[1]
                arrive(seg(k, ry, cx, b0, bn), rs.at[DX, k])
                c_dia(k)[1].start()
            elif op == R:
                b0, bn = halves(k)[1]
                arrive(seg(k, ry, csx, b0, bn), rs.at[SE, k])
            elif op == W:
                sent(1, k)
            elif op == S:
                wait_sib(k)
                if k == 1:
                    arrive(tl.at[:, cs], ts.at[3])
                    arrive(tl.at[:, csx], ts.at[5])
                    z_loc.wait()
                if k > SWAP + 1:
                    y_copy(k - SWAP - 2).start()
            elif op == T:
                for cp in t_copies:
                    cp.start()
            elif op == V:
                turn(k)
                if k == 2:
                    t_loc.wait()
                    for q in range(8):
                        tl[q, c] = jnp.concatenate([t_in[4 * q + t] for t in range(4)], axis=1)
            else:
                x_copy.start()

    def point(k, table):
        for kk, ops in table.items():
            @pl.when(k == kk)
            def _(ops=ops):
                do(ops)

    lane = lax.broadcasted_iota(jnp.int32, (128, 128), 1)
    sub = lax.broadcasted_iota(jnp.int32, (128, 128), 0)
    pr, pc = sub // 32, lane // 32
    level1 = (pr // 2 == pc // 2) & (pr < pc)
    level2 = pr // 2 < pc // 2

    def step(k, carry):
        point(k, BEFORE)
        J = STEPS - k
        base = 4 * k * (k - 1)
        acc[...] = jnp.zeros_like(acc)
        for rr in range(2):
            xt[rr, J] = z_in[pl.ds(pl.multiple_of(2048 * rr + 128 * J, 128), 128)].T

        def prepare(m, p):
            m = jnp.minimum(m, k - 1)
            for g in range(12):
                if g < 4:
                    here = [xt[rr, J + m, 32 * g : 32 * g + 32] for rr in range(2)]
                else:
                    tt, cc = divmod(g - 4, 4)
                    here = [land[base + (rr * 4 + cc) * k + m, 32 * tt : 32 * tt + 32] for rr in range(2)]
                for i, part in enumerate(split3(jnp.concatenate(here, axis=1))):
                    lp[p, i, 32 * g : 32 * g + 32] = part
                    if g >= 4:
                        vp[i, m, 32 * g - 128 : 32 * g - 96] = part

        def product(p):
            return mul6([lp[p, i] for i in range(3)], [lp[p, i, 128:384] for i in range(3)], NT)

        def four(i, carry):
            acc[...] += product(0) + product(1)
            prepare(4 * i + 2, 2)
            prepare(4 * i + 3, 3)
            acc[...] += product(2) + product(3)
            prepare(4 * i + 4, 0)
            prepare(4 * i + 5, 1)
            return carry

        fours, left = lax.div(k, 4), lax.rem(k, 4)
        mid = lax.div(fours + 1, 2)
        prepare(0, 0)
        prepare(1, 1)
        lax.fori_loop(0, mid, four, 0)
        point(k, MIDDLE)
        lax.fori_loop(mid, fours, four, 0)

        @pl.when(left == 1)
        def _():
            acc[...] += product(0)

        @pl.when(left >= 2)
        def _():
            acc[...] += product(0) + product(1)

        @pl.when(left == 3)
        def _():
            prepare(k - 1, 2)
            acc[...] += product(2)

        q, h = J // 2, lax.rem(J, 2)

        def diag(tt):
            rows = []
            for cc in range(4):
                t32 = tl[q, cc]
                t32 = jnp.where(h == 0, t32, pltpu.roll(t32, 64, 1))
                shift = (32 * cc - 32 * tt) % 128
                rows.append(pltpu.roll(t32, shift, 1) if shift else t32)
            full = jnp.concatenate(rows, axis=0)
            return jnp.where(pr == pc, full, 0.0)

        halves_t = []
        for tt in range(2):
            g = acc[128 + 128 * tt : 256 + 128 * tt, 128 * tt : 128 * tt + 128]
            t = diag(tt)
            t = t - mulf(t, mulf(jnp.where(level1, g, 0.0), t))
            t = t - mulf(t, mulf(jnp.where(level2, g, 0.0), t))
            halves_t.append(t)
        t1, t2 = halves_t
        t12 = -mulf(t1, mulf(acc[128:256, 128:256], t2))
        w1, w2 = acc[0:128, 0:128], acc[0:128, 128:256]
        w2s = split3(w2)
        y1 = mul6(split3(w1), split3(t1), NT) + mul6(w2s, split3(t12), NT)
        y2 = mul6(w2s, split3(t2), NT)
        y = jnp.concatenate([y1, y2], axis=1)
        for i, part in enumerate(split3(y)):
            yp[i] = part

        @pl.when(k > SWAP)
        def _():
            yo[k - SWAP - 1] = y

        point(k, AFTER)

        def update(m, n):
            ps = [yp[i] for i in range(3)]
            ds = [mul6(ps, [vp[i, m + u] for i in range(3)], NN) for u in range(n)]
            for u, d in enumerate(ds):
                xt[0, J + m + u] = xt[0, J + m + u] - d[:, :128]
                xt[1, J + m + u] = xt[1, J + m + u] - d[:, 128:]

        @pl.when(k < STEPS)
        def _():
            by_four(0, k, update)

        @pl.when(k == SWAP)
        def _():
            for m in range(STEPS - SWAP):
                xt[ry, m] = z_in[pl.ds(pl.multiple_of(2048 * ry + 128 * m, 128), 128)].T

            def stage(m, carry):
                xs[m] = xt[ry, m]
                return carry

            lax.fori_loop(0, STEPS, stage, 0)

        return carry

    lax.fori_loop(1, STEPS + 1, step, 0)

    def half(dst, k, parts, lo, hi, put=None):
        def tiles(m, n):
            ds = [mul6(parts, split3(rows(k, 8 * OFF[k], r, m + u)), NN) for u in range(n)]
            for u, d in enumerate(ds):
                x = dst[STEPS - k + m + u] - d
                if put is None:
                    dst[STEPS - k + m + u] = x
                else:
                    here = pl.ds(pl.multiple_of(128 * (m + u), 128), 128)
                    ob[here, pl.ds(pl.multiple_of(128 * put, 128), 128)] = x.T

        by_four(lo, hi, tiles)

    last = [yp[i] for i in range(3)]
    half(xt.at[r], STEPS, last, 0, 4, r)
    y_copy(REST - 1).start()
    half(xt.at[r], STEPS, last, 4, STEPS, r)
    arrive(xn, os.at[1])
    for i in range(REST):
        arrive(yn.at[i], ys.at[1, i])
        if i < REST - 1:
            half(xn, SWAP + 1 + i, split3(yn[i]), 0, SWAP + 1 + i)
    theirs = split3(yn[REST - 1])
    outs = []
    for i in range(4):
        half(xn, STEPS, theirs, 4 * i, 4 * i + 4, ry)
        here = pl.ds(512 * i, 512)
        outs.append(pltpu.make_async_copy(ob.at[here], out_ref.at[here], rs.at[LO, 9 + i]))
        if i:
            outs[i - 1].start()

    sent(14, STEPS)
    x_copy.wait_send()
    for i in range(REST):
        y_copy(i).wait_send()
    outs[3].start()
    for cp in outs:
        cp.wait()


def solution(mesh):
    def body(v_loc, t_loc, z_loc):
        return pl.pallas_call(
            kernel,
            out_shape=jax.ShapeDtypeStruct((2048, 256), F32),
            in_specs=[pl.BlockSpec(memory_space=pl.ANY)] * 3,
            out_specs=pl.BlockSpec(memory_space=pl.ANY),
            scratch_shapes=[
                pltpu.VMEM((256 * OFF[9], 128), F32),
                pltpu.VMEM((32, 32, 32), F32),
                pltpu.VMEM((4096, 128), F32),
                pltpu.VMEM((2048, 256), F32),
                pltpu.VMEM((8 * OFF[STEPS + 1], 64, 128), F32),
                pltpu.VMEM((8, 4, 32, 128), F32),
                pltpu.VMEM((2, 16, 128, 128), F32),
                pltpu.VMEM((16, 128, 128), F32),
                pltpu.VMEM((16, 128, 128), F32),
                pltpu.VMEM((REST, 128, 256), F32),
                pltpu.VMEM((REST, 128, 256), F32),
                pltpu.VMEM((3, 16, 256, 256), BF16),
                pltpu.VMEM((4, 3, 384, 256), BF16),
                pltpu.VMEM((384, 256), F32),
                pltpu.VMEM((3, 128, 256), BF16),
                pltpu.SemaphoreType.DMA((10, STEPS + 1)),
                pltpu.SemaphoreType.DMA((9, STEPS + 1)),
                pltpu.SemaphoreType.DMA((7,)),
                pltpu.SemaphoreType.DMA((1,)),
                pltpu.SemaphoreType.DMA((4,)),
                pltpu.SemaphoreType.DMA((2, REST)),
            ],
            compiler_params=pltpu.CompilerParams(
                collective_id=0, has_side_effects=True, vmem_limit_bytes=64 * 1024 * 1024 - 65536
            ),
        )(v_loc, t_loc, z_loc)

    return jax.shard_map(
        body,
        mesh=mesh,
        in_specs=(P("row", "col"), P("col", None, None), P(None, ("col", "row"))),
        out_specs=P("row", "col"),
        check_vma=False,
    )
```

```python
import functools

import jax
import jax.numpy as jnp
from jax import lax
from jax.experimental import pallas as pl
from jax.experimental.pallas import tpu as pltpu
from jax.sharding import PartitionSpec as P

MESH = pl.DeviceIdType.MESH
F32, BF16 = jnp.float32, jnp.bfloat16
STEPS = 16
OFF = [k * (k - 1) // 2 for k in range(STEPS + 2)]
NT = (((1,), (1,)), ((), ()))
NN = (((1,), (0,)), ((), ()))
SWAP = 14
REST = STEPS - SWAP
O, F, D, S, T, X, V, E, R, W = range(10)
BEFORE = {k: ((S, k),) for k in range(2, STEPS + 1)}
BEFORE[1] = ((V, 1), (V, 2), (O, 1), (O, 2), (V, 3), (T, 0), (O, 3), (O, 4), (F, 1), (F, 2), (D, 1), (S, 1))
BEFORE[14] = ((F, 15), (S, 14))
BEFORE[15] = ((F, 16), (X, 0), (D, 15), (W, 13), (S, 15))
BEFORE[16] = ((S, 16), (E, 16))
MIDDLE = {k: ((F, k + 2), (O, k + 4)) for k in range(1, 13)}
MIDDLE |= {k: MIDDLE[k] + ((V, (k + 7) // 2),) for k in range(1, 10, 2)}
MIDDLE[16] = ((R, 16),)
AFTER = {k: ((D, k + 1),) for k in (*range(1, 14), 15)}
ALONG_Y = [0, 0, 1, 1, 2, 2, 3, 4, 4, 5, 5, 6, 6, 7, 7, 5, 10]
FX, FY, DX, DY, SO, SX, SY, SD, SE, LO = range(10)
TX, TY, TS, GX, GY, HX, HY, HD, HE = range(9)


def split3(a):
    p1 = a.astype(BF16)
    rest = a - p1.astype(F32)
    p2 = rest.astype(BF16)
    p3 = (rest - p2.astype(F32)).astype(BF16)
    return p1, p2, p3


def mul6(a, b, dims):
    dot = functools.partial(lax.dot_general, dimension_numbers=dims, preferred_element_type=F32)
    return (
        dot(a[0], b[0]) + dot(a[1], b[0]) + dot(a[2], b[0]) + dot(a[0], b[1]) + dot(a[1], b[1]) + dot(a[0], b[2])
    )


def mulf(a, b, dims=NN):
    return mul6(split3(a), split3(b), dims)


def by_four(lo, hi, fn):
    fours = lax.div(hi - lo, 4)

    def four(i, carry):
        fn(lo + 4 * i, 4)
        return carry

    def one(m, carry):
        fn(m, 1)
        return carry

    lax.fori_loop(0, fours, four, 0)
    lax.fori_loop(lo + 4 * fours, hi, one, 0)


def kernel(v_ref, t_ref, z_ref, out_ref, vs_in, t_in, z_in, ob, land, tl, xt, xs, xn, yo, yn, vp, lp, acc, yp, rs, ss, ts, zs, os, ys):
    r, c = lax.axis_index("row"), lax.axis_index("col")
    cs = c + 1 - 2 * lax.rem(c, 2)
    cx = lax.rem(c + 2, 4)
    csx = lax.rem(cs + 2, 4)
    ry = 1 - r
    to_x, to_y, to_s = (r, cx), (ry, c), (r, cs)

    def seg(k, rr, cc, lo=0, n=None):
        return land.at[pl.ds(8 * OFF[k] + (rr * 4 + cc) * k + lo, k if n is None else n)]

    def rows(k, base, rr, m):
        got = [land[base + (rr * 4 + cc) * k + m] for cc in range(4)]
        return jnp.concatenate([g[:32] for g in got] + [g[32:] for g in got], axis=0)

    def remote(src, dst, send, recv, dev):
        return pltpu.make_async_remote_copy(
            src_ref=src, dst_ref=dst, send_sem=send, recv_sem=recv, device_id=dev, device_id_type=MESH
        )

    def halves(k):
        h = ALONG_Y[k]
        return (0, h), (h, k - h)

    def c_own(k):
        mine = seg(k, r, c)
        return [
            remote(mine, mine, ss.at[TX, k], rs.at[FX, k], to_x),
            remote(mine, mine, ss.at[TY, k], rs.at[FY, k], to_y),
            remote(mine, mine, ss.at[TS, k], rs.at[SO, k], to_s),
        ]

    def c_loc(n):
        q = STEPS // 2 - n
        return pltpu.make_async_copy(
            v_ref.at[pl.ds(256 * q, 256 * n), pl.ds(128 * q, 128)], vs_in.at[pl.ds(256 * OFF[n], 256 * n)], rs.at[LO, n]
        )

    def turn(n):
        c_loc(n).wait()
        even, odd = (8 * OFF[k] + (r * 4 + c) * k for k in (2 * n, 2 * n - 1))

        def tile(m, carry):
            t = vs_in[pl.ds(pl.multiple_of(256 * OFF[n] + 128 * m, 128), 128)].T
            land[even + m] = t[:64]

            @pl.when(m > 0)
            def _():
                land[odd + m - 1] = t[64:]

            return carry

        lax.fori_loop(0, 2 * n, tile, 0)

    def c_fwd(k):
        (a0, an), (b0, bn) = halves(k)
        out = []
        if k == STEPS:
            out.append(remote(seg(k, ry, c, a0, an), seg(k, ry, c, a0, an), ss.at[GY, k], rs.at[DY, k], to_x))
        elif an:
            out.append(remote(seg(k, r, cx, a0, an), seg(k, r, cx, a0, an), ss.at[GY, k], rs.at[DY, k], to_y))
        if bn:
            out.append(remote(seg(k, ry, c, b0, bn), seg(k, ry, c, b0, bn), ss.at[GX, k], rs.at[DX, k], to_x))
        return out

    def c_sib(k):
        return [
            remote(seg(k, r, cx), seg(k, r, cx), ss.at[HX, k], rs.at[SX, k], to_s),
            remote(seg(k, ry, c), seg(k, ry, c), ss.at[HY, k], rs.at[SY, k], to_s),
        ]

    def c_dia(k):
        (a0, an), (b0, bn) = halves(k)
        out = []
        if an:
            out.append(remote(seg(k, ry, cx, a0, an), seg(k, ry, cx, a0, an), ss.at[HD, k], rs.at[SD, k], to_s))
        if bn:
            out.append(remote(seg(k, ry, cx, b0, bn), seg(k, ry, cx, b0, bn), ss.at[HE, k], rs.at[SE, k], to_s))
        return out

    def arrive(dst, sem):
        pltpu.make_async_copy(dst, dst, sem).wait()

    def wait_first(k):
        arrive(seg(k, r, cx), rs.at[FX, k])
        arrive(seg(k, ry, c), rs.at[FY, k])

    def wait_dia(k):
        (a0, an), (b0, bn) = halves(k)
        if an:
            arrive(seg(k, ry, cx, a0, an), rs.at[DY, k])
        if bn and k < STEPS:
            arrive(seg(k, ry, cx, b0, bn), rs.at[DX, k])

    def wait_sib(k):
        arrive(seg(k, r, cs), rs.at[SO, k])
        arrive(seg(k, r, csx), rs.at[SX, k])
        arrive(seg(k, ry, cs), rs.at[SY, k])
        (a0, an), (b0, bn) = halves(k)
        if an:
            arrive(seg(k, ry, csx, a0, an), rs.at[SD, k])
        if bn and k < STEPS:
            arrive(seg(k, ry, csx, b0, bn), rs.at[SE, k])

    def start_own(k):
        for cp in c_own(k):
            cp.start()

    t_loc = pltpu.make_async_copy(t_ref, t_in, ts.at[6])
    z_loc = pltpu.make_async_copy(z_ref, z_in, zs.at[0])
    for n in range(1, STEPS // 2 + 1):
        c_loc(n).start()
        if n == 2:
            t_loc.start()
            z_loc.start()
    barrier = pltpu.get_barrier_semaphore()
    for dev in (to_x, to_y, to_s):
        pl.semaphore_signal(barrier, inc=1, device_id=dev, device_id_type=MESH)
    pl.semaphore_wait(barrier, 3)

    t_copies = [
        remote(tl.at[:, c], tl.at[:, c], ts.at[0], ts.at[1], to_x),
        remote(tl.at[:, c], tl.at[:, c], ts.at[2], ts.at[3], to_s),
    ]
    t_on = remote(tl.at[:, cx], tl.at[:, cx], ts.at[4], ts.at[5], to_s)

    x_copy = remote(xs, xn, os.at[0], os.at[1], to_y)

    def y_copy(i):
        return remote(yo.at[i], yn.at[i], ys.at[0, i], ys.at[1, i], to_y)

    def sent(lo, hi):
        if lo == 1:
            for cp in t_copies + [t_on]:
                cp.wait_send()
        for k in range(lo, hi + 1):
            for cp in c_own(k) + c_fwd(k) + c_sib(k) + c_dia(k):
                cp.wait_send()

    def do(ops):
        for op, k in ops:
            if op == O:
                start_own(k)
            elif op == F:
                wait_first(k)
                for cp in c_fwd(k) + c_sib(k):
                    cp.start()
                if k == 1:
                    arrive(tl.at[:, cx], ts.at[1])
                    t_on.start()
            elif op == D:
                wait_dia(k)
                for cp in c_dia(k)[: 1 if k == STEPS else 2]:
                    cp.start()
            elif op == E:
                b0, bn = halves(k)[1]
                arrive(seg(k, ry, cx, b0, bn), rs.at[DX, k])
                c_dia(k)[1].start()
            elif op == R:
                b0, bn = halves(k)[1]
                arrive(seg(k, ry, csx, b0, bn), rs.at[SE, k])
            elif op == W:
                sent(1, k)
            elif op == S:
                wait_sib(k)
                if k == 1:
                    arrive(tl.at[:, cs], ts.at[3])
                    arrive(tl.at[:, csx], ts.at[5])
                    z_loc.wait()
                if k > SWAP + 1:
                    y_copy(k - SWAP - 2).start()
            elif op == T:
                for cp in t_copies:
                    cp.start()
            elif op == V:
                turn(k)
                if k == 2:
                    t_loc.wait()
                    for q in range(8):
                        tl[q, c] = jnp.concatenate([t_in[4 * q + t] for t in range(4)], axis=1)
            else:
                x_copy.start()

    def point(k, table):
        for kk, ops in table.items():
            @pl.when(k == kk)
            def _(ops=ops):
                do(ops)

    lane = lax.broadcasted_iota(jnp.int32, (128, 128), 1)
    sub = lax.broadcasted_iota(jnp.int32, (128, 128), 0)
    pr, pc = sub // 32, lane // 32
    level1 = (pr // 2 == pc // 2) & (pr < pc)
    level2 = pr // 2 < pc // 2

    def step(k, carry):
        point(k, BEFORE)
        J = STEPS - k
        base = 4 * k * (k - 1)
        acc[...] = jnp.zeros_like(acc)
        for rr in range(2):
            xt[rr, J] = z_in[pl.ds(pl.multiple_of(2048 * rr + 128 * J, 128), 128)].T

        def prepare(m, p):
            m = jnp.minimum(m, k - 1)
            for g in range(12):
                if g < 4:
                    here = [xt[rr, J + m, 32 * g : 32 * g + 32] for rr in range(2)]
                else:
                    tt, cc = divmod(g - 4, 4)
                    here = [land[base + (rr * 4 + cc) * k + m, 32 * tt : 32 * tt + 32] for rr in range(2)]
                for i, part in enumerate(split3(jnp.concatenate(here, axis=1))):
                    lp[p, i, 32 * g : 32 * g + 32] = part
                    if g >= 4:
                        vp[i, m, 32 * g - 128 : 32 * g - 96] = part

        def product(p):
            return mul6([lp[p, i] for i in range(3)], [lp[p, i, 128:384] for i in range(3)], NT)

        def four(i, carry):
            acc[...] += product(0) + product(1)
            prepare(4 * i + 2, 2)
            prepare(4 * i + 3, 3)
            acc[...] += product(2) + product(3)
            prepare(4 * i + 4, 0)
            prepare(4 * i + 5, 1)
            return carry

        fours, left = lax.div(k, 4), lax.rem(k, 4)
        mid = lax.div(fours + 1, 2)
        prepare(0, 0)
        prepare(1, 1)
        lax.fori_loop(0, mid, four, 0)
        point(k, MIDDLE)
        lax.fori_loop(mid, fours, four, 0)

        @pl.when(left == 1)
        def _():
            acc[...] += product(0)

        @pl.when(left >= 2)
        def _():
            acc[...] += product(0) + product(1)

        @pl.when(left == 3)
        def _():
            prepare(k - 1, 2)
            acc[...] += product(2)

        q, h = J // 2, lax.rem(J, 2)

        def diag(tt):
            rows = []
            for cc in range(4):
                t32 = tl[q, cc]
                t32 = jnp.where(h == 0, t32, pltpu.roll(t32, 64, 1))
                shift = (32 * cc - 32 * tt) % 128
                rows.append(pltpu.roll(t32, shift, 1) if shift else t32)
            full = jnp.concatenate(rows, axis=0)
            return jnp.where(pr == pc, full, 0.0)

        halves_t = []
        for tt in range(2):
            g = acc[128 + 128 * tt : 256 + 128 * tt, 128 * tt : 128 * tt + 128]
            t = diag(tt)
            t = t - mulf(t, mulf(jnp.where(level1, g, 0.0), t))
            t = t - mulf(t, mulf(jnp.where(level2, g, 0.0), t))
            halves_t.append(t)
        t1, t2 = halves_t
        t12 = -mulf(t1, mulf(acc[128:256, 128:256], t2))
        w1, w2 = acc[0:128, 0:128], acc[0:128, 128:256]
        w2s = split3(w2)
        y1 = mul6(split3(w1), split3(t1), NT) + mul6(w2s, split3(t12), NT)
        y2 = mul6(w2s, split3(t2), NT)
        y = jnp.concatenate([y1, y2], axis=1)
        for i, part in enumerate(split3(y)):
            yp[i] = part

        @pl.when(k > SWAP)
        def _():
            yo[k - SWAP - 1] = y

        point(k, AFTER)

        def update(m, n):
            ps = [yp[i] for i in range(3)]
            ds = [mul6(ps, [vp[i, m + u] for i in range(3)], NN) for u in range(n)]
            for u, d in enumerate(ds):
                xt[0, J + m + u] = xt[0, J + m + u] - d[:, :128]
                xt[1, J + m + u] = xt[1, J + m + u] - d[:, 128:]

        @pl.when(k < STEPS)
        def _():
            by_four(0, k, update)

        @pl.when(k == SWAP)
        def _():
            for m in range(STEPS - SWAP):
                xt[ry, m] = z_in[pl.ds(pl.multiple_of(2048 * ry + 128 * m, 128), 128)].T

            def stage(m, carry):
                xs[m] = xt[ry, m]
                return carry

            lax.fori_loop(0, STEPS, stage, 0)

        return carry

    lax.fori_loop(1, STEPS + 1, step, 0)

    def half(dst, k, parts, lo, hi, put=None):
        def tiles(m, n):
            ds = [mul6(parts, split3(rows(k, 8 * OFF[k], r, m + u)), NN) for u in range(n)]
            for u, d in enumerate(ds):
                x = dst[STEPS - k + m + u] - d
                if put is None:
                    dst[STEPS - k + m + u] = x
                else:
                    here = pl.ds(pl.multiple_of(128 * (m + u), 128), 128)
                    ob[here, pl.ds(pl.multiple_of(128 * put, 128), 128)] = x.T

        by_four(lo, hi, tiles)

    last = [yp[i] for i in range(3)]
    half(xt.at[r], STEPS, last, 0, 4, r)
    y_copy(REST - 1).start()
    half(xt.at[r], STEPS, last, 4, STEPS, r)
    arrive(xn, os.at[1])
    for i in range(REST):
        arrive(yn.at[i], ys.at[1, i])
        if i < REST - 1:
            half(xn, SWAP + 1 + i, split3(yn[i]), 0, SWAP + 1 + i)
    theirs = split3(yn[REST - 1])
    outs = []
    for i in range(4):
        half(xn, STEPS, theirs, 4 * i, 4 * i + 4, ry)
        here = pl.ds(512 * i, 512)
        outs.append(pltpu.make_async_copy(ob.at[here], out_ref.at[here], rs.at[LO, 9 + i]))
        if i:
            outs[i - 1].start()

    sent(14, STEPS)
    x_copy.wait_send()
    for i in range(REST):
        y_copy(i).wait_send()
    outs[3].start()
    for cp in outs:
        cp.wait()


def solution(mesh):
    def body(v_loc, t_loc, z_loc):
        return pl.pallas_call(
            kernel,
            out_shape=jax.ShapeDtypeStruct((2048, 256), F32),
            in_specs=[pl.BlockSpec(memory_space=pl.ANY)] * 3,
            out_specs=pl.BlockSpec(memory_space=pl.ANY),
            scratch_shapes=[
                pltpu.VMEM((256 * OFF[9], 128), F32),
                pltpu.VMEM((32, 32, 32), F32),
                pltpu.VMEM((4096, 128), F32),
                pltpu.VMEM((2048, 256), F32),
                pltpu.VMEM((8 * OFF[STEPS + 1], 64, 128), F32),
                pltpu.VMEM((8, 4, 32, 128), F32),
                pltpu.VMEM((2, 16, 128, 128), F32),
                pltpu.VMEM((16, 128, 128), F32),
                pltpu.VMEM((16, 128, 128), F32),
                pltpu.VMEM((REST, 128, 256), F32),
                pltpu.VMEM((REST, 128, 256), F32),
                pltpu.VMEM((3, 16, 256, 256), BF16),
                pltpu.VMEM((4, 3, 384, 256), BF16),
                pltpu.VMEM((384, 256), F32),
                pltpu.VMEM((3, 128, 256), BF16),
                pltpu.SemaphoreType.DMA((10, STEPS + 1)),
                pltpu.SemaphoreType.DMA((9, STEPS + 1)),
                pltpu.SemaphoreType.DMA((7,)),
                pltpu.SemaphoreType.DMA((1,)),
                pltpu.SemaphoreType.DMA((4,)),
                pltpu.SemaphoreType.DMA((2, REST)),
            ],
            compiler_params=pltpu.CompilerParams(
                collective_id=0, has_side_effects=True, vmem_limit_bytes=64 * 1024 * 1024 - 65536
            ),
        )(v_loc, t_loc, z_loc)

    return jax.shard_map(
        body,
        mesh=mesh,
        in_specs=(P("row", "col"), P("col", None, None), P(None, ("col", "row"))),
        out_specs=P("row", "col"),
        check_vma=False,
    )
```

```python
import functools

import jax
import jax.numpy as jnp
from jax import lax
from jax.experimental import pallas as pl
from jax.experimental.pallas import tpu as pltpu
from jax.sharding import PartitionSpec as P

MESH = pl.DeviceIdType.MESH
F32, BF16 = jnp.float32, jnp.bfloat16
STEPS = 16
OFF = [k * (k - 1) // 2 for k in range(STEPS + 2)]
NT = (((1,), (1,)), ((), ()))
NN = (((1,), (0,)), ((), ()))
SWAP = 14
REST = STEPS - SWAP
O, F, D, S, T, X, V, E, R, W = range(10)
BEFORE = {k: ((S, k),) for k in range(2, STEPS + 1)}
BEFORE[1] = ((V, 1), (V, 2), (O, 1), (O, 2), (V, 3), (T, 0), (O, 3), (O, 4), (F, 1), (F, 2), (D, 1), (S, 1))
BEFORE[14] = ((F, 15), (S, 14))
BEFORE[15] = ((F, 16), (X, 0), (D, 15), (W, 13), (S, 15))
BEFORE[16] = ((S, 16), (E, 16))
MIDDLE = {k: ((F, k + 2), (O, k + 4)) for k in range(1, 13)}
MIDDLE |= {k: MIDDLE[k] + ((V, (k + 7) // 2),) for k in range(1, 10, 2)}
MIDDLE[16] = ((R, 16),)
AFTER = {k: ((D, k + 1),) for k in (*range(1, 14), 15)}
ALONG_Y = [0, 0, 1, 1, 2, 2, 3, 3, 4, 4, 5, 5, 6, 6, 7, 4, 10]
FX, FY, DX, DY, SO, SX, SY, SD, SE, LO = range(10)
TX, TY, TS, GX, GY, HX, HY, HD, HE = range(9)


def split3(a):
    p1 = a.astype(BF16)
    rest = a - p1.astype(F32)
    p2 = rest.astype(BF16)
    p3 = (rest - p2.astype(F32)).astype(BF16)
    return p1, p2, p3


def mul6(a, b, dims):
    dot = functools.partial(lax.dot_general, dimension_numbers=dims, preferred_element_type=F32)
    return (
        dot(a[0], b[0]) + dot(a[1], b[0]) + dot(a[2], b[0]) + dot(a[0], b[1]) + dot(a[1], b[1]) + dot(a[0], b[2])
    )


def mulf(a, b, dims=NN):
    return mul6(split3(a), split3(b), dims)


def by_four(lo, hi, fn):
    fours = lax.div(hi - lo, 4)

    def four(i, carry):
        fn(lo + 4 * i, 4)
        return carry

    def one(m, carry):
        fn(m, 1)
        return carry

    lax.fori_loop(0, fours, four, 0)
    lax.fori_loop(lo + 4 * fours, hi, one, 0)


def kernel(v_ref, t_ref, z_ref, out_ref, vs_in, t_in, z_in, ob, land, tl, xt, xs, xn, yo, yn, vp, lp, acc, yp, rs, ss, ts, zs, os, ys):
    r, c = lax.axis_index("row"), lax.axis_index("col")
    cs = c + 1 - 2 * lax.rem(c, 2)
    cx = lax.rem(c + 2, 4)
    csx = lax.rem(cs + 2, 4)
    ry = 1 - r
    to_x, to_y, to_s = (r, cx), (ry, c), (r, cs)

    def seg(k, rr, cc, lo=0, n=None):
        return land.at[pl.ds(8 * OFF[k] + (rr * 4 + cc) * k + lo, k if n is None else n)]

    def rows(k, base, rr, m):
        got = [land[base + (rr * 4 + cc) * k + m] for cc in range(4)]
        return jnp.concatenate([g[:32] for g in got] + [g[32:] for g in got], axis=0)

    def remote(src, dst, send, recv, dev):
        return pltpu.make_async_remote_copy(
            src_ref=src, dst_ref=dst, send_sem=send, recv_sem=recv, device_id=dev, device_id_type=MESH
        )

    def halves(k):
        h = ALONG_Y[k]
        return (0, h), (h, k - h)

    def c_own(k):
        mine = seg(k, r, c)
        return [
            remote(mine, mine, ss.at[TX, k], rs.at[FX, k], to_x),
            remote(mine, mine, ss.at[TY, k], rs.at[FY, k], to_y),
            remote(mine, mine, ss.at[TS, k], rs.at[SO, k], to_s),
        ]

    def c_loc(n):
        q = STEPS // 2 - n
        return pltpu.make_async_copy(
            v_ref.at[pl.ds(256 * q, 256 * n), pl.ds(128 * q, 128)], vs_in.at[pl.ds(256 * OFF[n], 256 * n)], rs.at[LO, n]
        )

    def turn(n):
        c_loc(n).wait()
        even, odd = (8 * OFF[k] + (r * 4 + c) * k for k in (2 * n, 2 * n - 1))

        def tile(m, carry):
            t = vs_in[pl.ds(pl.multiple_of(256 * OFF[n] + 128 * m, 128), 128)].T
            land[even + m] = t[:64]

            @pl.when(m > 0)
            def _():
                land[odd + m - 1] = t[64:]

            return carry

        lax.fori_loop(0, 2 * n, tile, 0)

    def c_fwd(k):
        (a0, an), (b0, bn) = halves(k)
        out = []
        if k == STEPS:
            out.append(remote(seg(k, ry, c, a0, an), seg(k, ry, c, a0, an), ss.at[GY, k], rs.at[DY, k], to_x))
        elif an:
            out.append(remote(seg(k, r, cx, a0, an), seg(k, r, cx, a0, an), ss.at[GY, k], rs.at[DY, k], to_y))
        if bn:
            out.append(remote(seg(k, ry, c, b0, bn), seg(k, ry, c, b0, bn), ss.at[GX, k], rs.at[DX, k], to_x))
        return out

    def c_sib(k):
        return [
            remote(seg(k, r, cx), seg(k, r, cx), ss.at[HX, k], rs.at[SX, k], to_s),
            remote(seg(k, ry, c), seg(k, ry, c), ss.at[HY, k], rs.at[SY, k], to_s),
        ]

    def c_dia(k):
        (a0, an), (b0, bn) = halves(k)
        out = []
        if an:
            out.append(remote(seg(k, ry, cx, a0, an), seg(k, ry, cx, a0, an), ss.at[HD, k], rs.at[SD, k], to_s))
        if bn:
            out.append(remote(seg(k, ry, cx, b0, bn), seg(k, ry, cx, b0, bn), ss.at[HE, k], rs.at[SE, k], to_s))
        return out

    def arrive(dst, sem):
        pltpu.make_async_copy(dst, dst, sem).wait()

    def wait_first(k):
        arrive(seg(k, r, cx), rs.at[FX, k])
        arrive(seg(k, ry, c), rs.at[FY, k])

    def wait_dia(k):
        (a0, an), (b0, bn) = halves(k)
        if an:
            arrive(seg(k, ry, cx, a0, an), rs.at[DY, k])
        if bn and k < STEPS:
            arrive(seg(k, ry, cx, b0, bn), rs.at[DX, k])

    def wait_sib(k):
        arrive(seg(k, r, cs), rs.at[SO, k])
        arrive(seg(k, r, csx), rs.at[SX, k])
        arrive(seg(k, ry, cs), rs.at[SY, k])
        (a0, an), (b0, bn) = halves(k)
        if an:
            arrive(seg(k, ry, csx, a0, an), rs.at[SD, k])
        if bn and k < STEPS:
            arrive(seg(k, ry, csx, b0, bn), rs.at[SE, k])

    def start_own(k):
        for cp in c_own(k):
            cp.start()

    t_loc = pltpu.make_async_copy(t_ref, t_in, ts.at[6])
    z_loc = pltpu.make_async_copy(z_ref, z_in, zs.at[0])
    for n in range(1, STEPS // 2 + 1):
        c_loc(n).start()
        if n == 2:
            t_loc.start()
            z_loc.start()
    barrier = pltpu.get_barrier_semaphore()
    for dev in (to_x, to_y, to_s):
        pl.semaphore_signal(barrier, inc=1, device_id=dev, device_id_type=MESH)
    pl.semaphore_wait(barrier, 3)

    t_copies = [
        remote(tl.at[:, c], tl.at[:, c], ts.at[0], ts.at[1], to_x),
        remote(tl.at[:, c], tl.at[:, c], ts.at[2], ts.at[3], to_s),
    ]
    t_on = remote(tl.at[:, cx], tl.at[:, cx], ts.at[4], ts.at[5], to_s)

    x_copy = remote(xs, xn, os.at[0], os.at[1], to_y)

    def y_copy(i):
        return remote(yo.at[i], yn.at[i], ys.at[0, i], ys.at[1, i], to_y)

    def sent(lo, hi):
        if lo == 1:
            for cp in t_copies + [t_on]:
                cp.wait_send()
        for k in range(lo, hi + 1):
            for cp in c_own(k) + c_fwd(k) + c_sib(k) + c_dia(k):
                cp.wait_send()

    def do(ops):
        for op, k in ops:
            if op == O:
                start_own(k)
            elif op == F:
                wait_first(k)
                for cp in c_fwd(k) + c_sib(k):
                    cp.start()
                if k == 1:
                    arrive(tl.at[:, cx], ts.at[1])
                    t_on.start()
            elif op == D:
                wait_dia(k)
                for cp in c_dia(k)[: 1 if k == STEPS else 2]:
                    cp.start()
            elif op == E:
                b0, bn = halves(k)[1]
                arrive(seg(k, ry, cx, b0, bn), rs.at[DX, k])
                c_dia(k)[1].start()
            elif op == R:
                b0, bn = halves(k)[1]
                arrive(seg(k, ry, csx, b0, bn), rs.at[SE, k])
            elif op == W:
                sent(1, k)
            elif op == S:
                wait_sib(k)
                if k == 1:
                    arrive(tl.at[:, cs], ts.at[3])
                    arrive(tl.at[:, csx], ts.at[5])
                    z_loc.wait()
                if k > SWAP + 1:
                    y_copy(k - SWAP - 2).start()
            elif op == T:
                for cp in t_copies:
                    cp.start()
            elif op == V:
                turn(k)
                if k == 2:
                    t_loc.wait()
                    for q in range(8):
                        tl[q, c] = jnp.concatenate([t_in[4 * q + t] for t in range(4)], axis=1)
            else:
                x_copy.start()

    def point(k, table):
        for kk, ops in table.items():
            @pl.when(k == kk)
            def _(ops=ops):
                do(ops)

    lane = lax.broadcasted_iota(jnp.int32, (128, 128), 1)
    sub = lax.broadcasted_iota(jnp.int32, (128, 128), 0)
    pr, pc = sub // 32, lane // 32
    level1 = (pr // 2 == pc // 2) & (pr < pc)
    level2 = pr // 2 < pc // 2

    def step(k, carry):
        point(k, BEFORE)
        J = STEPS - k
        base = 4 * k * (k - 1)
        acc[...] = jnp.zeros_like(acc)
        for rr in range(2):
            xt[rr, J] = z_in[pl.ds(pl.multiple_of(2048 * rr + 128 * J, 128), 128)].T

        def prepare(m, p):
            m = jnp.minimum(m, k - 1)
            for g in range(12):
                if g < 4:
                    here = [xt[rr, J + m, 32 * g : 32 * g + 32] for rr in range(2)]
                else:
                    tt, cc = divmod(g - 4, 4)
                    here = [land[base + (rr * 4 + cc) * k + m, 32 * tt : 32 * tt + 32] for rr in range(2)]
                for i, part in enumerate(split3(jnp.concatenate(here, axis=1))):
                    lp[p, i, 32 * g : 32 * g + 32] = part
                    if g >= 4:
                        vp[i, m, 32 * g - 128 : 32 * g - 96] = part

        def product(p):
            return mul6([lp[p, i] for i in range(3)], [lp[p, i, 128:384] for i in range(3)], NT)

        def four(i, carry):
            acc[...] += product(0) + product(1)
            prepare(4 * i + 2, 2)
            prepare(4 * i + 3, 3)
            acc[...] += product(2) + product(3)
            prepare(4 * i + 4, 0)
            prepare(4 * i + 5, 1)
            return carry

        fours, left = lax.div(k, 4), lax.rem(k, 4)
        mid = lax.div(fours + 1, 2)
        prepare(0, 0)
        prepare(1, 1)
        lax.fori_loop(0, mid, four, 0)
        point(k, MIDDLE)
        lax.fori_loop(mid, fours, four, 0)

        @pl.when(left == 1)
        def _():
            acc[...] += product(0)

        @pl.when(left >= 2)
        def _():
            acc[...] += product(0) + product(1)

        @pl.when(left == 3)
        def _():
            prepare(k - 1, 2)
            acc[...] += product(2)

        q, h = J // 2, lax.rem(J, 2)

        def diag(tt):
            rows = []
            for cc in range(4):
                t32 = tl[q, cc]
                t32 = jnp.where(h == 0, t32, pltpu.roll(t32, 64, 1))
                shift = (32 * cc - 32 * tt) % 128
                rows.append(pltpu.roll(t32, shift, 1) if shift else t32)
            full = jnp.concatenate(rows, axis=0)
            return jnp.where(pr == pc, full, 0.0)

        halves_t = []
        for tt in range(2):
            g = acc[128 + 128 * tt : 256 + 128 * tt, 128 * tt : 128 * tt + 128]
            t = diag(tt)
            t = t - mulf(t, mulf(jnp.where(level1, g, 0.0), t))
            t = t - mulf(t, mulf(jnp.where(level2, g, 0.0), t))
            halves_t.append(t)
        t1, t2 = halves_t
        t12 = -mulf(t1, mulf(acc[128:256, 128:256], t2))
        w1, w2 = acc[0:128, 0:128], acc[0:128, 128:256]
        w2s = split3(w2)
        y1 = mul6(split3(w1), split3(t1), NT) + mul6(w2s, split3(t12), NT)
        y2 = mul6(w2s, split3(t2), NT)
        y = jnp.concatenate([y1, y2], axis=1)
        for i, part in enumerate(split3(y)):
            yp[i] = part

        @pl.when(k > SWAP)
        def _():
            yo[k - SWAP - 1] = y

        point(k, AFTER)

        def update(m, n):
            ps = [yp[i] for i in range(3)]
            ds = [mul6(ps, [vp[i, m + u] for i in range(3)], NN) for u in range(n)]
            for u, d in enumerate(ds):
                xt[0, J + m + u] = xt[0, J + m + u] - d[:, :128]
                xt[1, J + m + u] = xt[1, J + m + u] - d[:, 128:]

        @pl.when(k < STEPS)
        def _():
            by_four(0, k, update)

        @pl.when(k == SWAP)
        def _():
            for m in range(STEPS - SWAP):
                xt[ry, m] = z_in[pl.ds(pl.multiple_of(2048 * ry + 128 * m, 128), 128)].T

            def stage(m, carry):
                xs[m] = xt[ry, m]
                return carry

            lax.fori_loop(0, STEPS, stage, 0)

        return carry

    lax.fori_loop(1, STEPS + 1, step, 0)

    def half(dst, k, parts, lo, hi, put=None):
        def tiles(m, n):
            ds = [mul6(parts, split3(rows(k, 8 * OFF[k], r, m + u)), NN) for u in range(n)]
            for u, d in enumerate(ds):
                x = dst[STEPS - k + m + u] - d
                if put is None:
                    dst[STEPS - k + m + u] = x
                else:
                    here = pl.ds(pl.multiple_of(128 * (m + u), 128), 128)
                    ob[here, pl.ds(pl.multiple_of(128 * put, 128), 128)] = x.T

        by_four(lo, hi, tiles)

    last = [yp[i] for i in range(3)]
    half(xt.at[r], STEPS, last, 0, 4, r)
    y_copy(REST - 1).start()
    half(xt.at[r], STEPS, last, 4, STEPS, r)
    arrive(xn, os.at[1])
    for i in range(REST):
        arrive(yn.at[i], ys.at[1, i])
        if i < REST - 1:
            half(xn, SWAP + 1 + i, split3(yn[i]), 0, SWAP + 1 + i)
    theirs = split3(yn[REST - 1])
    outs = []
    for i in range(4):
        half(xn, STEPS, theirs, 4 * i, 4 * i + 4, ry)
        here = pl.ds(512 * i, 512)
        outs.append(pltpu.make_async_copy(ob.at[here], out_ref.at[here], rs.at[LO, 9 + i]))
        if i:
            outs[i - 1].start()

    sent(14, STEPS)
    x_copy.wait_send()
    for i in range(REST):
        y_copy(i).wait_send()
    outs[3].start()
    for cp in outs:
        cp.wait()


def solution(mesh):
    def body(v_loc, t_loc, z_loc):
        return pl.pallas_call(
            kernel,
            out_shape=jax.ShapeDtypeStruct((2048, 256), F32),
            in_specs=[pl.BlockSpec(memory_space=pl.ANY)] * 3,
            out_specs=pl.BlockSpec(memory_space=pl.ANY),
            scratch_shapes=[
                pltpu.VMEM((256 * OFF[9], 128), F32),
                pltpu.VMEM((32, 32, 32), F32),
                pltpu.VMEM((4096, 128), F32),
                pltpu.VMEM((2048, 256), F32),
                pltpu.VMEM((8 * OFF[STEPS + 1], 64, 128), F32),
                pltpu.VMEM((8, 4, 32, 128), F32),
                pltpu.VMEM((2, 16, 128, 128), F32),
                pltpu.VMEM((16, 128, 128), F32),
                pltpu.VMEM((16, 128, 128), F32),
                pltpu.VMEM((REST, 128, 256), F32),
                pltpu.VMEM((REST, 128, 256), F32),
                pltpu.VMEM((3, 16, 256, 256), BF16),
                pltpu.VMEM((4, 3, 384, 256), BF16),
                pltpu.VMEM((384, 256), F32),
                pltpu.VMEM((3, 128, 256), BF16),
                pltpu.SemaphoreType.DMA((10, STEPS + 1)),
                pltpu.SemaphoreType.DMA((9, STEPS + 1)),
                pltpu.SemaphoreType.DMA((7,)),
                pltpu.SemaphoreType.DMA((1,)),
                pltpu.SemaphoreType.DMA((4,)),
                pltpu.SemaphoreType.DMA((2, REST)),
            ],
            compiler_params=pltpu.CompilerParams(
                collective_id=0, has_side_effects=True, vmem_limit_bytes=64 * 1024 * 1024 - 65536
            ),
        )(v_loc, t_loc, z_loc)

    return jax.shard_map(
        body,
        mesh=mesh,
        in_specs=(P("row", "col"), P("col", None, None), P(None, ("col", "row"))),
        out_specs=P("row", "col"),
        check_vma=False,
    )
```

```python
import functools

import jax
import jax.numpy as jnp
from jax import lax
from jax.experimental import pallas as pl
from jax.experimental.pallas import tpu as pltpu
from jax.sharding import PartitionSpec as P

MESH = pl.DeviceIdType.MESH
F32, BF16 = jnp.float32, jnp.bfloat16
STEPS = 16
OFF = [k * (k - 1) // 2 for k in range(STEPS + 2)]
NT = (((1,), (1,)), ((), ()))
NN = (((1,), (0,)), ((), ()))
SWAP = 14
REST = STEPS - SWAP
O, F, D, S, T, X, V, E, R, W = range(10)
BEFORE = {k: ((S, k),) for k in range(2, STEPS + 1)}
BEFORE[1] = ((V, 1), (V, 2), (O, 1), (O, 2), (V, 3), (T, 0), (O, 3), (O, 4), (F, 1), (F, 2), (D, 1), (S, 1))
BEFORE[14] = ((F, 15), (S, 14))
BEFORE[15] = ((F, 16), (X, 0), (D, 15), (W, 13), (S, 15))
BEFORE[16] = ((S, 16), (E, 16))
MIDDLE = {k: ((F, k + 2), (O, k + 4)) for k in range(1, 13)}
MIDDLE |= {k: MIDDLE[k] + ((V, (k + 7) // 2),) for k in range(1, 10, 2)}
MIDDLE[16] = ((R, 16),)
AFTER = {k: ((D, k + 1),) for k in (*range(1, 14), 15)}
ALONG_Y = [0, 0, 1, 1, 2, 2, 3, 3, 4, 5, 5, 6, 6, 7, 7, 7, 10]
FX, FY, DX, DY, SO, SX, SY, SD, SE, LO = range(10)
TX, TY, TS, GX, GY, HX, HY, HD, HE = range(9)


def split3(a):
    p1 = a.astype(BF16)
    rest = a - p1.astype(F32)
    p2 = rest.astype(BF16)
    p3 = (rest - p2.astype(F32)).astype(BF16)
    return p1, p2, p3


def mul6(a, b, dims):
    dot = functools.partial(lax.dot_general, dimension_numbers=dims, preferred_element_type=F32)
    return (
        dot(a[0], b[0]) + dot(a[1], b[0]) + dot(a[2], b[0]) + dot(a[0], b[1]) + dot(a[1], b[1]) + dot(a[0], b[2])
    )


def mulf(a, b, dims=NN):
    return mul6(split3(a), split3(b), dims)


def by_four(lo, hi, fn):
    fours = lax.div(hi - lo, 4)

    def four(i, carry):
        fn(lo + 4 * i, 4)
        return carry

    def one(m, carry):
        fn(m, 1)
        return carry

    lax.fori_loop(0, fours, four, 0)
    lax.fori_loop(lo + 4 * fours, hi, one, 0)


def kernel(v_ref, t_ref, z_ref, out_ref, vs_in, t_in, z_in, ob, land, tl, xt, xs, xn, yo, yn, vp, lp, acc, yp, rs, ss, ts, zs, os, ys):
    r, c = lax.axis_index("row"), lax.axis_index("col")
    cs = c + 1 - 2 * lax.rem(c, 2)
    cx = lax.rem(c + 2, 4)
    csx = lax.rem(cs + 2, 4)
    ry = 1 - r
    to_x, to_y, to_s = (r, cx), (ry, c), (r, cs)

    def seg(k, rr, cc, lo=0, n=None):
        return land.at[pl.ds(8 * OFF[k] + (rr * 4 + cc) * k + lo, k if n is None else n)]

    def rows(k, base, rr, m):
        got = [land[base + (rr * 4 + cc) * k + m] for cc in range(4)]
        return jnp.concatenate([g[:32] for g in got] + [g[32:] for g in got], axis=0)

    def remote(src, dst, send, recv, dev):
        return pltpu.make_async_remote_copy(
            src_ref=src, dst_ref=dst, send_sem=send, recv_sem=recv, device_id=dev, device_id_type=MESH
        )

    def halves(k):
        h = ALONG_Y[k]
        return (0, h), (h, k - h)

    def c_own(k):
        mine = seg(k, r, c)
        return [
            remote(mine, mine, ss.at[TX, k], rs.at[FX, k], to_x),
            remote(mine, mine, ss.at[TY, k], rs.at[FY, k], to_y),
            remote(mine, mine, ss.at[TS, k], rs.at[SO, k], to_s),
        ]

    def c_loc(n):
        q = STEPS // 2 - n
        return pltpu.make_async_copy(
            v_ref.at[pl.ds(256 * q, 256 * n), pl.ds(128 * q, 128)], vs_in.at[pl.ds(256 * OFF[n], 256 * n)], rs.at[LO, n]
        )

    def turn(n):
        c_loc(n).wait()
        even, odd = (8 * OFF[k] + (r * 4 + c) * k for k in (2 * n, 2 * n - 1))

        def tile(m, carry):
            t = vs_in[pl.ds(pl.multiple_of(256 * OFF[n] + 128 * m, 128), 128)].T
            land[even + m] = t[:64]

            @pl.when(m > 0)
            def _():
                land[odd + m - 1] = t[64:]

            return carry

        lax.fori_loop(0, 2 * n, tile, 0)

    def c_fwd(k):
        (a0, an), (b0, bn) = halves(k)
        out = []
        if k == STEPS:
            out.append(remote(seg(k, ry, c, a0, an), seg(k, ry, c, a0, an), ss.at[GY, k], rs.at[DY, k], to_x))
        elif an:
            out.append(remote(seg(k, r, cx, a0, an), seg(k, r, cx, a0, an), ss.at[GY, k], rs.at[DY, k], to_y))
        if bn:
            out.append(remote(seg(k, ry, c, b0, bn), seg(k, ry, c, b0, bn), ss.at[GX, k], rs.at[DX, k], to_x))
        return out

    def c_sib(k):
        return [
            remote(seg(k, r, cx), seg(k, r, cx), ss.at[HX, k], rs.at[SX, k], to_s),
            remote(seg(k, ry, c), seg(k, ry, c), ss.at[HY, k], rs.at[SY, k], to_s),
        ]

    def c_dia(k):
        (a0, an), (b0, bn) = halves(k)
        out = []
        if an:
            out.append(remote(seg(k, ry, cx, a0, an), seg(k, ry, cx, a0, an), ss.at[HD, k], rs.at[SD, k], to_s))
        if bn:
            out.append(remote(seg(k, ry, cx, b0, bn), seg(k, ry, cx, b0, bn), ss.at[HE, k], rs.at[SE, k], to_s))
        return out

    def arrive(dst, sem):
        pltpu.make_async_copy(dst, dst, sem).wait()

    def wait_first(k):
        arrive(seg(k, r, cx), rs.at[FX, k])
        arrive(seg(k, ry, c), rs.at[FY, k])

    def wait_dia(k):
        (a0, an), (b0, bn) = halves(k)
        if an:
            arrive(seg(k, ry, cx, a0, an), rs.at[DY, k])
        if bn and k < STEPS:
            arrive(seg(k, ry, cx, b0, bn), rs.at[DX, k])

    def wait_sib(k):
        arrive(seg(k, r, cs), rs.at[SO, k])
        arrive(seg(k, r, csx), rs.at[SX, k])
        arrive(seg(k, ry, cs), rs.at[SY, k])
        (a0, an), (b0, bn) = halves(k)
        if an:
            arrive(seg(k, ry, csx, a0, an), rs.at[SD, k])
        if bn and k < STEPS:
            arrive(seg(k, ry, csx, b0, bn), rs.at[SE, k])

    def start_own(k):
        for cp in c_own(k):
            cp.start()

    t_loc = pltpu.make_async_copy(t_ref, t_in, ts.at[6])
    z_loc = pltpu.make_async_copy(z_ref, z_in, zs.at[0])
    for n in range(1, STEPS // 2 + 1):
        c_loc(n).start()
        if n == 2:
            t_loc.start()
            z_loc.start()
    barrier = pltpu.get_barrier_semaphore()
    for dev in (to_x, to_y, to_s):
        pl.semaphore_signal(barrier, inc=1, device_id=dev, device_id_type=MESH)
    pl.semaphore_wait(barrier, 3)

    t_copies = [
        remote(tl.at[:, c], tl.at[:, c], ts.at[0], ts.at[1], to_x),
        remote(tl.at[:, c], tl.at[:, c], ts.at[2], ts.at[3], to_s),
    ]
    t_on = remote(tl.at[:, cx], tl.at[:, cx], ts.at[4], ts.at[5], to_s)

    x_copy = remote(xs, xn, os.at[0], os.at[1], to_y)

    def y_copy(i):
        return remote(yo.at[i], yn.at[i], ys.at[0, i], ys.at[1, i], to_y)

    def sent(lo, hi):
        if lo == 1:
            for cp in t_copies + [t_on]:
                cp.wait_send()
        for k in range(lo, hi + 1):
            for cp in c_own(k) + c_fwd(k) + c_sib(k) + c_dia(k):
                cp.wait_send()

    def do(ops):
        for op, k in ops:
            if op == O:
                start_own(k)
            elif op == F:
                wait_first(k)
                for cp in c_fwd(k) + c_sib(k):
                    cp.start()
                if k == 1:
                    arrive(tl.at[:, cx], ts.at[1])
                    t_on.start()
            elif op == D:
                wait_dia(k)
                for cp in c_dia(k)[: 1 if k == STEPS else 2]:
                    cp.start()
            elif op == E:
                b0, bn = halves(k)[1]
                arrive(seg(k, ry, cx, b0, bn), rs.at[DX, k])
                c_dia(k)[1].start()
            elif op == R:
                b0, bn = halves(k)[1]
                arrive(seg(k, ry, csx, b0, bn), rs.at[SE, k])
            elif op == W:
                sent(1, k)
            elif op == S:
                wait_sib(k)
                if k == 1:
                    arrive(tl.at[:, cs], ts.at[3])
                    arrive(tl.at[:, csx], ts.at[5])
                    z_loc.wait()
                if k > SWAP + 1:
                    y_copy(k - SWAP - 2).start()
            elif op == T:
                for cp in t_copies:
                    cp.start()
            elif op == V:
                turn(k)
                if k == 2:
                    t_loc.wait()
                    for q in range(8):
                        tl[q, c] = jnp.concatenate([t_in[4 * q + t] for t in range(4)], axis=1)
            else:
                x_copy.start()

    def point(k, table):
        for kk, ops in table.items():
            @pl.when(k == kk)
            def _(ops=ops):
                do(ops)

    lane = lax.broadcasted_iota(jnp.int32, (128, 128), 1)
    sub = lax.broadcasted_iota(jnp.int32, (128, 128), 0)
    pr, pc = sub // 32, lane // 32
    level1 = (pr // 2 == pc // 2) & (pr < pc)
    level2 = pr // 2 < pc // 2

    def step(k, carry):
        point(k, BEFORE)
        J = STEPS - k
        base = 4 * k * (k - 1)
        acc[...] = jnp.zeros_like(acc)
        for rr in range(2):
            xt[rr, J] = z_in[pl.ds(pl.multiple_of(2048 * rr + 128 * J, 128), 128)].T

        def prepare(m, p):
            m = jnp.minimum(m, k - 1)
            for g in range(12):
                if g < 4:
                    here = [xt[rr, J + m, 32 * g : 32 * g + 32] for rr in range(2)]
                else:
                    tt, cc = divmod(g - 4, 4)
                    here = [land[base + (rr * 4 + cc) * k + m, 32 * tt : 32 * tt + 32] for rr in range(2)]
                for i, part in enumerate(split3(jnp.concatenate(here, axis=1))):
                    lp[p, i, 32 * g : 32 * g + 32] = part
                    if g >= 4:
                        vp[i, m, 32 * g - 128 : 32 * g - 96] = part

        def product(p):
            return mul6([lp[p, i] for i in range(3)], [lp[p, i, 128:384] for i in range(3)], NT)

        def four(i, carry):
            acc[...] += product(0) + product(1)
            prepare(4 * i + 2, 2)
            prepare(4 * i + 3, 3)
            acc[...] += product(2) + product(3)
            prepare(4 * i + 4, 0)
            prepare(4 * i + 5, 1)
            return carry

        fours, left = lax.div(k, 4), lax.rem(k, 4)
        mid = lax.div(fours + 1, 2)
        prepare(0, 0)
        prepare(1, 1)
        lax.fori_loop(0, mid, four, 0)
        point(k, MIDDLE)
        lax.fori_loop(mid, fours, four, 0)

        @pl.when(left == 1)
        def _():
            acc[...] += product(0)

        @pl.when(left >= 2)
        def _():
            acc[...] += product(0) + product(1)

        @pl.when(left == 3)
        def _():
            prepare(k - 1, 2)
            acc[...] += product(2)

        q, h = J // 2, lax.rem(J, 2)

        def diag(tt):
            rows = []
            for cc in range(4):
                t32 = tl[q, cc]
                t32 = jnp.where(h == 0, t32, pltpu.roll(t32, 64, 1))
                shift = (32 * cc - 32 * tt) % 128
                rows.append(pltpu.roll(t32, shift, 1) if shift else t32)
            full = jnp.concatenate(rows, axis=0)
            return jnp.where(pr == pc, full, 0.0)

        halves_t = []
        for tt in range(2):
            g = acc[128 + 128 * tt : 256 + 128 * tt, 128 * tt : 128 * tt + 128]
            t = diag(tt)
            t = t - mulf(t, mulf(jnp.where(level1, g, 0.0), t))
            t = t - mulf(t, mulf(jnp.where(level2, g, 0.0), t))
            halves_t.append(t)
        t1, t2 = halves_t
        t12 = -mulf(t1, mulf(acc[128:256, 128:256], t2))
        w1, w2 = acc[0:128, 0:128], acc[0:128, 128:256]
        w2s = split3(w2)
        y1 = mul6(split3(w1), split3(t1), NT) + mul6(w2s, split3(t12), NT)
        y2 = mul6(w2s, split3(t2), NT)
        y = jnp.concatenate([y1, y2], axis=1)
        for i, part in enumerate(split3(y)):
            yp[i] = part

        @pl.when(k > SWAP)
        def _():
            yo[k - SWAP - 1] = y

        point(k, AFTER)

        def update(m, n):
            ps = [yp[i] for i in range(3)]
            ds = [mul6(ps, [vp[i, m + u] for i in range(3)], NN) for u in range(n)]
            for u, d in enumerate(ds):
                xt[0, J + m + u] = xt[0, J + m + u] - d[:, :128]
                xt[1, J + m + u] = xt[1, J + m + u] - d[:, 128:]

        @pl.when(k < STEPS)
        def _():
            by_four(0, k, update)

        @pl.when(k == SWAP)
        def _():
            for m in range(STEPS - SWAP):
                xt[ry, m] = z_in[pl.ds(pl.multiple_of(2048 * ry + 128 * m, 128), 128)].T

            def stage(m, carry):
                xs[m] = xt[ry, m]
                return carry

            lax.fori_loop(0, STEPS, stage, 0)

        return carry

    lax.fori_loop(1, STEPS + 1, step, 0)

    def half(dst, k, parts, lo, hi, put=None):
        def tiles(m, n):
            ds = [mul6(parts, split3(rows(k, 8 * OFF[k], r, m + u)), NN) for u in range(n)]
            for u, d in enumerate(ds):
                x = dst[STEPS - k + m + u] - d
                if put is None:
                    dst[STEPS - k + m + u] = x
                else:
                    here = pl.ds(pl.multiple_of(128 * (m + u), 128), 128)
                    ob[here, pl.ds(pl.multiple_of(128 * put, 128), 128)] = x.T

        by_four(lo, hi, tiles)

    last = [yp[i] for i in range(3)]
    half(xt.at[r], STEPS, last, 0, 4, r)
    y_copy(REST - 1).start()
    half(xt.at[r], STEPS, last, 4, STEPS, r)
    arrive(xn, os.at[1])
    for i in range(REST):
        arrive(yn.at[i], ys.at[1, i])
        if i < REST - 1:
            half(xn, SWAP + 1 + i, split3(yn[i]), 0, SWAP + 1 + i)
    theirs = split3(yn[REST - 1])
    outs = []
    for i in range(4):
        half(xn, STEPS, theirs, 4 * i, 4 * i + 4, ry)
        here = pl.ds(512 * i, 512)
        outs.append(pltpu.make_async_copy(ob.at[here], out_ref.at[here], rs.at[LO, 9 + i]))
        if i:
            outs[i - 1].start()

    sent(14, STEPS)
    x_copy.wait_send()
    for i in range(REST):
        y_copy(i).wait_send()
    outs[3].start()
    for cp in outs:
        cp.wait()


def solution(mesh):
    def body(v_loc, t_loc, z_loc):
        return pl.pallas_call(
            kernel,
            out_shape=jax.ShapeDtypeStruct((2048, 256), F32),
            in_specs=[pl.BlockSpec(memory_space=pl.ANY)] * 3,
            out_specs=pl.BlockSpec(memory_space=pl.ANY),
            scratch_shapes=[
                pltpu.VMEM((256 * OFF[9], 128), F32),
                pltpu.VMEM((32, 32, 32), F32),
                pltpu.VMEM((4096, 128), F32),
                pltpu.VMEM((2048, 256), F32),
                pltpu.VMEM((8 * OFF[STEPS + 1], 64, 128), F32),
                pltpu.VMEM((8, 4, 32, 128), F32),
                pltpu.VMEM((2, 16, 128, 128), F32),
                pltpu.VMEM((16, 128, 128), F32),
                pltpu.VMEM((16, 128, 128), F32),
                pltpu.VMEM((REST, 128, 256), F32),
                pltpu.VMEM((REST, 128, 256), F32),
                pltpu.VMEM((3, 16, 256, 256), BF16),
                pltpu.VMEM((4, 3, 384, 256), BF16),
                pltpu.VMEM((384, 256), F32),
                pltpu.VMEM((3, 128, 256), BF16),
                pltpu.SemaphoreType.DMA((10, STEPS + 1)),
                pltpu.SemaphoreType.DMA((9, STEPS + 1)),
                pltpu.SemaphoreType.DMA((7,)),
                pltpu.SemaphoreType.DMA((1,)),
                pltpu.SemaphoreType.DMA((4,)),
                pltpu.SemaphoreType.DMA((2, REST)),
            ],
            compiler_params=pltpu.CompilerParams(
                collective_id=0, has_side_effects=True, vmem_limit_bytes=64 * 1024 * 1024 - 65536
            ),
        )(v_loc, t_loc, z_loc)

    return jax.shard_map(
        body,
        mesh=mesh,
        in_specs=(P("row", "col"), P("col", None, None), P(None, ("col", "row"))),
        out_specs=P("row", "col"),
        check_vma=False,
    )
```

```python
import functools

import jax
import jax.numpy as jnp
from jax import lax
from jax.experimental import pallas as pl
from jax.experimental.pallas import tpu as pltpu
from jax.sharding import PartitionSpec as P

MESH = pl.DeviceIdType.MESH
F32, BF16 = jnp.float32, jnp.bfloat16
STEPS = 16
OFF = [k * (k - 1) // 2 for k in range(STEPS + 2)]
NT = (((1,), (1,)), ((), ()))
NN = (((1,), (0,)), ((), ()))
SWAP = 14
REST = STEPS - SWAP
O, F, D, S, T, X, V, E, R, W = range(10)
BEFORE = {k: ((S, k),) for k in range(2, STEPS + 1)}
BEFORE[1] = ((V, 1), (V, 2), (O, 1), (O, 2), (V, 3), (T, 0), (O, 3), (O, 4), (F, 1), (F, 2), (D, 1), (S, 1))
BEFORE[14] = ((F, 15), (S, 14))
BEFORE[15] = ((F, 16), (X, 0), (D, 15), (W, 13), (S, 15))
BEFORE[16] = ((S, 16),)
MIDDLE = {k: ((F, k + 2), (O, k + 4)) for k in range(1, 13)}
MIDDLE |= {k: MIDDLE[k] + ((V, (k + 7) // 2),) for k in range(1, 10, 2)}
MIDDLE[16] = ((E, 16), (R, 16))
AFTER = {k: ((D, k + 1),) for k in (*range(1, 14), 15)}
ALONG_Y = [0, 0, 1, 1, 2, 2, 3, 3, 4, 4, 5, 5, 6, 6, 7, 7, 10]
FX, FY, DX, DY, SO, SX, SY, SD, SE, LO = range(10)
TX, TY, TS, GX, GY, HX, HY, HD, HE = range(9)


def split3(a):
    p1 = a.astype(BF16)
    rest = a - p1.astype(F32)
    p2 = rest.astype(BF16)
    p3 = (rest - p2.astype(F32)).astype(BF16)
    return p1, p2, p3


def mul6(a, b, dims):
    dot = functools.partial(lax.dot_general, dimension_numbers=dims, preferred_element_type=F32)
    return (
        dot(a[0], b[0]) + dot(a[1], b[0]) + dot(a[2], b[0]) + dot(a[0], b[1]) + dot(a[1], b[1]) + dot(a[0], b[2])
    )


def mulf(a, b, dims=NN):
    return mul6(split3(a), split3(b), dims)


def by_four(lo, hi, fn):
    fours = lax.div(hi - lo, 4)

    def four(i, carry):
        fn(lo + 4 * i, 4)
        return carry

    def one(m, carry):
        fn(m, 1)
        return carry

    lax.fori_loop(0, fours, four, 0)
    lax.fori_loop(lo + 4 * fours, hi, one, 0)


def kernel(v_ref, t_ref, z_ref, out_ref, vs_in, t_in, z_in, ob, land, tl, xt, xs, xn, yo, yn, vp, lp, acc, yp, rs, ss, ts, zs, os, ys):
    r, c = lax.axis_index("row"), lax.axis_index("col")
    cs = c + 1 - 2 * lax.rem(c, 2)
    cx = lax.rem(c + 2, 4)
    csx = lax.rem(cs + 2, 4)
    ry = 1 - r
    to_x, to_y, to_s = (r, cx), (ry, c), (r, cs)

    def seg(k, rr, cc, lo=0, n=None):
        return land.at[pl.ds(8 * OFF[k] + (rr * 4 + cc) * k + lo, k if n is None else n)]

    def rows(k, base, rr, m):
        got = [land[base + (rr * 4 + cc) * k + m] for cc in range(4)]
        return jnp.concatenate([g[:32] for g in got] + [g[32:] for g in got], axis=0)

    def remote(src, dst, send, recv, dev):
        return pltpu.make_async_remote_copy(
            src_ref=src, dst_ref=dst, send_sem=send, recv_sem=recv, device_id=dev, device_id_type=MESH
        )

    def halves(k):
        h = ALONG_Y[k]
        return (0, h), (h, k - h)

    def c_own(k):
        mine = seg(k, r, c)
        return [
            remote(mine, mine, ss.at[TX, k], rs.at[FX, k], to_x),
            remote(mine, mine, ss.at[TY, k], rs.at[FY, k], to_y),
            remote(mine, mine, ss.at[TS, k], rs.at[SO, k], to_s),
        ]

    def c_loc(n):
        q = STEPS // 2 - n
        return pltpu.make_async_copy(
            v_ref.at[pl.ds(256 * q, 256 * n), pl.ds(128 * q, 128)], vs_in.at[pl.ds(256 * OFF[n], 256 * n)], rs.at[LO, n]
        )

    def turn(n):
        c_loc(n).wait()
        even, odd = (8 * OFF[k] + (r * 4 + c) * k for k in (2 * n, 2 * n - 1))

        def tile(m, carry):
            t = vs_in[pl.ds(pl.multiple_of(256 * OFF[n] + 128 * m, 128), 128)].T
            land[even + m] = t[:64]

            @pl.when(m > 0)
            def _():
                land[odd + m - 1] = t[64:]

            return carry

        lax.fori_loop(0, 2 * n, tile, 0)

    def c_fwd(k):
        (a0, an), (b0, bn) = halves(k)
        out = []
        if k == STEPS:
            out.append(remote(seg(k, ry, c, a0, an), seg(k, ry, c, a0, an), ss.at[GY, k], rs.at[DY, k], to_x))
        elif an:
            out.append(remote(seg(k, r, cx, a0, an), seg(k, r, cx, a0, an), ss.at[GY, k], rs.at[DY, k], to_y))
        if bn:
            out.append(remote(seg(k, ry, c, b0, bn), seg(k, ry, c, b0, bn), ss.at[GX, k], rs.at[DX, k], to_x))
        return out

    def c_sib(k):
        return [
            remote(seg(k, r, cx), seg(k, r, cx), ss.at[HX, k], rs.at[SX, k], to_s),
            remote(seg(k, ry, c), seg(k, ry, c), ss.at[HY, k], rs.at[SY, k], to_s),
        ]

    def c_dia(k):
        (a0, an), (b0, bn) = halves(k)
        out = []
        if an:
            out.append(remote(seg(k, ry, cx, a0, an), seg(k, ry, cx, a0, an), ss.at[HD, k], rs.at[SD, k], to_s))
        if bn:
            out.append(remote(seg(k, ry, cx, b0, bn), seg(k, ry, cx, b0, bn), ss.at[HE, k], rs.at[SE, k], to_s))
        return out

    def arrive(dst, sem):
        pltpu.make_async_copy(dst, dst, sem).wait()

    def wait_first(k):
        arrive(seg(k, r, cx), rs.at[FX, k])
        arrive(seg(k, ry, c), rs.at[FY, k])

    def wait_dia(k):
        (a0, an), (b0, bn) = halves(k)
        if an:
            arrive(seg(k, ry, cx, a0, an), rs.at[DY, k])
        if bn and k < STEPS:
            arrive(seg(k, ry, cx, b0, bn), rs.at[DX, k])

    def wait_sib(k):
        arrive(seg(k, r, cs), rs.at[SO, k])
        arrive(seg(k, r, csx), rs.at[SX, k])
        arrive(seg(k, ry, cs), rs.at[SY, k])
        (a0, an), (b0, bn) = halves(k)
        if an:
            arrive(seg(k, ry, csx, a0, an), rs.at[SD, k])
        if bn and k < STEPS:
            arrive(seg(k, ry, csx, b0, bn), rs.at[SE, k])

    def start_own(k):
        for cp in c_own(k):
            cp.start()

    t_loc = pltpu.make_async_copy(t_ref, t_in, ts.at[6])
    z_loc = pltpu.make_async_copy(z_ref, z_in, zs.at[0])
    for n in range(1, STEPS // 2 + 1):
        c_loc(n).start()
        if n == 2:
            t_loc.start()
            z_loc.start()
    barrier = pltpu.get_barrier_semaphore()
    for dev in (to_x, to_y, to_s):
        pl.semaphore_signal(barrier, inc=1, device_id=dev, device_id_type=MESH)
    pl.semaphore_wait(barrier, 3)

    t_copies = [
        remote(tl.at[:, c], tl.at[:, c], ts.at[0], ts.at[1], to_x),
        remote(tl.at[:, c], tl.at[:, c], ts.at[2], ts.at[3], to_s),
    ]
    t_on = remote(tl.at[:, cx], tl.at[:, cx], ts.at[4], ts.at[5], to_s)

    x_copy = remote(xs, xn, os.at[0], os.at[1], to_y)

    def y_copy(i):
        return remote(yo.at[i], yn.at[i], ys.at[0, i], ys.at[1, i], to_y)

    def sent(lo, hi):
        if lo == 1:
            for cp in t_copies + [t_on]:
                cp.wait_send()
        for k in range(lo, hi + 1):
            for cp in c_own(k) + c_fwd(k) + c_sib(k) + c_dia(k):
                cp.wait_send()

    def do(ops):
        for op, k in ops:
            if op == O:
                start_own(k)
            elif op == F:
                wait_first(k)
                for cp in c_fwd(k) + c_sib(k):
                    cp.start()
                if k == 1:
                    arrive(tl.at[:, cx], ts.at[1])
                    t_on.start()
            elif op == D:
                wait_dia(k)
                for cp in c_dia(k)[: 1 if k == STEPS else 2]:
                    cp.start()
            elif op == E:
                b0, bn = halves(k)[1]
                arrive(seg(k, ry, cx, b0, bn), rs.at[DX, k])
                c_dia(k)[1].start()
            elif op == R:
                b0, bn = halves(k)[1]
                arrive(seg(k, ry, csx, b0, bn), rs.at[SE, k])
            elif op == W:
                sent(1, k)
            elif op == S:
                wait_sib(k)
                if k == 1:
                    arrive(tl.at[:, cs], ts.at[3])
                    arrive(tl.at[:, csx], ts.at[5])
                    z_loc.wait()
                if k > SWAP + 1:
                    y_copy(k - SWAP - 2).start()
            elif op == T:
                for cp in t_copies:
                    cp.start()
            elif op == V:
                turn(k)
                if k == 2:
                    t_loc.wait()
                    for q in range(8):
                        tl[q, c] = jnp.concatenate([t_in[4 * q + t] for t in range(4)], axis=1)
            else:
                x_copy.start()

    def point(k, table):
        for kk, ops in table.items():
            @pl.when(k == kk)
            def _(ops=ops):
                do(ops)

    lane = lax.broadcasted_iota(jnp.int32, (128, 128), 1)
    sub = lax.broadcasted_iota(jnp.int32, (128, 128), 0)
    pr, pc = sub // 32, lane // 32
    level1 = (pr // 2 == pc // 2) & (pr < pc)
    level2 = pr // 2 < pc // 2

    def step(k, carry):
        point(k, BEFORE)
        J = STEPS - k
        base = 4 * k * (k - 1)
        acc[...] = jnp.zeros_like(acc)
        for rr in range(2):
            xt[rr, J] = z_in[pl.ds(pl.multiple_of(2048 * rr + 128 * J, 128), 128)].T

        def prepare(m, p):
            m = jnp.minimum(m, k - 1)
            for g in range(12):
                if g < 4:
                    here = [xt[rr, J + m, 32 * g : 32 * g + 32] for rr in range(2)]
                else:
                    tt, cc = divmod(g - 4, 4)
                    here = [land[base + (rr * 4 + cc) * k + m, 32 * tt : 32 * tt + 32] for rr in range(2)]
                for i, part in enumerate(split3(jnp.concatenate(here, axis=1))):
                    lp[p, i, 32 * g : 32 * g + 32] = part
                    if g >= 4:
                        vp[i, m, 32 * g - 128 : 32 * g - 96] = part

        def product(p):
            return mul6([lp[p, i] for i in range(3)], [lp[p, i, 128:384] for i in range(3)], NT)

        def four(i, carry):
            acc[...] += product(0) + product(1)
            prepare(4 * i + 2, 2)
            prepare(4 * i + 3, 3)
            acc[...] += product(2) + product(3)
            prepare(4 * i + 4, 0)
            prepare(4 * i + 5, 1)
            return carry

        fours, left = lax.div(k, 4), lax.rem(k, 4)
        mid = lax.div(fours + 1, 2)
        prepare(0, 0)
        prepare(1, 1)
        lax.fori_loop(0, mid, four, 0)
        point(k, MIDDLE)
        lax.fori_loop(mid, fours, four, 0)

        @pl.when(left == 1)
        def _():
            acc[...] += product(0)

        @pl.when(left >= 2)
        def _():
            acc[...] += product(0) + product(1)

        @pl.when(left == 3)
        def _():
            prepare(k - 1, 2)
            acc[...] += product(2)

        q, h = J // 2, lax.rem(J, 2)

        def diag(tt):
            rows = []
            for cc in range(4):
                t32 = tl[q, cc]
                t32 = jnp.where(h == 0, t32, pltpu.roll(t32, 64, 1))
                shift = (32 * cc - 32 * tt) % 128
                rows.append(pltpu.roll(t32, shift, 1) if shift else t32)
            full = jnp.concatenate(rows, axis=0)
            return jnp.where(pr == pc, full, 0.0)

        halves_t = []
        for tt in range(2):
            g = acc[128 + 128 * tt : 256 + 128 * tt, 128 * tt : 128 * tt + 128]
            t = diag(tt)
            t = t - mulf(t, mulf(jnp.where(level1, g, 0.0), t))
            t = t - mulf(t, mulf(jnp.where(level2, g, 0.0), t))
            halves_t.append(t)
        t1, t2 = halves_t
        t12 = -mulf(t1, mulf(acc[128:256, 128:256], t2))
        w1, w2 = acc[0:128, 0:128], acc[0:128, 128:256]
        w2s = split3(w2)
        y1 = mul6(split3(w1), split3(t1), NT) + mul6(w2s, split3(t12), NT)
        y2 = mul6(w2s, split3(t2), NT)
        y = jnp.concatenate([y1, y2], axis=1)
        for i, part in enumerate(split3(y)):
            yp[i] = part

        @pl.when(k > SWAP)
        def _():
            yo[k - SWAP - 1] = y

        point(k, AFTER)

        def update(m, n):
            ps = [yp[i] for i in range(3)]
            ds = [mul6(ps, [vp[i, m + u] for i in range(3)], NN) for u in range(n)]
            for u, d in enumerate(ds):
                xt[0, J + m + u] = xt[0, J + m + u] - d[:, :128]
                xt[1, J + m + u] = xt[1, J + m + u] - d[:, 128:]

        @pl.when(k < STEPS)
        def _():
            by_four(0, k, update)

        @pl.when(k == SWAP)
        def _():
            for m in range(STEPS - SWAP):
                xt[ry, m] = z_in[pl.ds(pl.multiple_of(2048 * ry + 128 * m, 128), 128)].T

            def stage(m, carry):
                xs[m] = xt[ry, m]
                return carry

            lax.fori_loop(0, STEPS, stage, 0)

        return carry

    lax.fori_loop(1, STEPS + 1, step, 0)

    def half(dst, k, parts, lo, hi, put=None):
        def tiles(m, n):
            ds = [mul6(parts, split3(rows(k, 8 * OFF[k], r, m + u)), NN) for u in range(n)]
            for u, d in enumerate(ds):
                x = dst[STEPS - k + m + u] - d
                if put is None:
                    dst[STEPS - k + m + u] = x
                else:
                    here = pl.ds(pl.multiple_of(128 * (m + u), 128), 128)
                    ob[here, pl.ds(pl.multiple_of(128 * put, 128), 128)] = x.T

        by_four(lo, hi, tiles)

    last = [yp[i] for i in range(3)]
    half(xt.at[r], STEPS, last, 0, 4, r)
    y_copy(REST - 1).start()
    half(xt.at[r], STEPS, last, 4, STEPS, r)
    arrive(xn, os.at[1])
    for i in range(REST):
        arrive(yn.at[i], ys.at[1, i])
        if i < REST - 1:
            half(xn, SWAP + 1 + i, split3(yn[i]), 0, SWAP + 1 + i)
    theirs = split3(yn[REST - 1])
    outs = []
    for i in range(4):
        half(xn, STEPS, theirs, 4 * i, 4 * i + 4, ry)
        here = pl.ds(512 * i, 512)
        outs.append(pltpu.make_async_copy(ob.at[here], out_ref.at[here], rs.at[LO, 9 + i]))
        if i:
            outs[i - 1].start()

    sent(14, STEPS)
    x_copy.wait_send()
    for i in range(REST):
        y_copy(i).wait_send()
    outs[3].start()
    for cp in outs:
        cp.wait()


def solution(mesh):
    def body(v_loc, t_loc, z_loc):
        return pl.pallas_call(
            kernel,
            out_shape=jax.ShapeDtypeStruct((2048, 256), F32),
            in_specs=[pl.BlockSpec(memory_space=pl.ANY)] * 3,
            out_specs=pl.BlockSpec(memory_space=pl.ANY),
            scratch_shapes=[
                pltpu.VMEM((256 * OFF[9], 128), F32),
                pltpu.VMEM((32, 32, 32), F32),
                pltpu.VMEM((4096, 128), F32),
                pltpu.VMEM((2048, 256), F32),
                pltpu.VMEM((8 * OFF[STEPS + 1], 64, 128), F32),
                pltpu.VMEM((8, 4, 32, 128), F32),
                pltpu.VMEM((2, 16, 128, 128), F32),
                pltpu.VMEM((16, 128, 128), F32),
                pltpu.VMEM((16, 128, 128), F32),
                pltpu.VMEM((REST, 128, 256), F32),
                pltpu.VMEM((REST, 128, 256), F32),
                pltpu.VMEM((3, 16, 256, 256), BF16),
                pltpu.VMEM((4, 3, 384, 256), BF16),
                pltpu.VMEM((384, 256), F32),
                pltpu.VMEM((3, 128, 256), BF16),
                pltpu.SemaphoreType.DMA((10, STEPS + 1)),
                pltpu.SemaphoreType.DMA((9, STEPS + 1)),
                pltpu.SemaphoreType.DMA((7,)),
                pltpu.SemaphoreType.DMA((1,)),
                pltpu.SemaphoreType.DMA((4,)),
                pltpu.SemaphoreType.DMA((2, REST)),
            ],
            compiler_params=pltpu.CompilerParams(
                collective_id=0, has_side_effects=True, vmem_limit_bytes=64 * 1024 * 1024 - 65536
            ),
        )(v_loc, t_loc, z_loc)

    return jax.shard_map(
        body,
        mesh=mesh,
        in_specs=(P("row", "col"), P("col", None, None), P(None, ("col", "row"))),
        out_specs=P("row", "col"),
        check_vma=False,
    )
```

```python
import functools

import jax
import jax.numpy as jnp
from jax import lax
from jax.experimental import pallas as pl
from jax.experimental.pallas import tpu as pltpu
from jax.sharding import PartitionSpec as P

MESH = pl.DeviceIdType.MESH
F32, BF16 = jnp.float32, jnp.bfloat16
STEPS = 16
OFF = [k * (k - 1) // 2 for k in range(STEPS + 2)]
NT = (((1,), (1,)), ((), ()))
NN = (((1,), (0,)), ((), ()))
SWAP = 14
REST = STEPS - SWAP
O, F, D, S, T, X, V, E, R, W = range(10)
BEFORE = {k: ((S, k),) for k in range(2, STEPS + 1)}
BEFORE[1] = ((V, 1), (V, 2), (O, 1), (O, 2), (V, 3), (T, 0), (O, 3), (F, 1), (O, 4), (F, 2), (D, 1), (S, 1))
BEFORE[14] = ((F, 15), (S, 14))
BEFORE[15] = ((F, 16), (X, 0), (D, 15), (W, 13), (S, 15))
BEFORE[16] = ((S, 16), (E, 16))
MIDDLE = {k: ((F, k + 2), (O, k + 4)) for k in range(1, 13)}
MIDDLE |= {k: MIDDLE[k] + ((V, (k + 7) // 2),) for k in range(1, 10, 2)}
MIDDLE[16] = ((R, 16),)
AFTER = {k: ((D, k + 1),) for k in (*range(1, 14), 15)}
ALONG_Y = [0, 0, 1, 1, 2, 2, 3, 4, 4, 5, 5, 6, 6, 7, 7, 5, 10]
FX, FY, DX, DY, SO, SX, SY, SD, SE, LO = range(10)
TX, TY, TS, GX, GY, HX, HY, HD, HE = range(9)


def split3(a):
    p1 = a.astype(BF16)
    rest = a - p1.astype(F32)
    p2 = rest.astype(BF16)
    p3 = (rest - p2.astype(F32)).astype(BF16)
    return p1, p2, p3


def mul6(a, b, dims):
    dot = functools.partial(lax.dot_general, dimension_numbers=dims, preferred_element_type=F32)
    return (
        dot(a[0], b[0]) + dot(a[1], b[0]) + dot(a[2], b[0]) + dot(a[0], b[1]) + dot(a[1], b[1]) + dot(a[0], b[2])
    )


def mulf(a, b, dims=NN):
    return mul6(split3(a), split3(b), dims)


def by_four(lo, hi, fn):
    fours = lax.div(hi - lo, 4)

    def four(i, carry):
        fn(lo + 4 * i, 4)
        return carry

    def one(m, carry):
        fn(m, 1)
        return carry

    lax.fori_loop(0, fours, four, 0)
    lax.fori_loop(lo + 4 * fours, hi, one, 0)


def kernel(v_ref, t_ref, z_ref, out_ref, vs_in, t_in, z_in, ob, land, tl, xt, xs, xn, yo, yn, vp, lp, acc, yp, rs, ss, ts, zs, os, ys):
    r, c = lax.axis_index("row"), lax.axis_index("col")
    cs = c + 1 - 2 * lax.rem(c, 2)
    cx = lax.rem(c + 2, 4)
    csx = lax.rem(cs + 2, 4)
    ry = 1 - r
    to_x, to_y, to_s = (r, cx), (ry, c), (r, cs)

    def seg(k, rr, cc, lo=0, n=None):
        return land.at[pl.ds(8 * OFF[k] + (rr * 4 + cc) * k + lo, k if n is None else n)]

    def rows(k, base, rr, m):
        got = [land[base + (rr * 4 + cc) * k + m] for cc in range(4)]
        return jnp.concatenate([g[:32] for g in got] + [g[32:] for g in got], axis=0)

    def remote(src, dst, send, recv, dev):
        return pltpu.make_async_remote_copy(
            src_ref=src, dst_ref=dst, send_sem=send, recv_sem=recv, device_id=dev, device_id_type=MESH
        )

    def halves(k):
        h = ALONG_Y[k]
        return (0, h), (h, k - h)

    def c_own(k):
        mine = seg(k, r, c)
        return [
            remote(mine, mine, ss.at[TX, k], rs.at[FX, k], to_x),
            remote(mine, mine, ss.at[TY, k], rs.at[FY, k], to_y),
            remote(mine, mine, ss.at[TS, k], rs.at[SO, k], to_s),
        ]

    def c_loc(n):
        q = STEPS // 2 - n
        return pltpu.make_async_copy(
            v_ref.at[pl.ds(256 * q, 256 * n), pl.ds(128 * q, 128)], vs_in.at[pl.ds(256 * OFF[n], 256 * n)], rs.at[LO, n]
        )

    def turn(n):
        c_loc(n).wait()
        even, odd = (8 * OFF[k] + (r * 4 + c) * k for k in (2 * n, 2 * n - 1))

        def tile(m, carry):
            t = vs_in[pl.ds(pl.multiple_of(256 * OFF[n] + 128 * m, 128), 128)].T
            land[even + m] = t[:64]

            @pl.when(m > 0)
            def _():
                land[odd + m - 1] = t[64:]

            return carry

        lax.fori_loop(0, 2 * n, tile, 0)

    def c_fwd(k):
        (a0, an), (b0, bn) = halves(k)
        out = []
        if k == STEPS:
            out.append(remote(seg(k, ry, c, a0, an), seg(k, ry, c, a0, an), ss.at[GY, k], rs.at[DY, k], to_x))
        elif an:
            out.append(remote(seg(k, r, cx, a0, an), seg(k, r, cx, a0, an), ss.at[GY, k], rs.at[DY, k], to_y))
        if bn:
            out.append(remote(seg(k, ry, c, b0, bn), seg(k, ry, c, b0, bn), ss.at[GX, k], rs.at[DX, k], to_x))
        return out

    def c_sib(k):
        return [
            remote(seg(k, r, cx), seg(k, r, cx), ss.at[HX, k], rs.at[SX, k], to_s),
            remote(seg(k, ry, c), seg(k, ry, c), ss.at[HY, k], rs.at[SY, k], to_s),
        ]

    def c_dia(k):
        (a0, an), (b0, bn) = halves(k)
        out = []
        if an:
            out.append(remote(seg(k, ry, cx, a0, an), seg(k, ry, cx, a0, an), ss.at[HD, k], rs.at[SD, k], to_s))
        if bn:
            out.append(remote(seg(k, ry, cx, b0, bn), seg(k, ry, cx, b0, bn), ss.at[HE, k], rs.at[SE, k], to_s))
        return out

    def arrive(dst, sem):
        pltpu.make_async_copy(dst, dst, sem).wait()

    def wait_first(k):
        arrive(seg(k, r, cx), rs.at[FX, k])
        arrive(seg(k, ry, c), rs.at[FY, k])

    def wait_dia(k):
        (a0, an), (b0, bn) = halves(k)
        if an:
            arrive(seg(k, ry, cx, a0, an), rs.at[DY, k])
        if bn and k < STEPS:
            arrive(seg(k, ry, cx, b0, bn), rs.at[DX, k])

    def wait_sib(k):
        arrive(seg(k, r, cs), rs.at[SO, k])
        arrive(seg(k, r, csx), rs.at[SX, k])
        arrive(seg(k, ry, cs), rs.at[SY, k])
        (a0, an), (b0, bn) = halves(k)
        if an:
            arrive(seg(k, ry, csx, a0, an), rs.at[SD, k])
        if bn and k < STEPS:
            arrive(seg(k, ry, csx, b0, bn), rs.at[SE, k])

    def start_own(k):
        for cp in c_own(k):
            cp.start()

    t_loc = pltpu.make_async_copy(t_ref, t_in, ts.at[6])
    z_loc = pltpu.make_async_copy(z_ref, z_in, zs.at[0])
    for n in range(1, STEPS // 2 + 1):
        c_loc(n).start()
        if n == 2:
            t_loc.start()
            z_loc.start()
    barrier = pltpu.get_barrier_semaphore()
    for dev in (to_x, to_y, to_s):
        pl.semaphore_signal(barrier, inc=1, device_id=dev, device_id_type=MESH)
    pl.semaphore_wait(barrier, 3)

    t_copies = [
        remote(tl.at[:, c], tl.at[:, c], ts.at[0], ts.at[1], to_x),
        remote(tl.at[:, c], tl.at[:, c], ts.at[2], ts.at[3], to_s),
    ]
    t_on = remote(tl.at[:, cx], tl.at[:, cx], ts.at[4], ts.at[5], to_s)

    x_copy = remote(xs, xn, os.at[0], os.at[1], to_y)

    def y_copy(i):
        return remote(yo.at[i], yn.at[i], ys.at[0, i], ys.at[1, i], to_y)

    def sent(lo, hi):
        if lo == 1:
            for cp in t_copies + [t_on]:
                cp.wait_send()
        for k in range(lo, hi + 1):
            for cp in c_own(k) + c_fwd(k) + c_sib(k) + c_dia(k):
                cp.wait_send()

    def do(ops):
        for op, k in ops:
            if op == O:
                start_own(k)
            elif op == F:
                wait_first(k)
                for cp in c_fwd(k) + c_sib(k):
                    cp.start()
                if k == 1:
                    arrive(tl.at[:, cx], ts.at[1])
                    t_on.start()
            elif op == D:
                wait_dia(k)
                for cp in c_dia(k)[: 1 if k == STEPS else 2]:
                    cp.start()
            elif op == E:
                b0, bn = halves(k)[1]
                arrive(seg(k, ry, cx, b0, bn), rs.at[DX, k])
                c_dia(k)[1].start()
            elif op == R:
                b0, bn = halves(k)[1]
                arrive(seg(k, ry, csx, b0, bn), rs.at[SE, k])
            elif op == W:
                sent(1, k)
            elif op == S:
                wait_sib(k)
                if k == 1:
                    arrive(tl.at[:, cs], ts.at[3])
                    arrive(tl.at[:, csx], ts.at[5])
                    z_loc.wait()
                if k > SWAP + 1:
                    y_copy(k - SWAP - 2).start()
            elif op == T:
                for cp in t_copies:
                    cp.start()
            elif op == V:
                turn(k)
                if k == 2:
                    t_loc.wait()
                    for q in range(8):
                        tl[q, c] = jnp.concatenate([t_in[4 * q + t] for t in range(4)], axis=1)
            else:
                x_copy.start()

    def point(k, table):
        for kk, ops in table.items():
            @pl.when(k == kk)
            def _(ops=ops):
                do(ops)

    lane = lax.broadcasted_iota(jnp.int32, (128, 128), 1)
    sub = lax.broadcasted_iota(jnp.int32, (128, 128), 0)
    pr, pc = sub // 32, lane // 32
    level1 = (pr // 2 == pc // 2) & (pr < pc)
    level2 = pr // 2 < pc // 2

    def step(k, carry):
        point(k, BEFORE)
        J = STEPS - k
        base = 4 * k * (k - 1)
        acc[...] = jnp.zeros_like(acc)
        for rr in range(2):
            xt[rr, J] = z_in[pl.ds(pl.multiple_of(2048 * rr + 128 * J, 128), 128)].T

        def prepare(m, p):
            m = jnp.minimum(m, k - 1)
            for g in range(12):
                if g < 4:
                    here = [xt[rr, J + m, 32 * g : 32 * g + 32] for rr in range(2)]
                else:
                    tt, cc = divmod(g - 4, 4)
                    here = [land[base + (rr * 4 + cc) * k + m, 32 * tt : 32 * tt + 32] for rr in range(2)]
                for i, part in enumerate(split3(jnp.concatenate(here, axis=1))):
                    lp[p, i, 32 * g : 32 * g + 32] = part
                    if g >= 4:
                        vp[i, m, 32 * g - 128 : 32 * g - 96] = part

        def product(p):
            return mul6([lp[p, i] for i in range(3)], [lp[p, i, 128:384] for i in range(3)], NT)

        def four(i, carry):
            acc[...] += product(0) + product(1)
            prepare(4 * i + 2, 2)
            prepare(4 * i + 3, 3)
            acc[...] += product(2) + product(3)
            prepare(4 * i + 4, 0)
            prepare(4 * i + 5, 1)
            return carry

        fours, left = lax.div(k, 4), lax.rem(k, 4)
        mid = lax.div(fours + 1, 2)
        prepare(0, 0)
        prepare(1, 1)
        lax.fori_loop(0, mid, four, 0)
        point(k, MIDDLE)
        lax.fori_loop(mid, fours, four, 0)

        @pl.when(left == 1)
        def _():
            acc[...] += product(0)

        @pl.when(left >= 2)
        def _():
            acc[...] += product(0) + product(1)

        @pl.when(left == 3)
        def _():
            prepare(k - 1, 2)
            acc[...] += product(2)

        q, h = J // 2, lax.rem(J, 2)

        def diag(tt):
            rows = []
            for cc in range(4):
                t32 = tl[q, cc]
                t32 = jnp.where(h == 0, t32, pltpu.roll(t32, 64, 1))
                shift = (32 * cc - 32 * tt) % 128
                rows.append(pltpu.roll(t32, shift, 1) if shift else t32)
            full = jnp.concatenate(rows, axis=0)
            return jnp.where(pr == pc, full, 0.0)

        halves_t = []
        for tt in range(2):
            g = acc[128 + 128 * tt : 256 + 128 * tt, 128 * tt : 128 * tt + 128]
            t = diag(tt)
            t = t - mulf(t, mulf(jnp.where(level1, g, 0.0), t))
            t = t - mulf(t, mulf(jnp.where(level2, g, 0.0), t))
            halves_t.append(t)
        t1, t2 = halves_t
        t12 = -mulf(t1, mulf(acc[128:256, 128:256], t2))
        w1, w2 = acc[0:128, 0:128], acc[0:128, 128:256]
        w2s = split3(w2)
        y1 = mul6(split3(w1), split3(t1), NT) + mul6(w2s, split3(t12), NT)
        y2 = mul6(w2s, split3(t2), NT)
        y = jnp.concatenate([y1, y2], axis=1)
        for i, part in enumerate(split3(y)):
            yp[i] = part

        @pl.when(k > SWAP)
        def _():
            yo[k - SWAP - 1] = y

        point(k, AFTER)

        def update(m, n):
            ps = [yp[i] for i in range(3)]
            ds = [mul6(ps, [vp[i, m + u] for i in range(3)], NN) for u in range(n)]
            for u, d in enumerate(ds):
                xt[0, J + m + u] = xt[0, J + m + u] - d[:, :128]
                xt[1, J + m + u] = xt[1, J + m + u] - d[:, 128:]

        @pl.when(k < STEPS)
        def _():
            by_four(0, k, update)

        @pl.when(k == SWAP)
        def _():
            for m in range(STEPS - SWAP):
                xt[ry, m] = z_in[pl.ds(pl.multiple_of(2048 * ry + 128 * m, 128), 128)].T

            def stage(m, carry):
                xs[m] = xt[ry, m]
                return carry

            lax.fori_loop(0, STEPS, stage, 0)

        return carry

    lax.fori_loop(1, STEPS + 1, step, 0)

    def half(dst, k, parts, lo, hi, put=None):
        def tiles(m, n):
            ds = [mul6(parts, split3(rows(k, 8 * OFF[k], r, m + u)), NN) for u in range(n)]
            for u, d in enumerate(ds):
                x = dst[STEPS - k + m + u] - d
                if put is None:
                    dst[STEPS - k + m + u] = x
                else:
                    here = pl.ds(pl.multiple_of(128 * (m + u), 128), 128)
                    ob[here, pl.ds(pl.multiple_of(128 * put, 128), 128)] = x.T

        by_four(lo, hi, tiles)

    last = [yp[i] for i in range(3)]
    half(xt.at[r], STEPS, last, 0, 4, r)
    y_copy(REST - 1).start()
    half(xt.at[r], STEPS, last, 4, STEPS, r)
    arrive(xn, os.at[1])
    for i in range(REST):
        arrive(yn.at[i], ys.at[1, i])
        if i < REST - 1:
            half(xn, SWAP + 1 + i, split3(yn[i]), 0, SWAP + 1 + i)
    theirs = split3(yn[REST - 1])
    outs = []
    for i in range(4):
        half(xn, STEPS, theirs, 4 * i, 4 * i + 4, ry)
        here = pl.ds(512 * i, 512)
        outs.append(pltpu.make_async_copy(ob.at[here], out_ref.at[here], rs.at[LO, 9 + i]))
        if i:
            outs[i - 1].start()

    sent(14, STEPS)
    x_copy.wait_send()
    for i in range(REST):
        y_copy(i).wait_send()
    outs[3].start()
    for cp in outs:
        cp.wait()


def solution(mesh):
    def body(v_loc, t_loc, z_loc):
        return pl.pallas_call(
            kernel,
            out_shape=jax.ShapeDtypeStruct((2048, 256), F32),
            in_specs=[pl.BlockSpec(memory_space=pl.ANY)] * 3,
            out_specs=pl.BlockSpec(memory_space=pl.ANY),
            scratch_shapes=[
                pltpu.VMEM((256 * OFF[9], 128), F32),
                pltpu.VMEM((32, 32, 32), F32),
                pltpu.VMEM((4096, 128), F32),
                pltpu.VMEM((2048, 256), F32),
                pltpu.VMEM((8 * OFF[STEPS + 1], 64, 128), F32),
                pltpu.VMEM((8, 4, 32, 128), F32),
                pltpu.VMEM((2, 16, 128, 128), F32),
                pltpu.VMEM((16, 128, 128), F32),
                pltpu.VMEM((16, 128, 128), F32),
                pltpu.VMEM((REST, 128, 256), F32),
                pltpu.VMEM((REST, 128, 256), F32),
                pltpu.VMEM((3, 16, 256, 256), BF16),
                pltpu.VMEM((4, 3, 384, 256), BF16),
                pltpu.VMEM((384, 256), F32),
                pltpu.VMEM((3, 128, 256), BF16),
                pltpu.SemaphoreType.DMA((10, STEPS + 1)),
                pltpu.SemaphoreType.DMA((9, STEPS + 1)),
                pltpu.SemaphoreType.DMA((7,)),
                pltpu.SemaphoreType.DMA((1,)),
                pltpu.SemaphoreType.DMA((4,)),
                pltpu.SemaphoreType.DMA((2, REST)),
            ],
            compiler_params=pltpu.CompilerParams(
                collective_id=0, has_side_effects=True, vmem_limit_bytes=64 * 1024 * 1024 - 65536
            ),
        )(v_loc, t_loc, z_loc)

    return jax.shard_map(
        body,
        mesh=mesh,
        in_specs=(P("row", "col"), P("col", None, None), P(None, ("col", "row"))),
        out_specs=P("row", "col"),
        check_vma=False,
    )
```
